128 devices in a mesh: dp: 1, sp: 128 (over z, y, x, core).
Axes of the slice: x: 4, y: 4, z: 4, core: 2. Of those that a mesh axis runs over, the one named last changes fastest.
Arguments:
- x_in: bfloat16 [4096, 3584], P(('dp', 'sp'))
- seg_id: int32 [4096], P(('dp', 'sp'))
- pos_id: int32 [4096], P(('dp', 'sp'))
- w_dq: bfloat16 [3584, 768], replicated
- g_q: bfloat16 [768], replicated
- w_uq: bfloat16 [768, 24576], replicated
- w_dkv: bfloat16 [3584, 576], replicated
- g_kv: bfloat16 [512], replicated
- w_ukv: bfloat16 [512, 32768], replicated
- w_o: bfloat16 [16384, 3584], replicated
- g_ffn: bfloat16 [3584], replicated
- w_gate: bfloat16 [3584, 9216], P(None, 'sp')
- w_up: bfloat16 [3584, 9216], P(None, 'sp')
- w_down: bfloat16 [9216, 3584], P('sp')
Outputs:
- output: bfloat16 [4096, 3584], P(('dp', 'sp'))
All inputs are finite; a program needn't handle non-finite values.
Results may differ from the reference program's by a relative error of at most 0.0161625.
Values are sent between devices in bfloat16 or wider.
A program may use at most 1 GiB of HBM per device.

```python
import jax
import jax.numpy as jnp
from jax import lax

D = 3584
HEADS = 128
Q_LAT = 768
FF = 9216
TOKENS = 4096
KV_LATENT = 512
ROPE_DIM = 64
NOPE_DIM = 128
VALUE_DIM = 128
MAX_CUTS = 3
QK_DIM = NOPE_DIM + ROPE_DIM
KV_DIM = NOPE_DIM + VALUE_DIM


def rms_norm(vec_in, gain_vec):
    mean_sq = jnp.mean(vec_in * vec_in, axis=-1, keepdims=True)
    return vec_in * lax.rsqrt(mean_sq + 1e-6) * gain_vec.astype(jnp.float32)


def apply_rope(vec_in, positions):
    half_dim = ROPE_DIM // 2
    inv_freq = 10000.0 ** (-jnp.arange(half_dim, dtype=jnp.float32) / half_dim)
    angles = positions.astype(jnp.float32)[..., None] * inv_freq
    cosine = jnp.cos(angles)
    sine_v = jnp.sin(angles)
    lo_half = vec_in[..., :half_dim]
    hi_half = vec_in[..., half_dim:]
    return jnp.concatenate([lo_half * cosine - hi_half * sine_v, hi_half * cosine + lo_half * sine_v], axis=-1)


def draw_prompts(root_key):
    cut_key, count_key = jax.random.split(root_key)
    cut_at = jax.random.randint(cut_key, (MAX_CUTS,), 1, TOKENS)
    n_cuts = jax.random.randint(count_key, (), 1, MAX_CUTS + 1)
    cut_used = (jnp.arange(MAX_CUTS) < n_cuts).astype(jnp.int32)
    cut_marks = jnp.zeros((TOKENS,), jnp.int32).at[cut_at].max(cut_used)
    seg_id = jnp.cumsum(cut_marks).astype(jnp.int32)
    tok_index = jnp.arange(TOKENS, dtype=jnp.int32)
    starts = lax.cummax(jnp.where(cut_marks > 0, tok_index, 0), axis=0)
    return seg_id, (tok_index - starts).astype(jnp.int32)


def normal_weight(w_key, arr_shape, fan_in):
    return (jax.random.normal(w_key, arr_shape, jnp.float32) * fan_in ** -0.5).astype(jnp.bfloat16)


def gain_draw(w_key, arr_shape):
    return jax.random.uniform(w_key, arr_shape, jnp.float32, 0.5, 1.5).astype(jnp.bfloat16)


def setup_inputs(seed: int = 0, part: int = 0) -> dict:
    root_key = jax.random.key(seed)
    shared_key, part_root = jax.random.split(root_key)
    part_key = jax.random.fold_in(part_root, part)
    x_key, prompt_key = jax.random.split(part_key)
    sub_keys = jax.random.split(shared_key, 11)
    seg_id, pos_id = draw_prompts(prompt_key)
    return {
        'x_in': jax.random.normal(x_key, (TOKENS, D), jnp.float32).astype(jnp.bfloat16),
        'seg_id': seg_id,
        'pos_id': pos_id,
        'w_dq': normal_weight(sub_keys[0], (D, Q_LAT), D),
        'g_q': gain_draw(sub_keys[1], (Q_LAT,)),
        'w_uq': normal_weight(sub_keys[2], (Q_LAT, HEADS * QK_DIM), Q_LAT),
        'w_dkv': normal_weight(sub_keys[3], (D, KV_LATENT + ROPE_DIM), D),
        'g_kv': gain_draw(sub_keys[4], (KV_LATENT,)),
        'w_ukv': normal_weight(sub_keys[5], (KV_LATENT, HEADS * KV_DIM), KV_LATENT),
        'w_o': normal_weight(sub_keys[6], (HEADS * VALUE_DIM, D), HEADS * VALUE_DIM),
        'g_ffn': gain_draw(sub_keys[7], (D,)),
        'w_gate': normal_weight(sub_keys[8], (D, FF), D),
        'w_up': normal_weight(sub_keys[9], (D, FF), D),
        'w_down': normal_weight(sub_keys[10], (FF, D), FF),
    }


def reference(x_in, seg_id, pos_id, w_dq, g_q, w_uq, w_dkv, g_kv, w_ukv, w_o, g_ffn, w_gate, w_up, w_down):
    q_lin = jnp.dot(x_in, w_dq, preferred_element_type=jnp.float32)
    c_q = rms_norm(q_lin, g_q).astype(jnp.bfloat16)
    kv_lin = jnp.dot(x_in, w_dkv, preferred_element_type=jnp.float32)
    c_kv = rms_norm(kv_lin[:, :KV_LATENT], g_kv).astype(jnp.bfloat16)
    k_rope = apply_rope(kv_lin[:, KV_LATENT:], pos_id).astype(jnp.bfloat16)
    allowed = (seg_id[:, None] == seg_id[None, :]) & (pos_id[None, :] <= pos_id[:, None])
    score_scale = QK_DIM ** -0.5
    w_uq_heads = jnp.transpose(w_uq.reshape(Q_LAT, HEADS, QK_DIM), (1, 0, 2))
    w_ukv_heads = jnp.transpose(w_ukv.reshape(KV_LATENT, HEADS, KV_DIM), (1, 0, 2))

    def one_head(weights):
        wq_head, wkv_head = weights
        q_head = jnp.dot(c_q, wq_head, preferred_element_type=jnp.float32)
        q_nope = q_head[:, :NOPE_DIM].astype(jnp.bfloat16)
        q_rope = apply_rope(q_head[:, NOPE_DIM:], pos_id).astype(jnp.bfloat16)
        kv_head = jnp.dot(c_kv, wkv_head, preferred_element_type=jnp.float32).astype(jnp.bfloat16)
        k_nope = kv_head[:, :NOPE_DIM]
        v_head = kv_head[:, NOPE_DIM:]
        scores = jnp.dot(q_nope, k_nope.T, preferred_element_type=jnp.float32) + jnp.dot(q_rope, k_rope.T, preferred_element_type=jnp.float32)
        scores = jnp.where(allowed, scores * score_scale, -jnp.inf)
        row_peak = jnp.max(scores, axis=1, keepdims=True)
        prob_w = jnp.exp(scores - row_peak)
        row_total = jnp.sum(prob_w, axis=1, keepdims=True)
        head_out = jnp.dot(prob_w.astype(jnp.bfloat16), v_head, preferred_element_type=jnp.float32) / row_total
        return head_out.astype(jnp.bfloat16)

    o_heads = lax.map(one_head, (w_uq_heads, w_ukv_heads))
    o_all = jnp.transpose(o_heads, (1, 0, 2)).reshape(TOKENS, HEADS * VALUE_DIM)
    y_att = jnp.dot(o_all, w_o, preferred_element_type=jnp.float32).astype(jnp.bfloat16)
    h_ffn = rms_norm(y_att.astype(jnp.float32), g_ffn).astype(jnp.bfloat16)
    gate_lin = jnp.dot(h_ffn, w_gate, preferred_element_type=jnp.float32)
    up_lin = jnp.dot(h_ffn, w_up, preferred_element_type=jnp.float32)
    act_val = (jax.nn.silu(gate_lin) * up_lin).astype(jnp.bfloat16)
    ffn_out = jnp.dot(act_val, w_down, preferred_element_type=jnp.float32)
    return (y_att.astype(jnp.float32) + ffn_out).astype(jnp.bfloat16)
```

```python
import functools

import jax
import jax.numpy as jnp
from jax import lax
from jax.experimental import pallas as pl
from jax.experimental.pallas import tpu as pltpu
from jax.sharding import PartitionSpec as P

NOPE_DIM = 128
ROPE_DIM = 64
VALUE_DIM = 128
KV_LATENT = 512
QK_DIM = NOPE_DIM + ROPE_DIM
KV_DIM = NOPE_DIM + VALUE_DIM
SCORE_SCALE = QK_DIM ** -0.5
LOG2E = 1.4426950408889634
MASKED = -0.7 * 3.4028234663852886e38

RING = 4
CORES = 2


def rms_norm(vec_in, gain_vec):
    mean_sq = jnp.mean(vec_in * vec_in, axis=-1, keepdims=True)
    return vec_in * lax.rsqrt(mean_sq + 1e-6) * gain_vec.astype(jnp.float32)


def rope_angles(positions):
    half_dim = ROPE_DIM // 2
    inv_freq = 10000.0 ** (-jnp.arange(half_dim, dtype=jnp.float32) / half_dim)
    return positions.astype(jnp.float32)[..., None] * inv_freq


def apply_rope(vec_in, positions):
    half_dim = ROPE_DIM // 2
    angles = rope_angles(positions)
    cosine = jnp.cos(angles)
    sine_v = jnp.sin(angles)
    lo_half = vec_in[..., :half_dim]
    hi_half = vec_in[..., half_dim:]
    return jnp.concatenate([lo_half * cosine - hi_half * sine_v, hi_half * cosine + lo_half * sine_v], axis=-1)


def attn_kernel(lo_ref, clear_ref, cq_ref, kv_ref, wq_ref, wk_ref, wv_ref, cos_ref, sin_ref, start_ref, pos_ref,
                o_ref, k_buf, v_buf, q_buf, acc_ref, *, blk, n_blk):
    i = pl.program_id(0)
    half = ROPE_DIM // 2
    nt = (((1,), (1,)), ((), ()))

    @pl.when(i == 0)
    def _():
        @pl.loop(0, n_blk)
        def _(b):
            rows = pl.ds(pl.multiple_of(b * blk, blk), blk)
            lat = kv_ref[rows, :KV_LATENT]
            k_buf[rows, :NOPE_DIM] = jnp.dot(lat, wk_ref[...], preferred_element_type=jnp.float32).astype(jnp.bfloat16)
            k_buf[rows, NOPE_DIM:] = kv_ref[rows, KV_LATENT:]
            v_buf[:, rows] = lax.dot_general(wv_ref[...], lat, nt, preferred_element_type=jnp.float32).astype(jnp.bfloat16)
        q_buf[QK_DIM:, :] = jnp.zeros((2 * NOPE_DIM - QK_DIM, blk), jnp.bfloat16)

    qt = lax.dot_general(wq_ref[...], cq_ref[...], nt, preferred_element_type=jnp.float32)
    q_buf[:NOPE_DIM, :] = qt[:NOPE_DIM].astype(jnp.bfloat16)
    lo_half = qt[NOPE_DIM:NOPE_DIM + half]
    hi_half = qt[NOPE_DIM + half:]
    q_buf[NOPE_DIM:NOPE_DIM + half, :] = (lo_half * cos_ref[...] - hi_half * sin_ref[...]).astype(jnp.bfloat16)
    q_buf[NOPE_DIM + half:QK_DIM, :] = (hi_half * cos_ref[...] + lo_half * sin_ref[...]).astype(jnp.bfloat16)
    acc_ref[...] = jnp.zeros_like(acc_ref)

    def block(masked, kb, carry):
        m_old, l_old = carry
        rows = pl.ds(pl.multiple_of(kb * blk, blk), blk)
        s = jnp.dot(k_buf[rows, :], q_buf[...], preferred_element_type=jnp.float32)
        if masked:
            key = kb * blk + lax.broadcasted_iota(jnp.int32, s.shape, 0)
            back = key - start_ref[...]
            s = jnp.where((back >= 0) & (back <= pos_ref[...]), s, MASKED)
        m_new = jnp.maximum(m_old, jnp.max(s, axis=0, keepdims=True))
        p = jnp.exp2((s - m_new) * (SCORE_SCALE * LOG2E))
        alpha = jnp.exp2((m_old - m_new) * (SCORE_SCALE * LOG2E))
        l_new = l_old * alpha + jnp.sum(p, axis=0, keepdims=True)
        acc_ref[...] = acc_ref[...] * alpha + jnp.dot(v_buf[:, rows], p.astype(jnp.bfloat16), preferred_element_type=jnp.float32)
        return m_new, l_new

    carry = (jnp.full((1, blk), MASKED, jnp.float32), jnp.zeros((1, blk), jnp.float32))
    lo = lo_ref[i]
    clear = clear_ref[i]
    carry = lax.fori_loop(lo, clear, functools.partial(block, True), carry)
    carry = lax.fori_loop(clear, i, functools.partial(block, False), carry)
    _, total = block(True, i, carry)
    o_ref[...] = (acc_ref[...] / total).T.astype(jnp.bfloat16)


def attention(cq_all, kv_all, w_uq, w_ukv, pos_all, blk):
    tok = cq_all.shape[0]
    n_blk = tok // blk
    half = ROPE_DIM // 2
    start = jnp.arange(tok, dtype=jnp.int32) - pos_all
    lo = start[::blk] // blk
    clear = jnp.clip((start[blk - 1::blk] + blk - 1) // blk, lo, jnp.arange(n_blk, dtype=jnp.int32))
    inv_freq = 10000.0 ** (-jnp.arange(half, dtype=jnp.float32) / half)
    angles = inv_freq[:, None] * pos_all.astype(jnp.float32)[None, :]
    whole = lambda a: pl.BlockSpec(a.shape, lambda i, *_: (0, 0), pipeline_mode=pl.Buffered(1))
    wq = w_uq.T
    wk = w_ukv[:, :NOPE_DIM]
    wv = w_ukv[:, NOPE_DIM:].T
    lane_blk = lambda r: pl.BlockSpec((r, blk), lambda i, *_: (0, i))
    return pl.pallas_call(
        functools.partial(attn_kernel, blk=blk, n_blk=n_blk),
        name="attention",
        out_shape=jax.ShapeDtypeStruct((tok, VALUE_DIM), jnp.bfloat16),
        grid_spec=pltpu.PrefetchScalarGridSpec(
            num_scalar_prefetch=2,
            grid=(n_blk,),
            in_specs=[
                pl.BlockSpec((blk, cq_all.shape[1]), lambda i, *_: (i, 0)),
                whole(kv_all), whole(wq), whole(wk), whole(wv),
                lane_blk(half), lane_blk(half), lane_blk(1), lane_blk(1),
            ],
            out_specs=pl.BlockSpec((blk, VALUE_DIM), lambda i, *_: (i, 0)),
            scratch_shapes=[
                pltpu.VMEM((tok, 2 * NOPE_DIM), jnp.bfloat16),
                pltpu.VMEM((VALUE_DIM, tok), jnp.bfloat16),
                pltpu.VMEM((2 * NOPE_DIM, blk), jnp.bfloat16),
                pltpu.VMEM((VALUE_DIM, blk), jnp.float32),
            ],
        ),
        cost_estimate=pl.CostEstimate(flops=10_000_000_000, bytes_accessed=14_000_000, transcendentals=9_000_000),
        compiler_params=pltpu.CompilerParams(dimension_semantics=("arbitrary",), vmem_limit_bytes=48 << 20),
    )(lo, clear, cq_all, kv_all, wq, wk, wv, jnp.cos(angles), jnp.sin(angles), start[None, :], pos_all[None, :])


def ffn_kernel(y_ref, g_ref, *rest, dim, pad, sub, tile_n):
    n_wt = 10
    weights = rest[:n_wt]
    (out_ref, ybuf, wgu, wdn, hbuf, gubuf, part, far_l, far_r, in_l, in_r, far2_l, far2_r, in2_l, in2_r,
     w_sem, ag_send, ag_recv, rs_send, rs_recv) = rest[n_wt:]
    me = lax.axis_index("sp")
    core = lax.rem(me, CORES)
    x = lax.rem(me // CORES, RING)
    y = lax.rem(me // (CORES * RING), RING)
    z = me // (CORES * RING * RING)

    def device(yy, xx):
        return {"sp": ((z * RING + yy) * RING + xx) * CORES + core}

    x_up, x_dn = device(y, lax.rem(x + 1, RING)), device(y, lax.rem(x + RING - 1, RING))
    y_up, y_dn = device(lax.rem(y + 1, RING), x), device(lax.rem(y + RING - 1, RING), x)
    up1, dn1, up2, dn2 = (x_up, y_up), (x_dn, y_dn), (y_up, x_up), (y_dn, x_dn)

    barrier = pltpu.get_barrier_semaphore()
    for nb in (x_up, x_dn, y_up, y_dn):
        pl.semaphore_signal(barrier, inc=1, device_id=nb, device_id_type=pl.DeviceIdType.MESH)

    w_copies = []

    def fetch(src, dst):
        cp = pltpu.make_async_copy(src, dst, w_sem.at[len(w_copies)])
        cp.start()
        w_copies.append(cp)

    cut = weights[3].shape[0]
    for side in range(2):
        own, left, right, f0, f1 = weights[5 * side:5 * side + 5]
        for n, blk in enumerate((own, left, right)):
            r = (4 * side + n) * pad
            fetch(blk.at[0:pad], wgu.at[r:r + pad])
            fetch(blk.at[pad:2 * pad], wgu.at[8 * pad + r:8 * pad + r + pad])
            fetch(blk.at[2 * pad:], wdn.at[r:r + pad])
        r = (4 * side + 3) * pad
        fetch(f0.at[0:pad], wgu.at[r:r + pad])
        fetch(f0.at[pad:cut], wgu.at[8 * pad + r:8 * pad + r + cut - pad])
        fetch(f1.at[0:2 * pad - cut], wgu.at[8 * pad + r + cut - pad:8 * pad + r + pad])
        fetch(f1.at[2 * pad - cut:], wdn.at[r:r + pad])

    for h in range(2):
        ybuf[h, 0] = y_ref[h * sub:(h + 1) * sub, :]
    pl.semaphore_wait(barrier, 4)

    cols = (slice(0, dim // 2), slice(dim // 2, dim))
    ag_copies = {}
    ag_n = [0]

    def ag_send_to(h, src_slot, dst_slot, dev, col=None):
        c = slice(None) if col is None else cols[col]
        key = (h, dst_slot, col)
        rsem = dst_slot if col != 1 else RING * RING
        cp = pltpu.make_async_remote_copy(
            src_ref=ybuf.at[h, src_slot, :, c], dst_ref=ybuf.at[h, dst_slot, :, c],
            send_sem=ag_send.at[ag_n[0]], recv_sem=ag_recv.at[h, rsem],
            device_id=dev, device_id_type=pl.DeviceIdType.MESH)
        ag_n[0] += 1
        cp.start()
        ag_copies[key] = cp

    far = 2
    for h in range(2):
        ag_send_to(h, 0, 3 * RING, up1[h])
        ag_send_to(h, 0, 1 * RING, dn1[h])
    for h in range(2):
        ag_send_to(h, 0, 3, up2[h])
        ag_send_to(h, 0, 1, dn2[h])
    for h in range(2):
        ag_copies[(h, 3 * RING, None)].wait_recv()
        ag_send_to(h, 3 * RING, far * RING, up1[h], 0)
        ag_copies[(h, 1 * RING, None)].wait_recv()
        ag_send_to(h, 1 * RING, far * RING, dn1[h], 1)
        for d1 in (3, 1):
            ag_send_to(h, d1 * RING, d1 * RING + 3, up2[h])
            ag_send_to(h, d1 * RING, d1 * RING + 1, dn2[h])
    for h in range(2):
        ag_copies[(h, far * RING, 0)].wait_recv()
        ag_copies[(h, far * RING, 1)].wait_recv()
        ag_send_to(h, far * RING, far * RING + 3, up2[h])
        ag_send_to(h, far * RING, far * RING + 1, dn2[h])
    for d1, d2, dev in ((0, 3, up2), (3, 3, up2), (1, 1, dn2), (2, 1, dn2)):
        for h in range(2):
            ag_copies[(h, d1 * RING + d2, None)].wait_recv()
            ag_send_to(h, d1 * RING + d2, d1 * RING + far, dev[h])
    for d1, d2 in ((0, 1), (3, 1), (1, 3), (2, 3), (0, 2), (3, 2), (1, 2), (2, 2)):
        for h in range(2):
            ag_copies[(h, d1 * RING + d2, None)].wait_recv()

    for cp in w_copies:
        cp.wait()

    rows = 2 * RING * sub
    nt = (((1,), (1,)), ((), ()))
    ff_pad = 8 * pad

    def compute(d1):
        for h in range(2):
            for d2 in range(RING):
                v = ybuf[h, d1 * RING + d2].astype(jnp.float32)
                mean_sq = jnp.mean(v * v, axis=-1, keepdims=True)
                r = (h * RING + d2) * sub
                hbuf[r:r + sub, :] = (v * lax.rsqrt(mean_sq + 1e-6) * g_ref[...].astype(jnp.float32)).astype(jnp.bfloat16)
        n_gu = gubuf.shape[1] // tile_n

        @pl.loop(0, n_gu)
        def _(j):
            c = pl.ds(pl.multiple_of(j * tile_n, tile_n), tile_n)
            gubuf[:, c] = lax.dot_general(hbuf[...], wgu[c, :], nt, preferred_element_type=jnp.float32)

        gate = gubuf[:, :ff_pad]
        act = (gate * jax.nn.sigmoid(gate) * gubuf[:, ff_pad:]).astype(jnp.bfloat16)
        wide = dim // 7 if dim % (7 * 128) == 0 else dim
        for j in range(dim // wide):
            c = slice(j * wide, (j + 1) * wide)
            res = jnp.dot(act, wdn[:, c], preferred_element_type=jnp.float32)
            for h in range(2):
                for d2 in range(RING):
                    r = (h * RING + d2) * sub
                    part[h, d1 * RING + d2, :, c] = res[r:r + sub]

    rs_copies = {}
    rs_n = [0]

    def rs_send_to(key, src, dst, dev):
        cp = pltpu.make_async_remote_copy(
            src_ref=src, dst_ref=dst, send_sem=rs_send.at[rs_n[0]], recv_sem=rs_recv.at[rs_n[0]],
            device_id=dev, device_id_type=pl.DeviceIdType.MESH)
        rs_n[0] += 1
        cp.start()
        rs_copies[key] = cp

    order = (2, 1, 3, 0)
    compute(far)
    for d2 in order:
        for h in range(2):
            rs_send_to(("fl", h, d2), part.at[h, far * RING + d2, :, cols[0]], far_l.at[h, d2], up1[h])
            rs_send_to(("fr", h, d2), part.at[h, far * RING + d2, :, cols[1]], far_r.at[h, d2], dn1[h])
    compute(1)
    compute(3)
    for d2 in order:
        for h in range(2):
            rs_copies[("fl", h, d2)].wait_recv()
            part[h, RING + d2, :, cols[0]] += far_l[h, d2]
            rs_send_to(("il", h, d2), part.at[h, RING + d2], in_l.at[h, d2], up1[h])
            rs_copies[("fr", h, d2)].wait_recv()
            part[h, 3 * RING + d2, :, cols[1]] += far_r[h, d2]
            rs_send_to(("ir", h, d2), part.at[h, 3 * RING + d2], in_r.at[h, d2], dn1[h])
    compute(0)

    def first_sum(h, d2):
        rs_copies[("il", h, d2)].wait_recv()
        rs_copies[("ir", h, d2)].wait_recv()
        part[h, d2] = part[h, d2] + in_l[h, d2] + in_r[h, d2]

    for h in range(2):
        first_sum(h, 2)
        rs_send_to(("gl", h), part.at[h, 2, :, cols[0]], far2_l.at[h], up2[h])
        rs_send_to(("gr", h), part.at[h, 2, :, cols[1]], far2_r.at[h], dn2[h])
    for h in range(2):
        first_sum(h, 1)
        rs_copies[("gl", h)].wait_recv()
        part[h, 1, :, cols[0]] += far2_l[h]
        rs_send_to(("jl", h), part.at[h, 1], in2_l.at[h], up2[h])
        first_sum(h, 3)
        rs_copies[("gr", h)].wait_recv()
        part[h, 3, :, cols[1]] += far2_r[h]
        rs_send_to(("jr", h), part.at[h, 3], in2_r.at[h], dn2[h])
    for h in range(2):
        first_sum(h, 0)
        rs_copies[("jl", h)].wait_recv()
        rs_copies[("jr", h)].wait_recv()
        total = part[h, 0] + in2_l[h] + in2_r[h]
        out_ref[h * sub:(h + 1) * sub, :] = (ybuf[h, 0].astype(jnp.float32) + total).astype(jnp.bfloat16)
    for cp in list(ag_copies.values()) + list(rs_copies.values()):
        cp.wait_send()


def ffn(y_own, g_ffn, weights, pad):
    rows, dim = y_own.shape
    sub = rows // 2
    chunk = 2 * RING * sub
    f32, bf16 = jnp.float32, jnp.bfloat16
    vm = pl.BlockSpec(memory_space=pltpu.VMEM)
    hbm = pl.BlockSpec(memory_space=pl.ANY)
    half = dim // 2
    return pl.pallas_call(
        functools.partial(ffn_kernel, dim=dim, pad=pad, sub=sub, tile_n=256 if (16 * pad) % 256 == 0 else 16 * pad),
        name="ffn",
        out_shape=jax.ShapeDtypeStruct((rows, dim), bf16),
        in_specs=[vm, vm] + [hbm] * 10,
        out_specs=vm,
        scratch_shapes=[
            pltpu.VMEM((2, RING * RING, sub, dim), bf16),
            pltpu.VMEM((16 * pad, dim), bf16),
            pltpu.VMEM((8 * pad, dim), bf16),
            pltpu.VMEM((chunk, dim), bf16),
            pltpu.VMEM((chunk, 16 * pad), f32),
            pltpu.VMEM((2, RING * RING, sub, dim), f32),
            pltpu.VMEM((2, RING, sub, half), f32),
            pltpu.VMEM((2, RING, sub, half), f32),
            pltpu.VMEM((2, RING, sub, dim), f32),
            pltpu.VMEM((2, RING, sub, dim), f32),
            pltpu.VMEM((2, sub, half), f32),
            pltpu.VMEM((2, sub, half), f32),
            pltpu.VMEM((2, sub, dim), f32),
            pltpu.VMEM((2, sub, dim), f32),
            pltpu.SemaphoreType.DMA((26,)),
            pltpu.SemaphoreType.DMA((32,)),
            pltpu.SemaphoreType.DMA((2, RING * RING + 1)),
            pltpu.SemaphoreType.DMA((40,)),
            pltpu.SemaphoreType.DMA((40,)),
        ],
        cost_estimate=pl.CostEstimate(flops=7_000_000_000, bytes_accessed=14_000_000, transcendentals=0),
        compiler_params=pltpu.CompilerParams(collective_id=1, has_side_effects=True, vmem_limit_bytes=56 << 20),
    )(y_own, g_ffn[None, :], *weights)


def gather_weights(w_gate, w_up, w_down, group_size):
    cols = w_down.shape[0]
    pad = -(-cols // 16) * 16
    wide = lambda w: jnp.pad(w, ((0, pad - cols), (0, 0)))
    own = jnp.concatenate([wide(w_gate.T), wide(w_up.T), wide(w_down)], axis=0)
    cut = pad + (pad // 2) // 16 * 16
    plane = RING * RING * CORES
    up = [(d, (d + plane) % group_size) for d in range(group_size)]
    down = [(d, (d - plane) % group_size) for d in range(group_size)]
    swap = [(d, d ^ 1) for d in range(group_size)]
    left = lax.ppermute(own, 'sp', up)
    right = lax.ppermute(own, 'sp', down)
    far0 = lax.ppermute(left[:cut], 'sp', up)
    far1 = lax.ppermute(right[cut:], 'sp', down)
    mine = [own, left, right, far0, far1]
    return mine + [lax.ppermute(w, 'sp', swap) for w in mine], pad


def solution(mesh):
    group_size = mesh.shape['sp']
    tok_spec = P(('dp', 'sp'), None)
    row_spec = P(('dp', 'sp'))
    full_spec = P()
    col_spec = P(None, 'sp')

    def device_fn(x_blk, seg_blk, pos_blk, w_dq, g_q, w_uq, w_dkv, g_kv, w_ukv, w_o, g_ffn, w_gate, w_up, w_down):
        blk_len = x_blk.shape[0]
        tok_total = blk_len * group_size
        weights, pad = gather_weights(w_gate, w_up, w_down, group_size)

        q_lin = jnp.dot(x_blk, w_dq, preferred_element_type=jnp.float32)
        c_q = rms_norm(q_lin, g_q).astype(jnp.bfloat16)
        kv_lin = jnp.dot(x_blk, w_dkv, preferred_element_type=jnp.float32)
        c_kv = rms_norm(kv_lin[:, :KV_LATENT], g_kv).astype(jnp.bfloat16)
        k_rope = apply_rope(kv_lin[:, KV_LATENT:], pos_blk).astype(jnp.bfloat16)
        pos_hi = (pos_blk // 64).astype(jnp.bfloat16)[:, None]
        pos_lo = (pos_blk % 64).astype(jnp.bfloat16)[:, None]
        spare = jnp.zeros((blk_len, NOPE_DIM - ROPE_DIM - 2), jnp.bfloat16)
        kv_blk = jnp.concatenate([c_kv, k_rope, pos_hi, pos_lo, spare], axis=1)
        cq_all = lax.all_gather(c_q, 'sp', axis=0, tiled=True)
        kv_all = lax.all_gather(kv_blk, 'sp', axis=0, tiled=True)
        at = KV_LATENT + ROPE_DIM
        pos_all = kv_all[:, at].astype(jnp.int32) * 64 + kv_all[:, at + 1].astype(jnp.int32)

        o_loc = attention(cq_all, kv_all, w_uq, w_ukv, pos_all, min(512, tok_total))
        o_tok = lax.all_to_all(o_loc, 'sp', 0, 1, tiled=True)
        y_att = jnp.dot(o_tok, w_o, preferred_element_type=jnp.float32).astype(jnp.bfloat16)
        return ffn(y_att, g_ffn, weights, pad)

    return jax.shard_map(device_fn, mesh=mesh, in_specs=(tok_spec, row_spec, row_spec, full_spec, full_spec, col_spec, full_spec, full_spec, col_spec, full_spec, full_spec, col_spec, col_spec, P('sp', None)), out_specs=tok_spec, check_vma=False)
```

```python
import functools

import jax
import jax.numpy as jnp
from jax import lax
from jax.experimental import pallas as pl
from jax.experimental.pallas import tpu as pltpu
from jax.sharding import PartitionSpec as P

NOPE_DIM = 128
ROPE_DIM = 64
VALUE_DIM = 128
KV_LATENT = 512
QK_DIM = NOPE_DIM + ROPE_DIM
KV_DIM = NOPE_DIM + VALUE_DIM
SCORE_SCALE = QK_DIM ** -0.5
LOG2E = 1.4426950408889634
MASKED = -0.7 * 3.4028234663852886e38

RING = 4
CORES = 2


def rms_norm(vec_in, gain_vec):
    mean_sq = jnp.mean(vec_in * vec_in, axis=-1, keepdims=True)
    return vec_in * lax.rsqrt(mean_sq + 1e-6) * gain_vec.astype(jnp.float32)


def rope_angles(positions):
    half_dim = ROPE_DIM // 2
    inv_freq = 10000.0 ** (-jnp.arange(half_dim, dtype=jnp.float32) / half_dim)
    return positions.astype(jnp.float32)[..., None] * inv_freq


def apply_rope(vec_in, positions):
    half_dim = ROPE_DIM // 2
    angles = rope_angles(positions)
    cosine = jnp.cos(angles)
    sine_v = jnp.sin(angles)
    lo_half = vec_in[..., :half_dim]
    hi_half = vec_in[..., half_dim:]
    return jnp.concatenate([lo_half * cosine - hi_half * sine_v, hi_half * cosine + lo_half * sine_v], axis=-1)


GATHER_ORDERS = (("x", "y", "z"), ("y", "z", "x"), ("z", "x", "y"))


def gather_kernel_copies(bufs, coord, send_sem, recv_sem, fill_own):
    core = coord["core"]

    def device(**moved):
        c = {**coord, **moved}
        return {"sp": ((c["z"] * RING + c["y"]) * RING + c["x"]) * CORES + c["core"]}

    def step(axis, by):
        return lax.rem(coord[axis] + (by % RING), RING)

    up = {a: device(**{a: step(a, 1)}) for a in "xyz"}
    down = {a: device(**{a: step(a, -1)}) for a in "xyz"}
    partner = device(core=1 - core)

    barrier = pltpu.get_barrier_semaphore()
    for nb in list(up.values()) + list(down.values()) + [partner]:
        pl.semaphore_signal(barrier, inc=1, device_id=nb, device_id_type=pl.DeviceIdType.MESH)
    fill_own()
    pl.semaphore_wait(barrier, 7)

    copies = [{} for _ in bufs]

    def send(p, key, dev, rows=None, **at):
        idx = tuple(slice(None) if at.get(a, 0) is None else at.get(a, coord[a]) for a in "zyx") + (core,)
        if rows is not None:
            idx = idx + (rows,)
        n = len(copies[p])
        cp = pltpu.make_async_remote_copy(
            src_ref=bufs[p].at[idx], dst_ref=bufs[p].at[idx], send_sem=send_sem.at[p, n], recv_sem=recv_sem.at[p, n],
            device_id=dev, device_id_type=pl.DeviceIdType.MESH)
        cp.start()
        copies[p][key] = cp

    n_p = len(bufs)
    pieces = range(n_p)
    half = bufs[0].shape[4] // 2
    order = (0, -1, 1, 2)

    def along_b(p, da):
        a, b, _ = GATHER_ORDERS[p]
        send(p, ("b+", da), up[b], **{a: step(a, da)})
        send(p, ("b-", da), down[b], **{a: step(a, da)})

    def along_d(p, db):
        a, b, d = GATHER_ORDERS[p]
        send(p, ("d+", db), up[d], **{a: None, b: step(b, db)})
        send(p, ("d-", db), down[d], **{a: None, b: step(b, db)})
        to_partner(p, db, 0)

    def to_partner(p, db, dd):
        a, b, d = GATHER_ORDERS[p]
        send(p, ("p", db, dd), partner, **{a: None, b: step(b, db), d: step(d, dd)})

    for p in pieces:
        a, b, d = GATHER_ORDERS[p]
        send(p, "a+", up[a])
        send(p, "a-", down[a])
        along_b(p, 0)
    for p in pieces:
        a, b, d = GATHER_ORDERS[p]
        copies[p]["a+"].wait_recv()
        send(p, "af+", up[a], rows=slice(0, half), **{a: step(a, -1)})
        copies[p]["a-"].wait_recv()
        send(p, "af-", down[a], rows=slice(half, 2 * half), **{a: step(a, 1)})
        along_b(p, -1)
        along_b(p, 1)
    for p in pieces:
        copies[p]["af+"].wait_recv()
        copies[p]["af-"].wait_recv()
        along_b(p, 2)
        along_d(p, 0)
    for p in pieces:
        a, b, d = GATHER_ORDERS[p]
        for da in (0, -1):
            copies[p][("b+", da)].wait_recv()
            send(p, ("bf+", da), up[b], **{a: step(a, da), b: step(b, -1)})
        for da in (1, 2):
            copies[p][("b-", da)].wait_recv()
            send(p, ("bf-", da), down[b], **{a: step(a, da), b: step(b, 1)})
        for da in (1, 2):
            copies[p][("b+", da)].wait_recv()
        along_d(p, -1)
        for da in (0, -1):
            copies[p][("b-", da)].wait_recv()
        along_d(p, 1)
    for p in pieces:
        for da in (0, -1):
            copies[p][("bf+", da)].wait_recv()
        for da in (1, 2):
            copies[p][("bf-", da)].wait_recv()
        along_d(p, 2)
    for db in order:
        for p in pieces:
            a, b, d = GATHER_ORDERS[p]
            copies[p][("d+", db)].wait_recv()
            if db in (0, -1):
                send(p, ("df+", db), up[d], **{a: None, b: step(b, db), d: step(d, -1)})
            to_partner(p, db, -1)
            copies[p][("d-", db)].wait_recv()
            if db in (1, 2):
                send(p, ("df-", db), down[d], **{a: None, b: step(b, db), d: step(d, 1)})
            to_partner(p, db, 1)
    for db in order:
        for p in pieces:
            copies[p][("df+" if db in (0, -1) else "df-", db)].wait_recv()
            to_partner(p, db, 2)
    for p in pieces:
        for db in order:
            for dd in order:
                copies[p][("p", db, dd)].wait_recv()
    for p in pieces:
        for cp in copies[p].values():
            cp.wait_send()


GATHER_COPIES = 44


def my_coord():
    me = lax.axis_index("sp")
    return {
        "core": lax.rem(me, CORES),
        "x": lax.rem(me // CORES, RING),
        "y": lax.rem(me // (CORES * RING), RING),
        "z": me // (CORES * RING * RING),
    }


def qkv_kernel(kv_own, qa_own, qb_own, wqa, wqb, wk, wv, inv_freq, pick, qt_out, k_out, vt_out, pos_out,
               kv_buf, qa_buf, qb_buf, send_sem, recv_sem, *, blk):
    coord = my_coord()

    def fill_own():
        at = (coord["z"], coord["y"], coord["x"], coord["core"])
        kv_buf[at] = kv_own[...]
        qa_buf[at] = qa_own[...]
        qb_buf[at] = qb_own[...]

    gather_kernel_copies((kv_buf, qa_buf, qb_buf), coord, send_sem, recv_sem, fill_own)

    nt = (((1,), (1,)), ((), ()))
    half = ROPE_DIM // 2
    tok_blk = kv_own.shape[0]
    shards = blk // tok_blk
    lines = shards // (RING * CORES)
    n_blk = qt_out.shape[1] // blk
    per_z = RING // lines
    f32, bf16 = jnp.float32, jnp.bfloat16

    @pl.loop(0, n_blk)
    def _(n):
        at = (n // per_z, pl.ds(lax.rem(n, per_z) * lines, lines))
        flat = lambda v: v.reshape(blk, v.shape[-1])
        lat = flat(kv_buf[at])
        qa = flat(qa_buf[at])
        qb = flat(qb_buf[at])
        tail = qb[:, qb.shape[1] - NOPE_DIM:]
        rows = pl.ds(pl.multiple_of(n * blk, blk), blk)
        k_out[rows, :NOPE_DIM] = jnp.dot(lat, wk[...], preferred_element_type=f32).astype(bf16)
        k_out[rows, NOPE_DIM:] = tail
        vt_out[:, rows] = lax.dot_general(wv[...], lat, nt, preferred_element_type=f32).astype(bf16)
        pos = lax.dot_general(pick[...], tail, nt, preferred_element_type=f32)
        pos_out[:, rows] = pos
        angle = inv_freq[...] * pos[0:1]
        cosine, sine = jnp.cos(angle), jnp.sin(angle)
        qt = lax.dot_general(wqa[...], qa, nt, preferred_element_type=f32)
        qt += lax.dot_general(wqb[...], qb[:, :qb.shape[1] - NOPE_DIM], nt, preferred_element_type=f32)
        lo, hi = qt[NOPE_DIM:NOPE_DIM + half], qt[NOPE_DIM + half:]
        qt_out[:NOPE_DIM, rows] = qt[:NOPE_DIM].astype(bf16)
        qt_out[NOPE_DIM:NOPE_DIM + half, rows] = (lo * cosine - hi * sine).astype(bf16)
        qt_out[NOPE_DIM + half:QK_DIM, rows] = (hi * cosine + lo * sine).astype(bf16)
        qt_out[QK_DIM:, rows] = jnp.zeros((2 * NOPE_DIM - QK_DIM, blk), bf16)


def gather_qkv(kv_own, qa_own, qb_own, w_uq, w_ukv, tok_total, blk):
    rows = kv_own.shape[0]
    f32, bf16 = jnp.float32, jnp.bfloat16
    half = ROPE_DIM // 2
    inv_freq = 10000.0 ** (-jnp.arange(half, dtype=f32) / half)
    lane = jnp.arange(NOPE_DIM)[None, :]
    pick = jnp.where(jnp.arange(8)[:, None] == 0, jnp.where(lane == ROPE_DIM, 64.0, jnp.where(lane == ROPE_DIM + 1, 1.0, 0.0)), 0.0).astype(bf16)
    vm = pl.BlockSpec(memory_space=pltpu.VMEM)
    wa = qa_own.shape[1]
    buf = lambda own: pltpu.VMEM((RING, RING, RING, CORES, rows, own.shape[1]), bf16)
    return pl.pallas_call(
        functools.partial(qkv_kernel, blk=blk),
        name="gather_qkv",
        out_shape=(
            jax.ShapeDtypeStruct((2 * NOPE_DIM, tok_total), bf16),
            jax.ShapeDtypeStruct((tok_total, 2 * NOPE_DIM), bf16),
            jax.ShapeDtypeStruct((VALUE_DIM, tok_total), bf16),
            jax.ShapeDtypeStruct((8, tok_total), f32),
        ),
        in_specs=[vm] * 9,
        out_specs=(vm,) * 4,
        scratch_shapes=[
            buf(kv_own), buf(qa_own), buf(qb_own),
            pltpu.SemaphoreType.DMA((3, GATHER_COPIES)),
            pltpu.SemaphoreType.DMA((3, GATHER_COPIES)),
        ],
        cost_estimate=pl.CostEstimate(flops=4_000_000_000, bytes_accessed=6_000_000, transcendentals=0),
        compiler_params=pltpu.CompilerParams(collective_id=2, has_side_effects=True, vmem_limit_bytes=40 << 20),
    )(kv_own, qa_own, qb_own, w_uq[:wa].T, w_uq[wa:].T, w_ukv[:, :NOPE_DIM], w_ukv[:, NOPE_DIM:].T, inv_freq[:, None], pick)


def attn_kernel(lo_ref, clear_ref, q_ref, k_ref, v_ref, start_ref, pos_ref, o_ref, acc_ref, *, blk):
    i = pl.program_id(0)
    acc_ref[...] = jnp.zeros_like(acc_ref)

    def block(masked, kb, carry):
        m_old, l_old = carry
        rows = pl.ds(pl.multiple_of(kb * blk, blk), blk)
        s = jnp.dot(k_ref[rows, :], q_ref[...], preferred_element_type=jnp.float32)
        if masked:
            key = kb * blk + lax.broadcasted_iota(jnp.int32, s.shape, 0)
            back = key - start_ref[...]
            s = jnp.where((back >= 0) & (back <= pos_ref[...]), s, MASKED)
        m_new = jnp.maximum(m_old, jnp.max(s, axis=0, keepdims=True))
        p = jnp.exp2((s - m_new) * (SCORE_SCALE * LOG2E))
        alpha = jnp.exp2((m_old - m_new) * (SCORE_SCALE * LOG2E))
        l_new = l_old * alpha + jnp.sum(p, axis=0, keepdims=True)
        acc_ref[...] = acc_ref[...] * alpha + jnp.dot(v_ref[:, rows], p.astype(jnp.bfloat16), preferred_element_type=jnp.float32)
        return m_new, l_new

    carry = (jnp.full((1, blk), MASKED, jnp.float32), jnp.zeros((1, blk), jnp.float32))
    lo = lo_ref[i]
    clear = clear_ref[i]
    carry = lax.fori_loop(lo, clear, functools.partial(block, True), carry)
    carry = lax.fori_loop(clear, i, functools.partial(block, False), carry)
    _, total = block(True, i, carry)
    o_ref[...] = (acc_ref[...] / total).T.astype(jnp.bfloat16)


def attention(qt, k, vt, pos_row, blk):
    tok = k.shape[0]
    n_blk = tok // blk
    pos_all = pos_row.astype(jnp.int32)
    start = jnp.arange(tok, dtype=jnp.int32)[None, :] - pos_all
    lo = start[0, ::blk] // blk
    clear = jnp.clip((start[0, blk - 1::blk] + blk - 1) // blk, lo, jnp.arange(n_blk, dtype=jnp.int32))
    whole = lambda a: pl.BlockSpec(a.shape, lambda i, *_: (0, 0), pipeline_mode=pl.Buffered(1))
    lane_blk = lambda r: pl.BlockSpec((r, blk), lambda i, *_: (0, i))
    return pl.pallas_call(
        functools.partial(attn_kernel, blk=blk),
        name="attention",
        out_shape=jax.ShapeDtypeStruct((tok, VALUE_DIM), jnp.bfloat16),
        grid_spec=pltpu.PrefetchScalarGridSpec(
            num_scalar_prefetch=2,
            grid=(n_blk,),
            in_specs=[lane_blk(2 * NOPE_DIM), whole(k), whole(vt), lane_blk(1), lane_blk(1)],
            out_specs=pl.BlockSpec((blk, VALUE_DIM), lambda i, *_: (i, 0)),
            scratch_shapes=[pltpu.VMEM((VALUE_DIM, blk), jnp.float32)],
        ),
        cost_estimate=pl.CostEstimate(flops=10_000_000_000, bytes_accessed=8_000_000, transcendentals=9_000_000),
        compiler_params=pltpu.CompilerParams(dimension_semantics=("arbitrary",), vmem_limit_bytes=40 << 20),
    )(lo, clear, qt, k, vt, start, pos_all)


def ffn_kernel(y_ref, g_ref, *rest, dim, pad, sub, tile_n):
    n_wt = 10
    weights = rest[:n_wt]
    (out_ref, ybuf, wgu, wdn, hbuf, gubuf, part, far_l, far_r, in_l, in_r, far2_l, far2_r, in2_l, in2_r,
     w_sem, ag_send, ag_recv, rs_send, rs_recv) = rest[n_wt:]
    me = lax.axis_index("sp")
    core = lax.rem(me, CORES)
    x = lax.rem(me // CORES, RING)
    y = lax.rem(me // (CORES * RING), RING)
    z = me // (CORES * RING * RING)

    def device(yy, xx):
        return {"sp": ((z * RING + yy) * RING + xx) * CORES + core}

    x_up, x_dn = device(y, lax.rem(x + 1, RING)), device(y, lax.rem(x + RING - 1, RING))
    y_up, y_dn = device(lax.rem(y + 1, RING), x), device(lax.rem(y + RING - 1, RING), x)
    up1, dn1, up2, dn2 = (x_up, y_up), (x_dn, y_dn), (y_up, x_up), (y_dn, x_dn)

    barrier = pltpu.get_barrier_semaphore()
    for nb in (x_up, x_dn, y_up, y_dn):
        pl.semaphore_signal(barrier, inc=1, device_id=nb, device_id_type=pl.DeviceIdType.MESH)

    w_copies = []

    def fetch(src, dst):
        cp = pltpu.make_async_copy(src, dst, w_sem.at[len(w_copies)])
        cp.start()
        w_copies.append(cp)

    cut = weights[3].shape[0]
    for side in range(2):
        own, left, right, f0, f1 = weights[5 * side:5 * side + 5]
        for n, blk in enumerate((own, left, right)):
            r = (4 * side + n) * pad
            fetch(blk.at[0:pad], wgu.at[r:r + pad])
            fetch(blk.at[pad:2 * pad], wgu.at[8 * pad + r:8 * pad + r + pad])
            fetch(blk.at[2 * pad:], wdn.at[r:r + pad])
        r = (4 * side + 3) * pad
        fetch(f0.at[0:pad], wgu.at[r:r + pad])
        fetch(f0.at[pad:cut], wgu.at[8 * pad + r:8 * pad + r + cut - pad])
        fetch(f1.at[0:2 * pad - cut], wgu.at[8 * pad + r + cut - pad:8 * pad + r + pad])
        fetch(f1.at[2 * pad - cut:], wdn.at[r:r + pad])

    for h in range(2):
        ybuf[h, 0] = y_ref[h * sub:(h + 1) * sub, :]
    pl.semaphore_wait(barrier, 4)

    cols = (slice(0, dim // 2), slice(dim // 2, dim))
    ag_copies = {}
    ag_n = [0]

    def ag_send_to(h, src_slot, dst_slot, dev, col=None):
        c = slice(None) if col is None else cols[col]
        key = (h, dst_slot, col)
        rsem = dst_slot if col != 1 else RING * RING
        cp = pltpu.make_async_remote_copy(
            src_ref=ybuf.at[h, src_slot, :, c], dst_ref=ybuf.at[h, dst_slot, :, c],
            send_sem=ag_send.at[ag_n[0]], recv_sem=ag_recv.at[h, rsem],
            device_id=dev, device_id_type=pl.DeviceIdType.MESH)
        ag_n[0] += 1
        cp.start()
        ag_copies[key] = cp

    far = 2
    for h in range(2):
        ag_send_to(h, 0, 3 * RING, up1[h])
        ag_send_to(h, 0, 1 * RING, dn1[h])
    for h in range(2):
        ag_send_to(h, 0, 3, up2[h])
        ag_send_to(h, 0, 1, dn2[h])
    for h in range(2):
        ag_copies[(h, 3 * RING, None)].wait_recv()
        ag_send_to(h, 3 * RING, far * RING, up1[h], 0)
        ag_copies[(h, 1 * RING, None)].wait_recv()
        ag_send_to(h, 1 * RING, far * RING, dn1[h], 1)
        for d1 in (3, 1):
            ag_send_to(h, d1 * RING, d1 * RING + 3, up2[h])
            ag_send_to(h, d1 * RING, d1 * RING + 1, dn2[h])
    for h in range(2):
        ag_copies[(h, far * RING, 0)].wait_recv()
        ag_copies[(h, far * RING, 1)].wait_recv()
        ag_send_to(h, far * RING, far * RING + 3, up2[h])
        ag_send_to(h, far * RING, far * RING + 1, dn2[h])
    for d1, d2, dev in ((0, 3, up2), (3, 3, up2), (1, 1, dn2), (2, 1, dn2)):
        for h in range(2):
            ag_copies[(h, d1 * RING + d2, None)].wait_recv()
            ag_send_to(h, d1 * RING + d2, d1 * RING + far, dev[h])
    for d1, d2 in ((0, 1), (3, 1), (1, 3), (2, 3), (0, 2), (3, 2), (1, 2), (2, 2)):
        for h in range(2):
            ag_copies[(h, d1 * RING + d2, None)].wait_recv()

    for cp in w_copies:
        cp.wait()

    rows = 2 * RING * sub
    nt = (((1,), (1,)), ((), ()))
    ff_pad = 8 * pad

    def compute(d1):
        for h in range(2):
            for d2 in range(RING):
                v = ybuf[h, d1 * RING + d2].astype(jnp.float32)
                mean_sq = jnp.mean(v * v, axis=-1, keepdims=True)
                r = (h * RING + d2) * sub
                hbuf[r:r + sub, :] = (v * lax.rsqrt(mean_sq + 1e-6) * g_ref[...].astype(jnp.float32)).astype(jnp.bfloat16)
        n_gu = gubuf.shape[1] // tile_n

        @pl.loop(0, n_gu)
        def _(j):
            c = pl.ds(pl.multiple_of(j * tile_n, tile_n), tile_n)
            gubuf[:, c] = lax.dot_general(hbuf[...], wgu[c, :], nt, preferred_element_type=jnp.float32)

        gate = gubuf[:, :ff_pad]
        act = (gate * jax.nn.sigmoid(gate) * gubuf[:, ff_pad:]).astype(jnp.bfloat16)
        wide = dim // 7 if dim % (7 * 128) == 0 else dim
        for j in range(dim // wide):
            c = slice(j * wide, (j + 1) * wide)
            res = jnp.dot(act, wdn[:, c], preferred_element_type=jnp.float32)
            for h in range(2):
                for d2 in range(RING):
                    r = (h * RING + d2) * sub
                    part[h, d1 * RING + d2, :, c] = res[r:r + sub]

    rs_copies = {}
    rs_n = [0]

    def rs_send_to(key, src, dst, dev):
        cp = pltpu.make_async_remote_copy(
            src_ref=src, dst_ref=dst, send_sem=rs_send.at[rs_n[0]], recv_sem=rs_recv.at[rs_n[0]],
            device_id=dev, device_id_type=pl.DeviceIdType.MESH)
        rs_n[0] += 1
        cp.start()
        rs_copies[key] = cp

    order = (2, 1, 3, 0)
    compute(far)
    for d2 in order:
        for h in range(2):
            rs_send_to(("fl", h, d2), part.at[h, far * RING + d2, :, cols[0]], far_l.at[h, d2], up1[h])
            rs_send_to(("fr", h, d2), part.at[h, far * RING + d2, :, cols[1]], far_r.at[h, d2], dn1[h])
    compute(1)
    compute(3)
    for d2 in order:
        for h in range(2):
            rs_copies[("fl", h, d2)].wait_recv()
            part[h, RING + d2, :, cols[0]] += far_l[h, d2]
            rs_send_to(("il", h, d2), part.at[h, RING + d2], in_l.at[h, d2], up1[h])
            rs_copies[("fr", h, d2)].wait_recv()
            part[h, 3 * RING + d2, :, cols[1]] += far_r[h, d2]
            rs_send_to(("ir", h, d2), part.at[h, 3 * RING + d2], in_r.at[h, d2], dn1[h])
    compute(0)

    def first_sum(h, d2):
        rs_copies[("il", h, d2)].wait_recv()
        rs_copies[("ir", h, d2)].wait_recv()
        part[h, d2] = part[h, d2] + in_l[h, d2] + in_r[h, d2]

    for h in range(2):
        first_sum(h, 2)
        rs_send_to(("gl", h), part.at[h, 2, :, cols[0]], far2_l.at[h], up2[h])
        rs_send_to(("gr", h), part.at[h, 2, :, cols[1]], far2_r.at[h], dn2[h])
    for h in range(2):
        first_sum(h, 1)
        rs_copies[("gl", h)].wait_recv()
        part[h, 1, :, cols[0]] += far2_l[h]
        rs_send_to(("jl", h), part.at[h, 1], in2_l.at[h], up2[h])
        first_sum(h, 3)
        rs_copies[("gr", h)].wait_recv()
        part[h, 3, :, cols[1]] += far2_r[h]
        rs_send_to(("jr", h), part.at[h, 3], in2_r.at[h], dn2[h])
    for h in range(2):
        first_sum(h, 0)
        rs_copies[("jl", h)].wait_recv()
        rs_copies[("jr", h)].wait_recv()
        total = part[h, 0] + in2_l[h] + in2_r[h]
        out_ref[h * sub:(h + 1) * sub, :] = (ybuf[h, 0].astype(jnp.float32) + total).astype(jnp.bfloat16)
    for cp in list(ag_copies.values()) + list(rs_copies.values()):
        cp.wait_send()


def ffn(y_own, g_ffn, weights, pad):
    rows, dim = y_own.shape
    sub = rows // 2
    chunk = 2 * RING * sub
    f32, bf16 = jnp.float32, jnp.bfloat16
    vm = pl.BlockSpec(memory_space=pltpu.VMEM)
    hbm = pl.BlockSpec(memory_space=pl.ANY)
    half = dim // 2
    return pl.pallas_call(
        functools.partial(ffn_kernel, dim=dim, pad=pad, sub=sub, tile_n=256 if (16 * pad) % 256 == 0 else 16 * pad),
        name="ffn",
        out_shape=jax.ShapeDtypeStruct((rows, dim), bf16),
        in_specs=[vm, vm] + [hbm] * 10,
        out_specs=vm,
        scratch_shapes=[
            pltpu.VMEM((2, RING * RING, sub, dim), bf16),
            pltpu.VMEM((16 * pad, dim), bf16),
            pltpu.VMEM((8 * pad, dim), bf16),
            pltpu.VMEM((chunk, dim), bf16),
            pltpu.VMEM((chunk, 16 * pad), f32),
            pltpu.VMEM((2, RING * RING, sub, dim), f32),
            pltpu.VMEM((2, RING, sub, half), f32),
            pltpu.VMEM((2, RING, sub, half), f32),
            pltpu.VMEM((2, RING, sub, dim), f32),
            pltpu.VMEM((2, RING, sub, dim), f32),
            pltpu.VMEM((2, sub, half), f32),
            pltpu.VMEM((2, sub, half), f32),
            pltpu.VMEM((2, sub, dim), f32),
            pltpu.VMEM((2, sub, dim), f32),
            pltpu.SemaphoreType.DMA((26,)),
            pltpu.SemaphoreType.DMA((32,)),
            pltpu.SemaphoreType.DMA((2, RING * RING + 1)),
            pltpu.SemaphoreType.DMA((40,)),
            pltpu.SemaphoreType.DMA((40,)),
        ],
        cost_estimate=pl.CostEstimate(flops=7_000_000_000, bytes_accessed=14_000_000, transcendentals=0),
        compiler_params=pltpu.CompilerParams(collective_id=1, has_side_effects=True, vmem_limit_bytes=56 << 20),
    )(y_own, g_ffn[None, :], *weights)


def gather_weights(w_gate, w_up, w_down, group_size):
    cols = w_down.shape[0]
    pad = -(-cols // 16) * 16
    wide = lambda w: jnp.pad(w, ((0, pad - cols), (0, 0)))
    own = jnp.concatenate([wide(w_gate.T), wide(w_up.T), wide(w_down)], axis=0)
    cut = pad + (pad // 2) // 16 * 16
    plane = RING * RING * CORES
    up = [(d, (d + plane) % group_size) for d in range(group_size)]
    down = [(d, (d - plane) % group_size) for d in range(group_size)]
    swap = [(d, d ^ 1) for d in range(group_size)]
    left = lax.ppermute(own, 'sp', up)
    right = lax.ppermute(own, 'sp', down)
    far0 = lax.ppermute(left[:cut], 'sp', up)
    far1 = lax.ppermute(right[cut:], 'sp', down)
    mine = [own, left, right, far0, far1]
    return mine + [lax.ppermute(w, 'sp', swap) for w in mine], pad


def solution(mesh):
    group_size = mesh.shape['sp']
    tok_spec = P(('dp', 'sp'), None)
    row_spec = P(('dp', 'sp'))
    full_spec = P()
    col_spec = P(None, 'sp')

    def device_fn(x_blk, seg_blk, pos_blk, w_dq, g_q, w_uq, w_dkv, g_kv, w_ukv, w_o, g_ffn, w_gate, w_up, w_down):
        blk_len = x_blk.shape[0]
        tok_total = blk_len * group_size
        weights, pad = gather_weights(w_gate, w_up, w_down, group_size)

        q_lin = jnp.dot(x_blk, w_dq, preferred_element_type=jnp.float32)
        c_q = rms_norm(q_lin, g_q).astype(jnp.bfloat16)
        kv_lin = jnp.dot(x_blk, w_dkv, preferred_element_type=jnp.float32)
        c_kv = rms_norm(kv_lin[:, :KV_LATENT], g_kv).astype(jnp.bfloat16)
        k_rope = apply_rope(kv_lin[:, KV_LATENT:], pos_blk).astype(jnp.bfloat16)
        pos_hi = (pos_blk // 64).astype(jnp.bfloat16)[:, None]
        pos_lo = (pos_blk % 64).astype(jnp.bfloat16)[:, None]
        spare = jnp.zeros((blk_len, NOPE_DIM - ROPE_DIM - 2), jnp.bfloat16)
        split = KV_LATENT
        q_rest = jnp.concatenate([c_q[:, split:], k_rope, pos_hi, pos_lo, spare], axis=1)
        blk = min(512, tok_total)
        qt, k, vt, pos_rows = gather_qkv(c_kv, c_q[:, :split], q_rest, w_uq, w_ukv, tok_total, blk)
        o_loc = attention(qt, k, vt, pos_rows[:1], blk)
        o_tok = lax.all_to_all(o_loc, 'sp', 0, 1, tiled=True)
        y_att = jnp.dot(o_tok, w_o, preferred_element_type=jnp.float32).astype(jnp.bfloat16)
        return ffn(y_att, g_ffn, weights, pad)

    return jax.shard_map(device_fn, mesh=mesh, in_specs=(tok_spec, row_spec, row_spec, full_spec, full_spec, col_spec, full_spec, full_spec, col_spec, full_spec, full_spec, col_spec, col_spec, P('sp', None)), out_specs=tok_spec, check_vma=False)
```

```python
import functools

import jax
import jax.numpy as jnp
from jax import lax
from jax.experimental import pallas as pl
from jax.experimental.pallas import tpu as pltpu
from jax.sharding import PartitionSpec as P

NOPE_DIM = 128
ROPE_DIM = 64
VALUE_DIM = 128
KV_LATENT = 512
QK_DIM = NOPE_DIM + ROPE_DIM
KV_DIM = NOPE_DIM + VALUE_DIM
SCORE_SCALE = QK_DIM ** -0.5
LOG2E = 1.4426950408889634
MASKED = -0.7 * 3.4028234663852886e38

RING = 4
CORES = 2


def rms_norm(vec_in, gain_vec):
    mean_sq = jnp.mean(vec_in * vec_in, axis=-1, keepdims=True)
    return vec_in * lax.rsqrt(mean_sq + 1e-6) * gain_vec.astype(jnp.float32)


def rope_angles(positions):
    half_dim = ROPE_DIM // 2
    inv_freq = 10000.0 ** (-jnp.arange(half_dim, dtype=jnp.float32) / half_dim)
    return positions.astype(jnp.float32)[..., None] * inv_freq


def apply_rope(vec_in, positions):
    half_dim = ROPE_DIM // 2
    angles = rope_angles(positions)
    cosine = jnp.cos(angles)
    sine_v = jnp.sin(angles)
    lo_half = vec_in[..., :half_dim]
    hi_half = vec_in[..., half_dim:]
    return jnp.concatenate([lo_half * cosine - hi_half * sine_v, hi_half * cosine + lo_half * sine_v], axis=-1)


GATHER_ORDERS = (("x", "y", "z"), ("y", "z", "x"), ("z", "x", "y"))


def gather_kernel_copies(bufs, coord, send_sem, recv_sem, fill_own):
    core = coord["core"]

    def device(**moved):
        c = {**coord, **moved}
        return {"sp": ((c["z"] * RING + c["y"]) * RING + c["x"]) * CORES + c["core"]}

    def step(axis, by):
        return lax.rem(coord[axis] + (by % RING), RING)

    up = {a: device(**{a: step(a, 1)}) for a in "xyz"}
    down = {a: device(**{a: step(a, -1)}) for a in "xyz"}
    partner = device(core=1 - core)

    barrier = pltpu.get_barrier_semaphore()
    for nb in list(up.values()) + list(down.values()) + [partner]:
        pl.semaphore_signal(barrier, inc=1, device_id=nb, device_id_type=pl.DeviceIdType.MESH)
    fill_own()
    pl.semaphore_wait(barrier, 7)

    copies = [{} for _ in bufs]

    def send(p, key, dev, rows=None, **at):
        idx = tuple(slice(None) if at.get(a, 0) is None else at.get(a, coord[a]) for a in "zyx") + (core,)
        if rows is not None:
            idx = idx + (rows,)
        n = len(copies[p])
        cp = pltpu.make_async_remote_copy(
            src_ref=bufs[p].at[idx], dst_ref=bufs[p].at[idx], send_sem=send_sem.at[p, n], recv_sem=recv_sem.at[p, n],
            device_id=dev, device_id_type=pl.DeviceIdType.MESH)
        cp.start()
        copies[p][key] = cp

    n_p = len(bufs)
    pieces = range(n_p)
    half = bufs[0].shape[4] // 2
    order = (0, -1, 1, 2)

    def along_b(p, da):
        a, b, _ = GATHER_ORDERS[p]
        send(p, ("b+", da), up[b], **{a: step(a, da)})
        send(p, ("b-", da), down[b], **{a: step(a, da)})

    def along_d(p, db):
        a, b, d = GATHER_ORDERS[p]
        send(p, ("d+", db), up[d], **{a: None, b: step(b, db)})
        send(p, ("d-", db), down[d], **{a: None, b: step(b, db)})
        to_partner(p, db, 0)

    def to_partner(p, db, dd):
        a, b, d = GATHER_ORDERS[p]
        send(p, ("p", db, dd), partner, **{a: None, b: step(b, db), d: step(d, dd)})

    for p in pieces:
        a, b, d = GATHER_ORDERS[p]
        send(p, "a+", up[a])
        send(p, "a-", down[a])
        along_b(p, 0)
    for p in pieces:
        a, b, d = GATHER_ORDERS[p]
        copies[p]["a+"].wait_recv()
        send(p, "af+", up[a], rows=slice(0, half), **{a: step(a, -1)})
        copies[p]["a-"].wait_recv()
        send(p, "af-", down[a], rows=slice(half, 2 * half), **{a: step(a, 1)})
        along_b(p, -1)
        along_b(p, 1)
    for p in pieces:
        copies[p]["af+"].wait_recv()
        copies[p]["af-"].wait_recv()
        along_b(p, 2)
        along_d(p, 0)
    for p in pieces:
        a, b, d = GATHER_ORDERS[p]
        for da in (0, -1):
            copies[p][("b+", da)].wait_recv()
            send(p, ("bf+", da), up[b], **{a: step(a, da), b: step(b, -1)})
        for da in (1, 2):
            copies[p][("b-", da)].wait_recv()
            send(p, ("bf-", da), down[b], **{a: step(a, da), b: step(b, 1)})
        for da in (1, 2):
            copies[p][("b+", da)].wait_recv()
        along_d(p, -1)
        for da in (0, -1):
            copies[p][("b-", da)].wait_recv()
        along_d(p, 1)
    for p in pieces:
        for da in (0, -1):
            copies[p][("bf+", da)].wait_recv()
        for da in (1, 2):
            copies[p][("bf-", da)].wait_recv()
        along_d(p, 2)
    for db in order:
        for p in pieces:
            a, b, d = GATHER_ORDERS[p]
            copies[p][("d+", db)].wait_recv()
            if db in (0, -1):
                send(p, ("df+", db), up[d], **{a: None, b: step(b, db), d: step(d, -1)})
            to_partner(p, db, -1)
            copies[p][("d-", db)].wait_recv()
            if db in (1, 2):
                send(p, ("df-", db), down[d], **{a: None, b: step(b, db), d: step(d, 1)})
            to_partner(p, db, 1)
    for db in order:
        for p in pieces:
            copies[p][("df+" if db in (0, -1) else "df-", db)].wait_recv()
            to_partner(p, db, 2)
    for p in pieces:
        for db in order:
            for dd in order:
                copies[p][("p", db, dd)].wait_recv()
    for p in pieces:
        for cp in copies[p].values():
            cp.wait_send()


GATHER_COPIES = 44


def my_coord():
    me = lax.axis_index("sp")
    return {
        "core": lax.rem(me, CORES),
        "x": lax.rem(me // CORES, RING),
        "y": lax.rem(me // (CORES * RING), RING),
        "z": me // (CORES * RING * RING),
    }


def qkv_kernel(kv_own, qa_own, qb_own, wqa, wqb, wk, wv, inv_freq, pick, qt_out, k_out, vt_out, pos_out,
               kv_buf, qa_buf, qb_buf, send_sem, recv_sem, *, blk):
    coord = my_coord()

    def fill_own():
        at = (coord["z"], coord["y"], coord["x"], coord["core"])
        kv_buf[at] = kv_own[...]
        qa_buf[at] = qa_own[...]
        qb_buf[at] = qb_own[...]

    gather_kernel_copies((kv_buf, qa_buf, qb_buf), coord, send_sem, recv_sem, fill_own)

    nt = (((1,), (1,)), ((), ()))
    half = ROPE_DIM // 2
    tok_blk = kv_own.shape[0]
    shards = blk // tok_blk
    lines = shards // (RING * CORES)
    n_blk = qt_out.shape[1] // blk
    per_z = RING // lines
    f32, bf16 = jnp.float32, jnp.bfloat16

    @pl.loop(0, n_blk)
    def _(n):
        at = (n // per_z, pl.ds(lax.rem(n, per_z) * lines, lines))
        flat = lambda v: v.reshape(blk, v.shape[-1])
        lat = flat(kv_buf[at])
        qa = flat(qa_buf[at])
        qb = flat(qb_buf[at])
        tail = qb[:, qb.shape[1] - NOPE_DIM:]
        rows = pl.ds(pl.multiple_of(n * blk, blk), blk)
        k_out[rows, :NOPE_DIM] = jnp.dot(lat, wk[...], preferred_element_type=f32).astype(bf16)
        k_out[rows, NOPE_DIM:] = tail
        vt_out[:, rows] = lax.dot_general(wv[...], lat, nt, preferred_element_type=f32).astype(bf16)
        pos = lax.dot_general(pick[...], tail, nt, preferred_element_type=f32)
        pos_out[:, rows] = pos
        angle = inv_freq[...] * pos[0:1]
        cosine, sine = jnp.cos(angle), jnp.sin(angle)
        qt = lax.dot_general(wqa[...], qa, nt, preferred_element_type=f32)
        qt += lax.dot_general(wqb[...], qb[:, :qb.shape[1] - NOPE_DIM], nt, preferred_element_type=f32)
        lo, hi = qt[NOPE_DIM:NOPE_DIM + half], qt[NOPE_DIM + half:]
        qt_out[:NOPE_DIM, rows] = qt[:NOPE_DIM].astype(bf16)
        qt_out[NOPE_DIM:NOPE_DIM + half, rows] = (lo * cosine - hi * sine).astype(bf16)
        qt_out[NOPE_DIM + half:QK_DIM, rows] = (hi * cosine + lo * sine).astype(bf16)
        qt_out[QK_DIM:, rows] = jnp.zeros((2 * NOPE_DIM - QK_DIM, blk), bf16)


def gather_qkv(kv_own, qa_own, qb_own, w_uq, w_ukv, tok_total, blk):
    rows = kv_own.shape[0]
    f32, bf16 = jnp.float32, jnp.bfloat16
    half = ROPE_DIM // 2
    inv_freq = 10000.0 ** (-jnp.arange(half, dtype=f32) / half)
    lane = jnp.arange(NOPE_DIM)[None, :]
    pick = jnp.where(jnp.arange(8)[:, None] == 0, jnp.where(lane == ROPE_DIM, 64.0, jnp.where(lane == ROPE_DIM + 1, 1.0, 0.0)), 0.0).astype(bf16)
    vm = pl.BlockSpec(memory_space=pltpu.VMEM)
    wa = qa_own.shape[1]
    buf = lambda own: pltpu.VMEM((RING, RING, RING, CORES, rows, own.shape[1]), bf16)
    return pl.pallas_call(
        functools.partial(qkv_kernel, blk=blk),
        name="gather_qkv",
        out_shape=(
            jax.ShapeDtypeStruct((2 * NOPE_DIM, tok_total), bf16),
            jax.ShapeDtypeStruct((tok_total, 2 * NOPE_DIM), bf16),
            jax.ShapeDtypeStruct((VALUE_DIM, tok_total), bf16),
            jax.ShapeDtypeStruct((8, tok_total), f32),
        ),
        in_specs=[vm] * 9,
        out_specs=(vm,) * 4,
        scratch_shapes=[
            buf(kv_own), buf(qa_own), buf(qb_own),
            pltpu.SemaphoreType.DMA((3, GATHER_COPIES)),
            pltpu.SemaphoreType.DMA((3, GATHER_COPIES)),
        ],
        cost_estimate=pl.CostEstimate(flops=4_000_000_000, bytes_accessed=6_000_000, transcendentals=0),
        compiler_params=pltpu.CompilerParams(collective_id=2, has_side_effects=True, vmem_limit_bytes=40 << 20),
    )(kv_own, qa_own, qb_own, w_uq[:wa].T, w_uq[wa:].T, w_ukv[:, :NOPE_DIM], w_ukv[:, NOPE_DIM:].T, inv_freq[:, None], pick)


def attn_kernel(lo_ref, clear_ref, q_ref, k_ref, v_ref, start_ref, pos_ref, o_ref, acc_ref, *, blk):
    i = pl.program_id(0)
    acc_ref[...] = jnp.zeros_like(acc_ref)

    def block(masked, kb, carry):
        m_old, l_old = carry
        rows = pl.ds(pl.multiple_of(kb * blk, blk), blk)
        s = jnp.dot(k_ref[rows, :], q_ref[...], preferred_element_type=jnp.float32)
        if masked:
            key = kb * blk + lax.broadcasted_iota(jnp.int32, s.shape, 0)
            back = key - start_ref[...]
            s = jnp.where((back >= 0) & (back <= pos_ref[...]), s, MASKED)
        m_new = jnp.maximum(m_old, jnp.max(s, axis=0, keepdims=True))
        p = jnp.exp2((s - m_new) * (SCORE_SCALE * LOG2E))
        alpha = jnp.exp2((m_old - m_new) * (SCORE_SCALE * LOG2E))
        l_new = l_old * alpha + jnp.sum(p, axis=0, keepdims=True)
        acc_ref[...] = acc_ref[...] * alpha + jnp.dot(v_ref[:, rows], p.astype(jnp.bfloat16), preferred_element_type=jnp.float32)
        return m_new, l_new

    carry = (jnp.full((1, blk), MASKED, jnp.float32), jnp.zeros((1, blk), jnp.float32))
    lo = lo_ref[i]
    clear = clear_ref[i]
    carry = lax.fori_loop(lo, clear, functools.partial(block, True), carry)
    carry = lax.fori_loop(clear, i, functools.partial(block, False), carry)
    _, total = block(True, i, carry)
    o_ref[...] = (acc_ref[...] / total).T.astype(jnp.bfloat16)


def attention(qt, k, vt, pos_row, blk):
    tok = k.shape[0]
    n_blk = tok // blk
    pos_all = pos_row.astype(jnp.int32)
    start = jnp.arange(tok, dtype=jnp.int32)[None, :] - pos_all
    lo = start[0, ::blk] // blk
    clear = jnp.clip((start[0, blk - 1::blk] + blk - 1) // blk, lo, jnp.arange(n_blk, dtype=jnp.int32))
    whole = lambda a: pl.BlockSpec(a.shape, lambda i, *_: (0, 0), pipeline_mode=pl.Buffered(1))
    lane_blk = lambda r: pl.BlockSpec((r, blk), lambda i, *_: (0, i))
    return pl.pallas_call(
        functools.partial(attn_kernel, blk=blk),
        name="attention",
        out_shape=jax.ShapeDtypeStruct((tok, VALUE_DIM), jnp.bfloat16),
        grid_spec=pltpu.PrefetchScalarGridSpec(
            num_scalar_prefetch=2,
            grid=(n_blk,),
            in_specs=[lane_blk(2 * NOPE_DIM), whole(k), whole(vt), lane_blk(1), lane_blk(1)],
            out_specs=pl.BlockSpec((blk, VALUE_DIM), lambda i, *_: (i, 0)),
            scratch_shapes=[pltpu.VMEM((VALUE_DIM, blk), jnp.float32)],
        ),
        cost_estimate=pl.CostEstimate(flops=10_000_000_000, bytes_accessed=8_000_000, transcendentals=9_000_000),
        compiler_params=pltpu.CompilerParams(dimension_semantics=("arbitrary",), vmem_limit_bytes=40 << 20),
    )(lo, clear, qt, k, vt, start, pos_all)


def project_kernel(o_ref, wo_ref, y_ref, o_all, w_buf, acc, y_half, y_in, w_sem, send_sem, recv_sem, fwd_send, fwd_recv,
                   y_sem, *, n_buf):
    coord = my_coord()
    core, x, y, z = (coord[a] for a in ("core", "x", "y", "z"))
    lines = RING * RING
    chip_rows, head = o_all.shape[3], o_all.shape[4]
    w_rows, cols = w_buf.shape[1], w_buf.shape[2]
    mesh_id = pl.DeviceIdType.MESH

    def line_of(k):
        return lax.rem(z + k // RING, RING) * RING + lax.rem(y + lax.rem(k, RING), RING)

    def w_copy(k):
        rows = pl.ds(pl.multiple_of(line_of(k) * w_rows, w_rows), w_rows)
        side = pl.ds(pl.multiple_of(core * cols, 128), cols)
        slot = lax.rem(k, n_buf)
        return pltpu.make_async_copy(wo_ref.at[rows, side], w_buf.at[slot], w_sem.at[slot])

    @pl.loop(0, n_buf)
    def _(k):
        w_copy(k).start()

    def chip(k, dx):
        zz = lax.rem(z + RING - k // RING, RING)
        yy = lax.rem(y + RING - lax.rem(k, RING), RING)
        xx = lax.rem(x + RING - dx, RING)
        return (zz * RING + yy) * RING + xx

    me_chip = (z * RING + y) * RING + x
    partner = {"sp": me_chip * CORES + 1 - core}
    n_chips = lines * RING

    barrier = pltpu.get_barrier_semaphore()
    pl.semaphore_signal(barrier, inc=1, device_id=partner, device_id_type=mesh_id)

    @pl.loop(1, n_chips)
    def _(n):
        to = {"sp": chip(n // RING, lax.rem(n, RING)) * CORES + core}
        pl.semaphore_signal(barrier, inc=1, device_id=to, device_id_type=mesh_id)

    my_line = z * RING + y
    o_all[my_line, x, core] = o_ref[pl.ds(pl.multiple_of(me_chip * chip_rows, chip_rows), chip_rows), :]
    pl.semaphore_wait(barrier, n_chips)

    def head_copy(n):
        to = chip(n // RING, lax.rem(n, RING))
        rows = pl.ds(pl.multiple_of(to * chip_rows, chip_rows), chip_rows)
        return pltpu.make_async_remote_copy(
            src_ref=o_ref.at[rows, :], dst_ref=o_all.at[my_line, x, core], send_sem=send_sem, recv_sem=recv_sem.at[n // RING],
            device_id={"sp": to * CORES + core}, device_id_type=mesh_id)

    @pl.loop(1, n_chips)
    def _(n):
        head_copy(n).start()

    def forward(k):
        at = o_all.at[line_of(k), :, core]
        return pltpu.make_async_remote_copy(
            src_ref=at, dst_ref=at, send_sem=fwd_send.at[k], recv_sem=fwd_recv.at[k], device_id=partner, device_id_type=mesh_id)

    def arrive(k, n_heads):
        at = o_all.at[line_of(k), pl.ds(0, n_heads), core]
        pltpu.make_async_copy(at, at, recv_sem.at[k]).wait()
        forward(k).start()

    acc[...] = jnp.zeros_like(acc)
    arrive(0, RING - 1)

    @pl.loop(0, lines)
    def _(k):
        @pl.when(k + 1 < lines)
        def _():
            arrive(k + 1, RING)

        forward(k).wait_recv()
        w_copy(k).wait()
        line = line_of(k)
        lhs = jnp.concatenate([o_all[line, i, j] for i in range(RING) for j in range(CORES)], axis=1)
        acc[...] += jnp.dot(lhs, w_buf[lax.rem(k, n_buf)], preferred_element_type=jnp.float32)

        @pl.when(k + n_buf < lines)
        def _():
            w_copy(k + n_buf).start()

    own_rows = chip_rows // CORES
    y_half[...] = acc[...].astype(jnp.bfloat16)
    swap = pltpu.make_async_remote_copy(
        src_ref=y_half.at[pl.ds(pl.multiple_of((1 - core) * own_rows, own_rows), own_rows), :], dst_ref=y_in,
        send_sem=y_sem.at[0], recv_sem=y_sem.at[1], device_id=partner, device_id_type=mesh_id)
    swap.start()
    mine = y_half[pl.ds(pl.multiple_of(core * own_rows, own_rows), own_rows), :]
    swap.wait_recv()
    other = y_in[...]
    y_ref[:, :cols] = jnp.where(core == 0, mine, other)
    y_ref[:, cols:] = jnp.where(core == 0, other, mine)
    swap.wait_send()

    @pl.loop(0, lines)
    def _(k):
        forward(k).wait_send()

    everything = o_ref.at[pl.ds(0, (n_chips - 1) * chip_rows), :]
    pltpu.make_async_copy(everything, everything, send_sem).wait()


def project(o_loc, w_o, group_size, n_buf):
    tok, head = o_loc.shape
    own_rows = tok // group_size
    dim = w_o.shape[1]
    lines = RING * RING
    w_rows = w_o.shape[0] // lines
    f32, bf16 = jnp.float32, jnp.bfloat16
    vm = pl.BlockSpec(memory_space=pltpu.VMEM)
    return pl.pallas_call(
        functools.partial(project_kernel, n_buf=n_buf),
        name="project",
        out_shape=jax.ShapeDtypeStruct((own_rows, dim), bf16),
        in_specs=[vm, pl.BlockSpec(memory_space=pl.ANY)],
        out_specs=vm,
        scratch_shapes=[
            pltpu.VMEM((lines, RING, CORES, CORES * own_rows, head), bf16),
            pltpu.VMEM((n_buf, w_rows, dim // CORES), bf16),
            pltpu.VMEM((CORES * own_rows, dim // CORES), f32),
            pltpu.VMEM((CORES * own_rows, dim // CORES), bf16),
            pltpu.VMEM((own_rows, dim // CORES), bf16),
            pltpu.SemaphoreType.DMA((n_buf,)),
            pltpu.SemaphoreType.DMA,
            pltpu.SemaphoreType.DMA((lines,)),
            pltpu.SemaphoreType.DMA((lines,)),
            pltpu.SemaphoreType.DMA((lines,)),
            pltpu.SemaphoreType.DMA((2,)),
        ],
        cost_estimate=pl.CostEstimate(flops=4_000_000_000, bytes_accessed=60_000_000, transcendentals=0),
        compiler_params=pltpu.CompilerParams(collective_id=3, has_side_effects=True, vmem_limit_bytes=56 << 20),
    )(o_loc, w_o)


def ffn_kernel(y_ref, g_ref, *rest, dim, pad, sub, tile_n):
    n_wt = 10
    weights = rest[:n_wt]
    (out_ref, ybuf, wgu, wdn, hbuf, gubuf, part, far_l, far_r, in_l, in_r, far2_l, far2_r, in2_l, in2_r,
     w_sem, ag_send, ag_recv, rs_send, rs_recv) = rest[n_wt:]
    me = lax.axis_index("sp")
    core = lax.rem(me, CORES)
    x = lax.rem(me // CORES, RING)
    y = lax.rem(me // (CORES * RING), RING)
    z = me // (CORES * RING * RING)

    def device(yy, xx):
        return {"sp": ((z * RING + yy) * RING + xx) * CORES + core}

    x_up, x_dn = device(y, lax.rem(x + 1, RING)), device(y, lax.rem(x + RING - 1, RING))
    y_up, y_dn = device(lax.rem(y + 1, RING), x), device(lax.rem(y + RING - 1, RING), x)
    up1, dn1, up2, dn2 = (x_up, y_up), (x_dn, y_dn), (y_up, x_up), (y_dn, x_dn)

    barrier = pltpu.get_barrier_semaphore()
    for nb in (x_up, x_dn, y_up, y_dn):
        pl.semaphore_signal(barrier, inc=1, device_id=nb, device_id_type=pl.DeviceIdType.MESH)

    w_copies = []

    def fetch(src, dst):
        cp = pltpu.make_async_copy(src, dst, w_sem.at[len(w_copies)])
        cp.start()
        w_copies.append(cp)

    cut = weights[3].shape[0]
    for side in range(2):
        own, left, right, f0, f1 = weights[5 * side:5 * side + 5]
        for n, blk in enumerate((own, left, right)):
            r = (4 * side + n) * pad
            fetch(blk.at[0:pad], wgu.at[r:r + pad])
            fetch(blk.at[pad:2 * pad], wgu.at[8 * pad + r:8 * pad + r + pad])
            fetch(blk.at[2 * pad:], wdn.at[r:r + pad])
        r = (4 * side + 3) * pad
        fetch(f0.at[0:pad], wgu.at[r:r + pad])
        fetch(f0.at[pad:cut], wgu.at[8 * pad + r:8 * pad + r + cut - pad])
        fetch(f1.at[0:2 * pad - cut], wgu.at[8 * pad + r + cut - pad:8 * pad + r + pad])
        fetch(f1.at[2 * pad - cut:], wdn.at[r:r + pad])

    for h in range(2):
        ybuf[h, 0] = y_ref[h * sub:(h + 1) * sub, :]
    pl.semaphore_wait(barrier, 4)

    cols = (slice(0, dim // 2), slice(dim // 2, dim))
    ag_copies = {}
    ag_n = [0]

    def ag_send_to(h, src_slot, dst_slot, dev, col=None):
        c = slice(None) if col is None else cols[col]
        key = (h, dst_slot, col)
        rsem = dst_slot if col != 1 else RING * RING
        cp = pltpu.make_async_remote_copy(
            src_ref=ybuf.at[h, src_slot, :, c], dst_ref=ybuf.at[h, dst_slot, :, c],
            send_sem=ag_send.at[ag_n[0]], recv_sem=ag_recv.at[h, rsem],
            device_id=dev, device_id_type=pl.DeviceIdType.MESH)
        ag_n[0] += 1
        cp.start()
        ag_copies[key] = cp

    far = 2
    for h in range(2):
        ag_send_to(h, 0, 3 * RING, up1[h])
        ag_send_to(h, 0, 1 * RING, dn1[h])
    for h in range(2):
        ag_send_to(h, 0, 3, up2[h])
        ag_send_to(h, 0, 1, dn2[h])
    for h in range(2):
        ag_copies[(h, 3 * RING, None)].wait_recv()
        ag_send_to(h, 3 * RING, far * RING, up1[h], 0)
        ag_copies[(h, 1 * RING, None)].wait_recv()
        ag_send_to(h, 1 * RING, far * RING, dn1[h], 1)
        for d1 in (3, 1):
            ag_send_to(h, d1 * RING, d1 * RING + 3, up2[h])
            ag_send_to(h, d1 * RING, d1 * RING + 1, dn2[h])
    for h in range(2):
        ag_copies[(h, far * RING, 0)].wait_recv()
        ag_copies[(h, far * RING, 1)].wait_recv()
        ag_send_to(h, far * RING, far * RING + 3, up2[h])
        ag_send_to(h, far * RING, far * RING + 1, dn2[h])
    for d1, d2, dev in ((0, 3, up2), (3, 3, up2), (1, 1, dn2), (2, 1, dn2)):
        for h in range(2):
            ag_copies[(h, d1 * RING + d2, None)].wait_recv()
            ag_send_to(h, d1 * RING + d2, d1 * RING + far, dev[h])
    for d1, d2 in ((0, 1), (3, 1), (1, 3), (2, 3), (0, 2), (3, 2), (1, 2), (2, 2)):
        for h in range(2):
            ag_copies[(h, d1 * RING + d2, None)].wait_recv()

    for cp in w_copies:
        cp.wait()

    rows = 2 * RING * sub
    nt = (((1,), (1,)), ((), ()))
    ff_pad = 8 * pad

    def compute(d1):
        for h in range(2):
            for d2 in range(RING):
                v = ybuf[h, d1 * RING + d2].astype(jnp.float32)
                mean_sq = jnp.mean(v * v, axis=-1, keepdims=True)
                r = (h * RING + d2) * sub
                hbuf[r:r + sub, :] = (v * lax.rsqrt(mean_sq + 1e-6) * g_ref[...].astype(jnp.float32)).astype(jnp.bfloat16)
        n_gu = gubuf.shape[1] // tile_n

        @pl.loop(0, n_gu)
        def _(j):
            c = pl.ds(pl.multiple_of(j * tile_n, tile_n), tile_n)
            gubuf[:, c] = lax.dot_general(hbuf[...], wgu[c, :], nt, preferred_element_type=jnp.float32)

        gate = gubuf[:, :ff_pad]
        act = (gate * jax.nn.sigmoid(gate) * gubuf[:, ff_pad:]).astype(jnp.bfloat16)
        wide = dim // 7 if dim % (7 * 128) == 0 else dim
        for j in range(dim // wide):
            c = slice(j * wide, (j + 1) * wide)
            res = jnp.dot(act, wdn[:, c], preferred_element_type=jnp.float32)
            for h in range(2):
                for d2 in range(RING):
                    r = (h * RING + d2) * sub
                    part[h, d1 * RING + d2, :, c] = res[r:r + sub]

    rs_copies = {}
    rs_n = [0]

    def rs_send_to(key, src, dst, dev):
        cp = pltpu.make_async_remote_copy(
            src_ref=src, dst_ref=dst, send_sem=rs_send.at[rs_n[0]], recv_sem=rs_recv.at[rs_n[0]],
            device_id=dev, device_id_type=pl.DeviceIdType.MESH)
        rs_n[0] += 1
        cp.start()
        rs_copies[key] = cp

    order = (2, 1, 3, 0)
    compute(far)
    for d2 in order:
        for h in range(2):
            rs_send_to(("fl", h, d2), part.at[h, far * RING + d2, :, cols[0]], far_l.at[h, d2], up1[h])
            rs_send_to(("fr", h, d2), part.at[h, far * RING + d2, :, cols[1]], far_r.at[h, d2], dn1[h])
    compute(1)
    compute(3)
    for d2 in order:
        for h in range(2):
            rs_copies[("fl", h, d2)].wait_recv()
            part[h, RING + d2, :, cols[0]] += far_l[h, d2]
            rs_send_to(("il", h, d2), part.at[h, RING + d2], in_l.at[h, d2], up1[h])
            rs_copies[("fr", h, d2)].wait_recv()
            part[h, 3 * RING + d2, :, cols[1]] += far_r[h, d2]
            rs_send_to(("ir", h, d2), part.at[h, 3 * RING + d2], in_r.at[h, d2], dn1[h])
    compute(0)

    def first_sum(h, d2):
        rs_copies[("il", h, d2)].wait_recv()
        rs_copies[("ir", h, d2)].wait_recv()
        part[h, d2] = part[h, d2] + in_l[h, d2] + in_r[h, d2]

    for h in range(2):
        first_sum(h, 2)
        rs_send_to(("gl", h), part.at[h, 2, :, cols[0]], far2_l.at[h], up2[h])
        rs_send_to(("gr", h), part.at[h, 2, :, cols[1]], far2_r.at[h], dn2[h])
    for h in range(2):
        first_sum(h, 1)
        rs_copies[("gl", h)].wait_recv()
        part[h, 1, :, cols[0]] += far2_l[h]
        rs_send_to(("jl", h), part.at[h, 1], in2_l.at[h], up2[h])
        first_sum(h, 3)
        rs_copies[("gr", h)].wait_recv()
        part[h, 3, :, cols[1]] += far2_r[h]
        rs_send_to(("jr", h), part.at[h, 3], in2_r.at[h], dn2[h])
    for h in range(2):
        first_sum(h, 0)
        rs_copies[("jl", h)].wait_recv()
        rs_copies[("jr", h)].wait_recv()
        total = part[h, 0] + in2_l[h] + in2_r[h]
        out_ref[h * sub:(h + 1) * sub, :] = (ybuf[h, 0].astype(jnp.float32) + total).astype(jnp.bfloat16)
    for cp in list(ag_copies.values()) + list(rs_copies.values()):
        cp.wait_send()


def ffn(y_own, g_ffn, weights, pad):
    rows, dim = y_own.shape
    sub = rows // 2
    chunk = 2 * RING * sub
    f32, bf16 = jnp.float32, jnp.bfloat16
    vm = pl.BlockSpec(memory_space=pltpu.VMEM)
    hbm = pl.BlockSpec(memory_space=pl.ANY)
    half = dim // 2
    return pl.pallas_call(
        functools.partial(ffn_kernel, dim=dim, pad=pad, sub=sub, tile_n=256 if (16 * pad) % 256 == 0 else 16 * pad),
        name="ffn",
        out_shape=jax.ShapeDtypeStruct((rows, dim), bf16),
        in_specs=[vm, vm] + [hbm] * 10,
        out_specs=vm,
        scratch_shapes=[
            pltpu.VMEM((2, RING * RING, sub, dim), bf16),
            pltpu.VMEM((16 * pad, dim), bf16),
            pltpu.VMEM((8 * pad, dim), bf16),
            pltpu.VMEM((chunk, dim), bf16),
            pltpu.VMEM((chunk, 16 * pad), f32),
            pltpu.VMEM((2, RING * RING, sub, dim), f32),
            pltpu.VMEM((2, RING, sub, half), f32),
            pltpu.VMEM((2, RING, sub, half), f32),
            pltpu.VMEM((2, RING, sub, dim), f32),
            pltpu.VMEM((2, RING, sub, dim), f32),
            pltpu.VMEM((2, sub, half), f32),
            pltpu.VMEM((2, sub, half), f32),
            pltpu.VMEM((2, sub, dim), f32),
            pltpu.VMEM((2, sub, dim), f32),
            pltpu.SemaphoreType.DMA((26,)),
            pltpu.SemaphoreType.DMA((32,)),
            pltpu.SemaphoreType.DMA((2, RING * RING + 1)),
            pltpu.SemaphoreType.DMA((40,)),
            pltpu.SemaphoreType.DMA((40,)),
        ],
        cost_estimate=pl.CostEstimate(flops=7_000_000_000, bytes_accessed=14_000_000, transcendentals=0),
        compiler_params=pltpu.CompilerParams(collective_id=1, has_side_effects=True, vmem_limit_bytes=56 << 20),
    )(y_own, g_ffn[None, :], *weights)


def gather_weights(w_gate, w_up, w_down, group_size):
    cols = w_down.shape[0]
    pad = -(-cols // 16) * 16
    wide = lambda w: jnp.pad(w, ((0, pad - cols), (0, 0)))
    own = jnp.concatenate([wide(w_gate.T), wide(w_up.T), wide(w_down)], axis=0)
    cut = pad + (pad // 2) // 16 * 16
    plane = RING * RING * CORES
    up = [(d, (d + plane) % group_size) for d in range(group_size)]
    down = [(d, (d - plane) % group_size) for d in range(group_size)]
    swap = [(d, d ^ 1) for d in range(group_size)]
    left = lax.ppermute(own, 'sp', up)
    right = lax.ppermute(own, 'sp', down)
    far0 = lax.ppermute(left[:cut], 'sp', up)
    far1 = lax.ppermute(right[cut:], 'sp', down)
    mine = [own, left, right, far0, far1]
    return mine + [lax.ppermute(w, 'sp', swap) for w in mine], pad


def solution(mesh):
    group_size = mesh.shape['sp']
    tok_spec = P(('dp', 'sp'), None)
    row_spec = P(('dp', 'sp'))
    full_spec = P()
    col_spec = P(None, 'sp')

    def device_fn(x_blk, seg_blk, pos_blk, w_dq, g_q, w_uq, w_dkv, g_kv, w_ukv, w_o, g_ffn, w_gate, w_up, w_down):
        blk_len = x_blk.shape[0]
        tok_total = blk_len * group_size
        weights, pad = gather_weights(w_gate, w_up, w_down, group_size)

        q_lin = jnp.dot(x_blk, w_dq, preferred_element_type=jnp.float32)
        c_q = rms_norm(q_lin, g_q).astype(jnp.bfloat16)
        kv_lin = jnp.dot(x_blk, w_dkv, preferred_element_type=jnp.float32)
        c_kv = rms_norm(kv_lin[:, :KV_LATENT], g_kv).astype(jnp.bfloat16)
        k_rope = apply_rope(kv_lin[:, KV_LATENT:], pos_blk).astype(jnp.bfloat16)
        pos_hi = (pos_blk // 64).astype(jnp.bfloat16)[:, None]
        pos_lo = (pos_blk % 64).astype(jnp.bfloat16)[:, None]
        spare = jnp.zeros((blk_len, NOPE_DIM - ROPE_DIM - 2), jnp.bfloat16)
        split = KV_LATENT
        q_rest = jnp.concatenate([c_q[:, split:], k_rope, pos_hi, pos_lo, spare], axis=1)
        blk = min(512, tok_total)
        qt, k, vt, pos_rows = gather_qkv(c_kv, c_q[:, :split], q_rest, w_uq, w_ukv, tok_total, blk)
        o_loc = attention(qt, k, vt, pos_rows[:1], blk)
        y_att = project(o_loc, w_o, group_size, 12)
        return ffn(y_att, g_ffn, weights, pad)

    return jax.shard_map(device_fn, mesh=mesh, in_specs=(tok_spec, row_spec, row_spec, full_spec, full_spec, col_spec, full_spec, full_spec, col_spec, full_spec, full_spec, col_spec, col_spec, P('sp', None)), out_specs=tok_spec, check_vma=False)
```

```python
import functools

import jax
import jax.numpy as jnp
from jax import lax
from jax.experimental import pallas as pl
from jax.experimental.pallas import tpu as pltpu
from jax.sharding import PartitionSpec as P

NOPE_DIM = 128
ROPE_DIM = 64
VALUE_DIM = 128
KV_LATENT = 512
QK_DIM = NOPE_DIM + ROPE_DIM
KV_DIM = NOPE_DIM + VALUE_DIM
SCORE_SCALE = QK_DIM ** -0.5
LOG2E = 1.4426950408889634
MASKED = -0.7 * 3.4028234663852886e38

RING = 4
CORES = 2


def rms_norm(vec_in, gain_vec):
    mean_sq = jnp.mean(vec_in * vec_in, axis=-1, keepdims=True)
    return vec_in * lax.rsqrt(mean_sq + 1e-6) * gain_vec.astype(jnp.float32)


def rope_angles(positions):
    half_dim = ROPE_DIM // 2
    inv_freq = 10000.0 ** (-jnp.arange(half_dim, dtype=jnp.float32) / half_dim)
    return positions.astype(jnp.float32)[..., None] * inv_freq


def apply_rope(vec_in, positions):
    half_dim = ROPE_DIM // 2
    angles = rope_angles(positions)
    cosine = jnp.cos(angles)
    sine_v = jnp.sin(angles)
    lo_half = vec_in[..., :half_dim]
    hi_half = vec_in[..., half_dim:]
    return jnp.concatenate([lo_half * cosine - hi_half * sine_v, hi_half * cosine + lo_half * sine_v], axis=-1)


GATHER_ORDERS = (("x", "y", "z"), ("y", "z", "x"), ("z", "x", "y"))


def gather_kernel_copies(bufs, coord, send_sem, recv_sem, fill_own):
    core = coord["core"]

    def device(**moved):
        c = {**coord, **moved}
        return {"sp": ((c["z"] * RING + c["y"]) * RING + c["x"]) * CORES + c["core"]}

    def step(axis, by):
        return lax.rem(coord[axis] + (by % RING), RING)

    up = {a: device(**{a: step(a, 1)}) for a in "xyz"}
    down = {a: device(**{a: step(a, -1)}) for a in "xyz"}
    partner = device(core=1 - core)

    barrier = pltpu.get_barrier_semaphore()
    for nb in list(up.values()) + list(down.values()) + [partner]:
        pl.semaphore_signal(barrier, inc=1, device_id=nb, device_id_type=pl.DeviceIdType.MESH)
    fill_own()
    pl.semaphore_wait(barrier, 7)

    copies = [{} for _ in bufs]

    def send(p, key, dev, rows=None, **at):
        idx = tuple(slice(None) if at.get(a, 0) is None else at.get(a, coord[a]) for a in "zyx") + (core,)
        if rows is not None:
            idx = idx + (rows,)
        n = len(copies[p])
        cp = pltpu.make_async_remote_copy(
            src_ref=bufs[p].at[idx], dst_ref=bufs[p].at[idx], send_sem=send_sem.at[p, n], recv_sem=recv_sem.at[p, n],
            device_id=dev, device_id_type=pl.DeviceIdType.MESH)
        cp.start()
        copies[p][key] = cp

    n_p = len(bufs)
    pieces = range(n_p)
    half = bufs[0].shape[4] // 2
    order = (0, -1, 1, 2)

    def along_b(p, da):
        a, b, _ = GATHER_ORDERS[p]
        send(p, ("b+", da), up[b], **{a: step(a, da)})
        send(p, ("b-", da), down[b], **{a: step(a, da)})

    def along_d(p, db):
        a, b, d = GATHER_ORDERS[p]
        send(p, ("d+", db), up[d], **{a: None, b: step(b, db)})
        send(p, ("d-", db), down[d], **{a: None, b: step(b, db)})
        to_partner(p, db, 0)

    def to_partner(p, db, dd):
        a, b, d = GATHER_ORDERS[p]
        send(p, ("p", db, dd), partner, **{a: None, b: step(b, db), d: step(d, dd)})

    for p in pieces:
        a, b, d = GATHER_ORDERS[p]
        send(p, "a+", up[a])
        send(p, "a-", down[a])
        along_b(p, 0)
    for p in pieces:
        a, b, d = GATHER_ORDERS[p]
        copies[p]["a+"].wait_recv()
        send(p, "af+", up[a], rows=slice(0, half), **{a: step(a, -1)})
        copies[p]["a-"].wait_recv()
        send(p, "af-", down[a], rows=slice(half, 2 * half), **{a: step(a, 1)})
        along_b(p, -1)
        along_b(p, 1)
    for p in pieces:
        copies[p]["af+"].wait_recv()
        copies[p]["af-"].wait_recv()
        along_b(p, 2)
        along_d(p, 0)
    for p in pieces:
        a, b, d = GATHER_ORDERS[p]
        for da in (0, -1):
            copies[p][("b+", da)].wait_recv()
            send(p, ("bf+", da), up[b], **{a: step(a, da), b: step(b, -1)})
        for da in (1, 2):
            copies[p][("b-", da)].wait_recv()
            send(p, ("bf-", da), down[b], **{a: step(a, da), b: step(b, 1)})
        for da in (1, 2):
            copies[p][("b+", da)].wait_recv()
        along_d(p, -1)
        for da in (0, -1):
            copies[p][("b-", da)].wait_recv()
        along_d(p, 1)
    for p in pieces:
        for da in (0, -1):
            copies[p][("bf+", da)].wait_recv()
        for da in (1, 2):
            copies[p][("bf-", da)].wait_recv()
        along_d(p, 2)
    for db in order:
        for p in pieces:
            a, b, d = GATHER_ORDERS[p]
            copies[p][("d+", db)].wait_recv()
            if db in (0, -1):
                send(p, ("df+", db), up[d], **{a: None, b: step(b, db), d: step(d, -1)})
            to_partner(p, db, -1)
            copies[p][("d-", db)].wait_recv()
            if db in (1, 2):
                send(p, ("df-", db), down[d], **{a: None, b: step(b, db), d: step(d, 1)})
            to_partner(p, db, 1)
    for db in order:
        for p in pieces:
            copies[p][("df+" if db in (0, -1) else "df-", db)].wait_recv()
            to_partner(p, db, 2)
    for p in pieces:
        for db in order:
            for dd in order:
                copies[p][("p", db, dd)].wait_recv()
    for p in pieces:
        for cp in copies[p].values():
            cp.wait_send()


GATHER_COPIES = 44


def my_coord():
    me = lax.axis_index("sp")
    return {
        "core": lax.rem(me, CORES),
        "x": lax.rem(me // CORES, RING),
        "y": lax.rem(me // (CORES * RING), RING),
        "z": me // (CORES * RING * RING),
    }


def qkv_kernel(kv_own, qa_own, qb_own, wqa, wqb, wk, wv, inv_freq, pick, qt_out, k_out, vt_out, pos_out,
               kv_buf, qa_buf, qb_buf, send_sem, recv_sem, *, blk):
    coord = my_coord()

    def fill_own():
        at = (coord["z"], coord["y"], coord["x"], coord["core"])
        kv_buf[at] = kv_own[...]
        qa_buf[at] = qa_own[...]
        qb_buf[at] = qb_own[...]

    gather_kernel_copies((kv_buf, qa_buf, qb_buf), coord, send_sem, recv_sem, fill_own)

    nt = (((1,), (1,)), ((), ()))
    half = ROPE_DIM // 2
    tok_blk = kv_own.shape[0]
    shards = blk // tok_blk
    lines = shards // (RING * CORES)
    n_blk = qt_out.shape[1] // blk
    per_z = RING // lines
    f32, bf16 = jnp.float32, jnp.bfloat16

    @pl.loop(0, n_blk)
    def _(n):
        at = (n // per_z, pl.ds(lax.rem(n, per_z) * lines, lines))
        flat = lambda v: v.reshape(blk, v.shape[-1])
        lat = flat(kv_buf[at])
        qa = flat(qa_buf[at])
        qb = flat(qb_buf[at])
        tail = qb[:, qb.shape[1] - NOPE_DIM:]
        rows = pl.ds(pl.multiple_of(n * blk, blk), blk)
        k_out[rows, :NOPE_DIM] = jnp.dot(lat, wk[...], preferred_element_type=f32).astype(bf16)
        k_out[rows, NOPE_DIM:] = tail
        vt_out[:, rows] = lax.dot_general(wv[...], lat, nt, preferred_element_type=f32).astype(bf16)
        pos = lax.dot_general(pick[...], tail, nt, preferred_element_type=f32)
        pos_out[:, rows] = pos
        angle = inv_freq[...] * pos[0:1]
        cosine, sine = jnp.cos(angle), jnp.sin(angle)
        qt = lax.dot_general(wqa[...], qa, nt, preferred_element_type=f32)
        qt += lax.dot_general(wqb[...], qb[:, :qb.shape[1] - NOPE_DIM], nt, preferred_element_type=f32)
        lo, hi = qt[NOPE_DIM:NOPE_DIM + half], qt[NOPE_DIM + half:]
        qt_out[:NOPE_DIM, rows] = qt[:NOPE_DIM].astype(bf16)
        qt_out[NOPE_DIM:NOPE_DIM + half, rows] = (lo * cosine - hi * sine).astype(bf16)
        qt_out[NOPE_DIM + half:QK_DIM, rows] = (hi * cosine + lo * sine).astype(bf16)
        qt_out[QK_DIM:, rows] = jnp.zeros((2 * NOPE_DIM - QK_DIM, blk), bf16)


def gather_qkv(kv_own, qa_own, qb_own, w_uq, w_ukv, tok_total, blk):
    rows = kv_own.shape[0]
    f32, bf16 = jnp.float32, jnp.bfloat16
    half = ROPE_DIM // 2
    inv_freq = 10000.0 ** (-jnp.arange(half, dtype=f32) / half)
    lane = jnp.arange(NOPE_DIM)[None, :]
    pick = jnp.where(jnp.arange(8)[:, None] == 0, jnp.where(lane == ROPE_DIM, 64.0, jnp.where(lane == ROPE_DIM + 1, 1.0, 0.0)), 0.0).astype(bf16)
    vm = pl.BlockSpec(memory_space=pltpu.VMEM)
    wa = qa_own.shape[1]
    buf = lambda own: pltpu.VMEM((RING, RING, RING, CORES, rows, own.shape[1]), bf16)
    return pl.pallas_call(
        functools.partial(qkv_kernel, blk=blk),
        name="gather_qkv",
        out_shape=(
            jax.ShapeDtypeStruct((2 * NOPE_DIM, tok_total), bf16),
            jax.ShapeDtypeStruct((tok_total, 2 * NOPE_DIM), bf16),
            jax.ShapeDtypeStruct((VALUE_DIM, tok_total), bf16),
            jax.ShapeDtypeStruct((8, tok_total), f32),
        ),
        in_specs=[vm] * 9,
        out_specs=(vm,) * 4,
        scratch_shapes=[
            buf(kv_own), buf(qa_own), buf(qb_own),
            pltpu.SemaphoreType.DMA((3, GATHER_COPIES)),
            pltpu.SemaphoreType.DMA((3, GATHER_COPIES)),
        ],
        cost_estimate=pl.CostEstimate(flops=4_000_000_000, bytes_accessed=6_000_000, transcendentals=0),
        compiler_params=pltpu.CompilerParams(collective_id=2, has_side_effects=True, vmem_limit_bytes=40 << 20),
    )(kv_own, qa_own, qb_own, w_uq[:wa].T, w_uq[wa:].T, w_ukv[:, :NOPE_DIM], w_ukv[:, NOPE_DIM:].T, inv_freq[:, None], pick)


def attn_kernel(q_ref, k_ref, v_ref, pos_ref, o_ref, acc_ref, *, blk):
    i = pl.program_id(0)
    pos = pos_ref[0:1].astype(jnp.int32)
    start = i * blk + lax.broadcasted_iota(jnp.int32, (1, blk), 1) - pos
    acc_ref[...] = jnp.zeros_like(acc_ref)

    def block(masked, kb, carry):
        m_old, l_old = carry
        rows = pl.ds(pl.multiple_of(kb * blk, blk), blk)
        s = jnp.dot(k_ref[rows, :], q_ref[...], preferred_element_type=jnp.float32)
        if masked:
            key = kb * blk + lax.broadcasted_iota(jnp.int32, s.shape, 0)
            back = key - start
            s = jnp.where((back >= 0) & (back <= pos), s, MASKED)
        m_new = jnp.maximum(m_old, jnp.max(s, axis=0, keepdims=True))
        p = jnp.exp2((s - m_new) * (SCORE_SCALE * LOG2E))
        alpha = jnp.exp2((m_old - m_new) * (SCORE_SCALE * LOG2E))
        l_new = l_old * alpha + jnp.sum(p, axis=0, keepdims=True)
        acc_ref[...] = acc_ref[...] * alpha + jnp.dot(v_ref[:, rows], p.astype(jnp.bfloat16), preferred_element_type=jnp.float32)
        return m_new, l_new

    carry = (jnp.full((1, blk), MASKED, jnp.float32), jnp.zeros((1, blk), jnp.float32))
    lo = jnp.min(start) // blk
    clear = jnp.minimum((jnp.max(start) + (blk - 1)) // blk, i)
    carry = lax.fori_loop(lo, clear, functools.partial(block, True), carry)
    carry = lax.fori_loop(clear, i, functools.partial(block, False), carry)
    _, total = block(True, i, carry)
    o_ref[...] = (acc_ref[...] / total).T.astype(jnp.bfloat16)


def attention(qt, k, vt, pos_rows, blk):
    tok = k.shape[0]
    n_blk = tok // blk
    whole = lambda a: pl.BlockSpec(a.shape, lambda i: (0, 0), pipeline_mode=pl.Buffered(1))
    lane_blk = lambda a: pl.BlockSpec((a.shape[0], blk), lambda i: (0, i))
    return pl.pallas_call(
        functools.partial(attn_kernel, blk=blk),
        name="attention",
        out_shape=jax.ShapeDtypeStruct((tok, VALUE_DIM), jnp.bfloat16),
        grid=(n_blk,),
        in_specs=[lane_blk(qt), whole(k), whole(vt), lane_blk(pos_rows)],
        out_specs=pl.BlockSpec((blk, VALUE_DIM), lambda i: (i, 0)),
        scratch_shapes=[pltpu.VMEM((VALUE_DIM, blk), jnp.float32)],
        cost_estimate=pl.CostEstimate(flops=10_000_000_000, bytes_accessed=8_000_000, transcendentals=9_000_000),
        compiler_params=pltpu.CompilerParams(dimension_semantics=("arbitrary",), vmem_limit_bytes=40 << 20),
    )(qt, k, vt, pos_rows)


def project_kernel(o_ref, wo_ref, y_ref, o_all, w_buf, acc, y_half, y_in, w_sem, send_sem, recv_sem, fwd_send, fwd_recv,
                   y_sem, *, n_buf):
    coord = my_coord()
    core, x, y, z = (coord[a] for a in ("core", "x", "y", "z"))
    lines = RING * RING
    chip_rows, head = o_all.shape[3], o_all.shape[4]
    w_rows, cols = w_buf.shape[1], w_buf.shape[2]
    mesh_id = pl.DeviceIdType.MESH

    def line_of(k):
        return lax.rem(z + k // RING, RING) * RING + lax.rem(y + lax.rem(k, RING), RING)

    def w_copy(k):
        rows = pl.ds(pl.multiple_of(line_of(k) * w_rows, w_rows), w_rows)
        side = pl.ds(pl.multiple_of(core * cols, 128), cols)
        slot = lax.rem(k, n_buf)
        return pltpu.make_async_copy(wo_ref.at[rows, side], w_buf.at[slot], w_sem.at[slot])

    @pl.loop(0, n_buf)
    def _(k):
        w_copy(k).start()

    def chip(k, dx):
        zz = lax.rem(z + RING - k // RING, RING)
        yy = lax.rem(y + RING - lax.rem(k, RING), RING)
        xx = lax.rem(x + RING - dx, RING)
        return (zz * RING + yy) * RING + xx

    me_chip = (z * RING + y) * RING + x
    partner = {"sp": me_chip * CORES + 1 - core}
    n_chips = lines * RING

    barrier = pltpu.get_barrier_semaphore()
    pl.semaphore_signal(barrier, inc=1, device_id=partner, device_id_type=mesh_id)

    @pl.loop(1, n_chips)
    def _(n):
        to = {"sp": chip(n // RING, lax.rem(n, RING)) * CORES + core}
        pl.semaphore_signal(barrier, inc=1, device_id=to, device_id_type=mesh_id)

    my_line = z * RING + y
    o_all[my_line, x, core] = o_ref[pl.ds(pl.multiple_of(me_chip * chip_rows, chip_rows), chip_rows), :]
    pl.semaphore_wait(barrier, n_chips)

    def head_copy(n):
        to = chip(n // RING, lax.rem(n, RING))
        rows = pl.ds(pl.multiple_of(to * chip_rows, chip_rows), chip_rows)
        return pltpu.make_async_remote_copy(
            src_ref=o_ref.at[rows, :], dst_ref=o_all.at[my_line, x, core], send_sem=send_sem, recv_sem=recv_sem.at[n // RING],
            device_id={"sp": to * CORES + core}, device_id_type=mesh_id)

    @pl.loop(1, n_chips)
    def _(n):
        head_copy(n).start()

    def forward(k):
        at = o_all.at[line_of(k), :, core]
        return pltpu.make_async_remote_copy(
            src_ref=at, dst_ref=at, send_sem=fwd_send.at[k], recv_sem=fwd_recv.at[k], device_id=partner, device_id_type=mesh_id)

    def arrive(k, n_heads):
        at = o_all.at[line_of(k), pl.ds(0, n_heads), core]
        pltpu.make_async_copy(at, at, recv_sem.at[k]).wait()
        forward(k).start()

    acc[...] = jnp.zeros_like(acc)
    arrive(0, RING - 1)

    @pl.loop(0, lines)
    def _(k):
        @pl.when(k + 1 < lines)
        def _():
            arrive(k + 1, RING)

        forward(k).wait_recv()
        w_copy(k).wait()
        line = line_of(k)
        lhs = jnp.concatenate([o_all[line, i, j] for i in range(RING) for j in range(CORES)], axis=1)
        acc[...] += jnp.dot(lhs, w_buf[lax.rem(k, n_buf)], preferred_element_type=jnp.float32)

        @pl.when(k + n_buf < lines)
        def _():
            w_copy(k + n_buf).start()

    own_rows = chip_rows // CORES
    y_half[...] = acc[...].astype(jnp.bfloat16)
    swap = pltpu.make_async_remote_copy(
        src_ref=y_half.at[pl.ds(pl.multiple_of((1 - core) * own_rows, own_rows), own_rows), :], dst_ref=y_in,
        send_sem=y_sem.at[0], recv_sem=y_sem.at[1], device_id=partner, device_id_type=mesh_id)
    swap.start()
    mine = y_half[pl.ds(pl.multiple_of(core * own_rows, own_rows), own_rows), :]
    swap.wait_recv()
    other = y_in[...]
    y_ref[:, :cols] = jnp.where(core == 0, mine, other)
    y_ref[:, cols:] = jnp.where(core == 0, other, mine)
    swap.wait_send()

    @pl.loop(0, lines)
    def _(k):
        forward(k).wait_send()

    everything = o_ref.at[pl.ds(0, (n_chips - 1) * chip_rows), :]
    pltpu.make_async_copy(everything, everything, send_sem).wait()


def project(o_loc, w_o, group_size, n_buf):
    tok, head = o_loc.shape
    own_rows = tok // group_size
    dim = w_o.shape[1]
    lines = RING * RING
    w_rows = w_o.shape[0] // lines
    f32, bf16 = jnp.float32, jnp.bfloat16
    vm = pl.BlockSpec(memory_space=pltpu.VMEM)
    return pl.pallas_call(
        functools.partial(project_kernel, n_buf=n_buf),
        name="project",
        out_shape=jax.ShapeDtypeStruct((own_rows, dim), bf16),
        in_specs=[vm, pl.BlockSpec(memory_space=pl.ANY)],
        out_specs=vm,
        scratch_shapes=[
            pltpu.VMEM((lines, RING, CORES, CORES * own_rows, head), bf16),
            pltpu.VMEM((n_buf, w_rows, dim // CORES), bf16),
            pltpu.VMEM((CORES * own_rows, dim // CORES), f32),
            pltpu.VMEM((CORES * own_rows, dim // CORES), bf16),
            pltpu.VMEM((own_rows, dim // CORES), bf16),
            pltpu.SemaphoreType.DMA((n_buf,)),
            pltpu.SemaphoreType.DMA,
            pltpu.SemaphoreType.DMA((lines,)),
            pltpu.SemaphoreType.DMA((lines,)),
            pltpu.SemaphoreType.DMA((lines,)),
            pltpu.SemaphoreType.DMA((2,)),
        ],
        cost_estimate=pl.CostEstimate(flops=4_000_000_000, bytes_accessed=60_000_000, transcendentals=0),
        compiler_params=pltpu.CompilerParams(collective_id=3, has_side_effects=True, vmem_limit_bytes=56 << 20),
    )(o_loc, w_o)


def ffn_kernel(y_ref, g_ref, *rest, dim, pad, sub, tile_n):
    n_wt = 5
    weights = rest[:n_wt]
    (out_ref, ybuf, wgu, wdn, hbuf, gubuf, part, far_l, far_r, in_l, in_r, far2_l, far2_r, in2_l, in2_r,
     w_sem, wx_send, wx_recv, ag_send, ag_recv, rs_send, rs_recv) = rest[n_wt:]
    coord = my_coord()

    def device(axis, by):
        c = {**coord, axis: lax.rem(coord[axis] + (by % RING), RING) if axis != "core" else 1 - coord[axis]}
        return {"sp": ((c["z"] * RING + c["y"]) * RING + c["x"]) * CORES + c["core"]}

    x_up, x_dn, y_up, y_dn = device("x", 1), device("x", -1), device("y", 1), device("y", -1)
    z_up, z_dn, partner = device("z", 1), device("z", -1), device("core", 1)
    up1, dn1, up2, dn2 = (x_up, y_up), (x_dn, y_dn), (y_up, x_up), (y_dn, x_dn)

    barrier = pltpu.get_barrier_semaphore()
    for nb in (x_up, x_dn, y_up, y_dn, z_up, z_dn, partner):
        pl.semaphore_signal(barrier, inc=1, device_id=nb, device_id_type=pl.DeviceIdType.MESH)

    w_copies = []

    def fetch(src, dst):
        cp = pltpu.make_async_copy(src, dst, w_sem.at[len(w_copies)])
        cp.start()
        w_copies.append(cp)

    up0 = 8 * pad
    own, left_a, left_b, right_a, right_b = weights
    cut = left_a.shape[0]
    fetch(own.at[0:pad], wgu.at[0:pad])
    fetch(own.at[pad:2 * pad], wgu.at[up0:up0 + pad])
    fetch(own.at[2 * pad:], wdn.at[0:pad])
    for n, (part_a, part_b) in ((1, (left_a, left_b)), (2, (right_a, right_b))):
        r = n * pad
        fetch(part_a.at[0:pad], wgu.at[r:r + pad])
        fetch(part_a.at[pad:cut], wgu.at[up0 + r:up0 + r + cut - pad])
        fetch(part_b.at[0:2 * pad - cut], wgu.at[up0 + r + cut - pad:up0 + r + pad])
        fetch(part_b.at[2 * pad - cut:], wdn.at[r:r + pad])

    wx_copies = []

    def exchange(buf, src, dst, rows, dev):
        n = len(wx_copies)
        cp = pltpu.make_async_remote_copy(
            src_ref=buf.at[src:src + rows], dst_ref=buf.at[dst:dst + rows], send_sem=wx_send.at[n], recv_sem=wx_recv.at[n],
            device_id=dev, device_id_type=pl.DeviceIdType.MESH)
        cp.start()
        wx_copies.append(cp)

    for h in range(2):
        ybuf[h, 0] = y_ref[h * sub:(h + 1) * sub, :]
    pl.semaphore_wait(barrier, 7)

    cols = (slice(0, dim // 2), slice(dim // 2, dim))
    ag_copies = {}
    ag_n = [0]

    def ag_send_to(h, src_slot, dst_slot, dev, col=None):
        c = slice(None) if col is None else cols[col]
        key = (h, dst_slot, col)
        rsem = dst_slot if col != 1 else RING * RING
        cp = pltpu.make_async_remote_copy(
            src_ref=ybuf.at[h, src_slot, :, c], dst_ref=ybuf.at[h, dst_slot, :, c],
            send_sem=ag_send.at[ag_n[0]], recv_sem=ag_recv.at[h, rsem],
            device_id=dev, device_id_type=pl.DeviceIdType.MESH)
        ag_n[0] += 1
        cp.start()
        ag_copies[key] = cp

    far = 2
    for h in range(2):
        ag_send_to(h, 0, 3 * RING, up1[h])
        ag_send_to(h, 0, 1 * RING, dn1[h])
    for h in range(2):
        ag_send_to(h, 0, 3, up2[h])
        ag_send_to(h, 0, 1, dn2[h])
    for cp in w_copies:
        cp.wait()
    split = cut - pad
    exchange(wgu, pad, 3 * pad, pad, z_up)
    exchange(wgu, up0 + pad, up0 + 3 * pad, split, z_up)
    exchange(wgu, up0 + 2 * pad + split, up0 + 3 * pad + split, pad - split, z_dn)
    exchange(wdn, 2 * pad, 3 * pad, pad, z_dn)
    exchange(wgu, 0, 4 * pad, 3 * pad, partner)
    exchange(wgu, up0, up0 + 4 * pad, 3 * pad, partner)
    exchange(wdn, 0, 4 * pad, 3 * pad, partner)
    for h in range(2):
        ag_copies[(h, 3 * RING, None)].wait_recv()
        ag_send_to(h, 3 * RING, far * RING, up1[h], 0)
        ag_copies[(h, 1 * RING, None)].wait_recv()
        ag_send_to(h, 1 * RING, far * RING, dn1[h], 1)
        for d1 in (3, 1):
            ag_send_to(h, d1 * RING, d1 * RING + 3, up2[h])
            ag_send_to(h, d1 * RING, d1 * RING + 1, dn2[h])
    for h in range(2):
        ag_copies[(h, far * RING, 0)].wait_recv()
        ag_copies[(h, far * RING, 1)].wait_recv()
        ag_send_to(h, far * RING, far * RING + 3, up2[h])
        ag_send_to(h, far * RING, far * RING + 1, dn2[h])
    for d1, d2, dev in ((0, 3, up2), (3, 3, up2), (1, 1, dn2), (2, 1, dn2)):
        for h in range(2):
            ag_copies[(h, d1 * RING + d2, None)].wait_recv()
            ag_send_to(h, d1 * RING + d2, d1 * RING + far, dev[h])
    for d1, d2 in ((0, 1), (3, 1), (1, 3), (2, 3), (0, 2), (3, 2), (1, 2), (2, 2)):
        for h in range(2):
            ag_copies[(h, d1 * RING + d2, None)].wait_recv()

    for n in range(4):
        wx_copies[n].wait_recv()
    exchange(wgu, 3 * pad, 7 * pad, pad, partner)
    exchange(wgu, up0 + 3 * pad, up0 + 7 * pad, pad, partner)
    exchange(wdn, 3 * pad, 7 * pad, pad, partner)
    for n in range(4, 10):
        wx_copies[n].wait_recv()

    rows = 2 * RING * sub
    nt = (((1,), (1,)), ((), ()))
    ff_pad = 8 * pad

    def compute(d1):
        for h in range(2):
            for d2 in range(RING):
                v = ybuf[h, d1 * RING + d2].astype(jnp.float32)
                mean_sq = jnp.mean(v * v, axis=-1, keepdims=True)
                r = (h * RING + d2) * sub
                hbuf[r:r + sub, :] = (v * lax.rsqrt(mean_sq + 1e-6) * g_ref[...].astype(jnp.float32)).astype(jnp.bfloat16)
        n_gu = gubuf.shape[1] // tile_n

        @pl.loop(0, n_gu)
        def _(j):
            c = pl.ds(pl.multiple_of(j * tile_n, tile_n), tile_n)
            gubuf[:, c] = lax.dot_general(hbuf[...], wgu[c, :], nt, preferred_element_type=jnp.float32)

        gate = gubuf[:, :ff_pad]
        act = (gate * jax.nn.sigmoid(gate) * gubuf[:, ff_pad:]).astype(jnp.bfloat16)
        wide = dim // 7 if dim % (7 * 128) == 0 else dim
        for j in range(dim // wide):
            c = slice(j * wide, (j + 1) * wide)
            res = jnp.dot(act, wdn[:, c], preferred_element_type=jnp.float32)
            for h in range(2):
                for d2 in range(RING):
                    r = (h * RING + d2) * sub
                    part[h, d1 * RING + d2, :, c] = res[r:r + sub]

    rs_copies = {}
    rs_n = [0]

    def rs_send_to(key, src, dst, dev):
        cp = pltpu.make_async_remote_copy(
            src_ref=src, dst_ref=dst, send_sem=rs_send.at[rs_n[0]], recv_sem=rs_recv.at[rs_n[0]],
            device_id=dev, device_id_type=pl.DeviceIdType.MESH)
        rs_n[0] += 1
        cp.start()
        rs_copies[key] = cp

    order = (2, 1, 3, 0)
    compute(far)
    for d2 in order:
        for h in range(2):
            rs_send_to(("fl", h, d2), part.at[h, far * RING + d2, :, cols[0]], far_l.at[h, d2], up1[h])
            rs_send_to(("fr", h, d2), part.at[h, far * RING + d2, :, cols[1]], far_r.at[h, d2], dn1[h])
    compute(1)
    compute(3)
    for d2 in order:
        for h in range(2):
            rs_copies[("fl", h, d2)].wait_recv()
            part[h, RING + d2, :, cols[0]] += far_l[h, d2]
            rs_send_to(("il", h, d2), part.at[h, RING + d2], in_l.at[h, d2], up1[h])
            rs_copies[("fr", h, d2)].wait_recv()
            part[h, 3 * RING + d2, :, cols[1]] += far_r[h, d2]
            rs_send_to(("ir", h, d2), part.at[h, 3 * RING + d2], in_r.at[h, d2], dn1[h])
    compute(0)

    def first_sum(h, d2):
        rs_copies[("il", h, d2)].wait_recv()
        rs_copies[("ir", h, d2)].wait_recv()
        part[h, d2] = part[h, d2] + in_l[h, d2] + in_r[h, d2]

    for h in range(2):
        first_sum(h, 2)
        rs_send_to(("gl", h), part.at[h, 2, :, cols[0]], far2_l.at[h], up2[h])
        rs_send_to(("gr", h), part.at[h, 2, :, cols[1]], far2_r.at[h], dn2[h])
    for h in range(2):
        first_sum(h, 1)
        rs_copies[("gl", h)].wait_recv()
        part[h, 1, :, cols[0]] += far2_l[h]
        rs_send_to(("jl", h), part.at[h, 1], in2_l.at[h], up2[h])
        first_sum(h, 3)
        rs_copies[("gr", h)].wait_recv()
        part[h, 3, :, cols[1]] += far2_r[h]
        rs_send_to(("jr", h), part.at[h, 3], in2_r.at[h], dn2[h])
    for h in range(2):
        first_sum(h, 0)
        rs_copies[("jl", h)].wait_recv()
        rs_copies[("jr", h)].wait_recv()
        total = part[h, 0] + in2_l[h] + in2_r[h]
        out_ref[h * sub:(h + 1) * sub, :] = (ybuf[h, 0].astype(jnp.float32) + total).astype(jnp.bfloat16)
    for cp in wx_copies + list(ag_copies.values()) + list(rs_copies.values()):
        cp.wait_send()


def ffn(y_own, g_ffn, weights, pad):
    rows, dim = y_own.shape
    sub = rows // 2
    chunk = 2 * RING * sub
    f32, bf16 = jnp.float32, jnp.bfloat16
    vm = pl.BlockSpec(memory_space=pltpu.VMEM)
    hbm = pl.BlockSpec(memory_space=pl.ANY)
    half = dim // 2
    return pl.pallas_call(
        functools.partial(ffn_kernel, dim=dim, pad=pad, sub=sub, tile_n=256 if (16 * pad) % 256 == 0 else 16 * pad),
        name="ffn",
        out_shape=jax.ShapeDtypeStruct((rows, dim), bf16),
        in_specs=[vm, vm] + [hbm] * 5,
        out_specs=vm,
        scratch_shapes=[
            pltpu.VMEM((2, RING * RING, sub, dim), bf16),
            pltpu.VMEM((16 * pad, dim), bf16),
            pltpu.VMEM((8 * pad, dim), bf16),
            pltpu.VMEM((chunk, dim), bf16),
            pltpu.VMEM((chunk, 16 * pad), f32),
            pltpu.VMEM((2, RING * RING, sub, dim), f32),
            pltpu.VMEM((2, RING, sub, half), f32),
            pltpu.VMEM((2, RING, sub, half), f32),
            pltpu.VMEM((2, RING, sub, dim), f32),
            pltpu.VMEM((2, RING, sub, dim), f32),
            pltpu.VMEM((2, sub, half), f32),
            pltpu.VMEM((2, sub, half), f32),
            pltpu.VMEM((2, sub, dim), f32),
            pltpu.VMEM((2, sub, dim), f32),
            pltpu.SemaphoreType.DMA((11,)),
            pltpu.SemaphoreType.DMA((10,)),
            pltpu.SemaphoreType.DMA((10,)),
            pltpu.SemaphoreType.DMA((32,)),
            pltpu.SemaphoreType.DMA((2, RING * RING + 1)),
            pltpu.SemaphoreType.DMA((40,)),
            pltpu.SemaphoreType.DMA((40,)),
        ],
        cost_estimate=pl.CostEstimate(flops=7_000_000_000, bytes_accessed=14_000_000, transcendentals=0),
        compiler_params=pltpu.CompilerParams(collective_id=1, has_side_effects=True, vmem_limit_bytes=56 << 20),
    )(y_own, g_ffn[None, :], *weights)


def weight_block(w_gate, w_up, w_down):
    cols = w_down.shape[0]
    pad = -(-cols // 16) * 16
    wide = lambda w: jnp.pad(w, ((0, pad - cols), (0, 0)))
    return jnp.concatenate([wide(w_gate.T), wide(w_up.T), wide(w_down)], axis=0), pad


def from_z_neighbours(block, group_size):
    plane = RING * RING * CORES
    up = [(d, (d + plane) % group_size) for d in range(group_size)]
    down = [(d, (d - plane) % group_size) for d in range(group_size)]
    return lax.ppermute(block, 'sp', up), lax.ppermute(block, 'sp', down)


def solution(mesh):
    group_size = mesh.shape['sp']
    tok_spec = P(('dp', 'sp'), None)
    row_spec = P(('dp', 'sp'))
    full_spec = P()
    col_spec = P(None, 'sp')

    def device_fn(x_blk, seg_blk, pos_blk, w_dq, g_q, w_uq, w_dkv, g_kv, w_ukv, w_o, g_ffn, w_gate, w_up, w_down):
        blk_len = x_blk.shape[0]
        tok_total = blk_len * group_size
        w_own, pad = weight_block(w_gate, w_up, w_down)
        cut = pad + (pad // 2) // 16 * 16
        left_a, right_a = from_z_neighbours(w_own[:cut], group_size)

        q_lin = jnp.dot(x_blk, w_dq, preferred_element_type=jnp.float32)
        c_q = rms_norm(q_lin, g_q).astype(jnp.bfloat16)
        kv_lin = jnp.dot(x_blk, w_dkv, preferred_element_type=jnp.float32)
        c_kv = rms_norm(kv_lin[:, :KV_LATENT], g_kv).astype(jnp.bfloat16)
        k_rope = apply_rope(kv_lin[:, KV_LATENT:], pos_blk).astype(jnp.bfloat16)
        pos_hi = (pos_blk // 64).astype(jnp.bfloat16)[:, None]
        pos_lo = (pos_blk % 64).astype(jnp.bfloat16)[:, None]
        spare = jnp.zeros((blk_len, NOPE_DIM - ROPE_DIM - 2), jnp.bfloat16)
        split = KV_LATENT
        q_rest = jnp.concatenate([c_q[:, split:], k_rope, pos_hi, pos_lo, spare], axis=1)
        blk = min(512, tok_total)
        qt, k, vt, pos_rows = gather_qkv(c_kv, c_q[:, :split], q_rest, w_uq, w_ukv, tok_total, blk)
        w_late, pos_rows = lax.optimization_barrier((w_own[cut:], pos_rows))
        left_b, right_b = from_z_neighbours(w_late, group_size)
        o_loc = attention(qt, k, vt, pos_rows, blk)
        y_att = project(o_loc, w_o, group_size, 12)
        return ffn(y_att, g_ffn, (w_own, left_a, left_b, right_a, right_b), pad)

    return jax.shard_map(device_fn, mesh=mesh, in_specs=(tok_spec, row_spec, row_spec, full_spec, full_spec, col_spec, full_spec, full_spec, col_spec, full_spec, full_spec, col_spec, col_spec, P('sp', None)), out_specs=tok_spec, check_vma=False)
```

```python
import functools

import jax
import jax.numpy as jnp
from jax import lax
from jax.experimental import pallas as pl
from jax.experimental.pallas import tpu as pltpu
from jax.sharding import PartitionSpec as P

NOPE_DIM = 128
ROPE_DIM = 64
VALUE_DIM = 128
KV_LATENT = 512
QK_DIM = NOPE_DIM + ROPE_DIM
KV_DIM = NOPE_DIM + VALUE_DIM
SCORE_SCALE = QK_DIM ** -0.5
LOG2E = 1.4426950408889634
MASKED = -0.7 * 3.4028234663852886e38

RING = 4
CORES = 2


def rms_norm(vec_in, gain_vec):
    mean_sq = jnp.mean(vec_in * vec_in, axis=-1, keepdims=True)
    return vec_in * lax.rsqrt(mean_sq + 1e-6) * gain_vec.astype(jnp.float32)


def rope_angles(positions):
    half_dim = ROPE_DIM // 2
    inv_freq = 10000.0 ** (-jnp.arange(half_dim, dtype=jnp.float32) / half_dim)
    return positions.astype(jnp.float32)[..., None] * inv_freq


def apply_rope(vec_in, positions):
    half_dim = ROPE_DIM // 2
    angles = rope_angles(positions)
    cosine = jnp.cos(angles)
    sine_v = jnp.sin(angles)
    lo_half = vec_in[..., :half_dim]
    hi_half = vec_in[..., half_dim:]
    return jnp.concatenate([lo_half * cosine - hi_half * sine_v, hi_half * cosine + lo_half * sine_v], axis=-1)


GATHER_ORDERS = (("x", "y", "z"), ("y", "z", "x"), ("z", "x", "y"))


def gather_kernel_copies(bufs, coord, send_sem, recv_sem, fill_own):
    core = coord["core"]

    def device(**moved):
        c = {**coord, **moved}
        return {"sp": ((c["z"] * RING + c["y"]) * RING + c["x"]) * CORES + c["core"]}

    def step(axis, by):
        return lax.rem(coord[axis] + (by % RING), RING)

    up = {a: device(**{a: step(a, 1)}) for a in "xyz"}
    down = {a: device(**{a: step(a, -1)}) for a in "xyz"}
    partner = device(core=1 - core)

    barrier = pltpu.get_barrier_semaphore()
    for nb in list(up.values()) + list(down.values()) + [partner]:
        pl.semaphore_signal(barrier, inc=1, device_id=nb, device_id_type=pl.DeviceIdType.MESH)
    fill_own()
    pl.semaphore_wait(barrier, 7)

    copies = [{} for _ in bufs]

    def send(p, key, dev, rows=None, **at):
        idx = tuple(slice(None) if at.get(a, 0) is None else at.get(a, coord[a]) for a in "zyx") + (core,)
        if rows is not None:
            idx = idx + (rows,)
        n = len(copies[p])
        cp = pltpu.make_async_remote_copy(
            src_ref=bufs[p].at[idx], dst_ref=bufs[p].at[idx], send_sem=send_sem.at[p, n], recv_sem=recv_sem.at[p, n],
            device_id=dev, device_id_type=pl.DeviceIdType.MESH)
        cp.start()
        copies[p][key] = cp

    n_p = len(bufs)
    pieces = range(n_p)
    half = bufs[0].shape[4] // 2
    order = (0, -1, 1, 2)

    def along_b(p, da):
        a, b, _ = GATHER_ORDERS[p]
        send(p, ("b+", da), up[b], **{a: step(a, da)})
        send(p, ("b-", da), down[b], **{a: step(a, da)})

    def along_d(p, db):
        a, b, d = GATHER_ORDERS[p]
        send(p, ("d+", db), up[d], **{a: None, b: step(b, db)})
        send(p, ("d-", db), down[d], **{a: None, b: step(b, db)})
        to_partner(p, db, 0)

    def to_partner(p, db, dd):
        a, b, d = GATHER_ORDERS[p]
        send(p, ("p", db, dd), partner, **{a: None, b: step(b, db), d: step(d, dd)})

    for p in pieces:
        a, b, d = GATHER_ORDERS[p]
        send(p, "a+", up[a])
        send(p, "a-", down[a])
        along_b(p, 0)
    for p in pieces:
        a, b, d = GATHER_ORDERS[p]
        copies[p]["a+"].wait_recv()
        send(p, "af+", up[a], rows=slice(0, half), **{a: step(a, -1)})
        copies[p]["a-"].wait_recv()
        send(p, "af-", down[a], rows=slice(half, 2 * half), **{a: step(a, 1)})
        along_b(p, -1)
        along_b(p, 1)
    for p in pieces:
        copies[p]["af+"].wait_recv()
        copies[p]["af-"].wait_recv()
        along_b(p, 2)
        along_d(p, 0)
    for p in pieces:
        a, b, d = GATHER_ORDERS[p]
        for da in (0, -1):
            copies[p][("b+", da)].wait_recv()
            send(p, ("bf+", da), up[b], **{a: step(a, da), b: step(b, -1)})
        for da in (1, 2):
            copies[p][("b-", da)].wait_recv()
            send(p, ("bf-", da), down[b], **{a: step(a, da), b: step(b, 1)})
        for da in (1, 2):
            copies[p][("b+", da)].wait_recv()
        along_d(p, -1)
        for da in (0, -1):
            copies[p][("b-", da)].wait_recv()
        along_d(p, 1)
    for p in pieces:
        for da in (0, -1):
            copies[p][("bf+", da)].wait_recv()
        for da in (1, 2):
            copies[p][("bf-", da)].wait_recv()
        along_d(p, 2)
    for db in order:
        for p in pieces:
            a, b, d = GATHER_ORDERS[p]
            copies[p][("d+", db)].wait_recv()
            if db in (0, -1):
                send(p, ("df+", db), up[d], **{a: None, b: step(b, db), d: step(d, -1)})
            to_partner(p, db, -1)
            copies[p][("d-", db)].wait_recv()
            if db in (1, 2):
                send(p, ("df-", db), down[d], **{a: None, b: step(b, db), d: step(d, 1)})
            to_partner(p, db, 1)
    for db in order:
        for p in pieces:
            copies[p][("df+" if db in (0, -1) else "df-", db)].wait_recv()
            to_partner(p, db, 2)
    for p in pieces:
        for db in order:
            for dd in order:
                copies[p][("p", db, dd)].wait_recv()
    for p in pieces:
        for cp in copies[p].values():
            cp.wait_send()


GATHER_COPIES = 44


def my_coord():
    me = lax.axis_index("sp")
    return {
        "core": lax.rem(me, CORES),
        "x": lax.rem(me // CORES, RING),
        "y": lax.rem(me // (CORES * RING), RING),
        "z": me // (CORES * RING * RING),
    }


def qkv_kernel(kv_own, qa_own, qb_own, wqa, wqb, wk, wv, inv_freq, pick, qt_out, k_out, vt_out, pos_out,
               kv_buf, qa_buf, qb_buf, send_sem, recv_sem, *, blk):
    coord = my_coord()

    def fill_own():
        at = (coord["z"], coord["y"], coord["x"], coord["core"])
        kv_buf[at] = kv_own[...]
        qa_buf[at] = qa_own[...]
        qb_buf[at] = qb_own[...]

    gather_kernel_copies((kv_buf, qa_buf, qb_buf), coord, send_sem, recv_sem, fill_own)

    nt = (((1,), (1,)), ((), ()))
    half = ROPE_DIM // 2
    tok_blk = kv_own.shape[0]
    shards = blk // tok_blk
    lines = shards // (RING * CORES)
    n_blk = qt_out.shape[1] // blk
    per_z = RING // lines
    f32, bf16 = jnp.float32, jnp.bfloat16

    @pl.loop(0, n_blk)
    def _(n):
        at = (n // per_z, pl.ds(lax.rem(n, per_z) * lines, lines))
        flat = lambda v: v.reshape(blk, v.shape[-1])
        lat = flat(kv_buf[at])
        qa = flat(qa_buf[at])
        qb = flat(qb_buf[at])
        tail = qb[:, qb.shape[1] - NOPE_DIM:]
        rows = pl.ds(pl.multiple_of(n * blk, blk), blk)
        k_out[rows, :NOPE_DIM] = jnp.dot(lat, wk[...], preferred_element_type=f32).astype(bf16)
        k_out[rows, NOPE_DIM:] = tail
        vt_out[:, rows] = lax.dot_general(wv[...], lat, nt, preferred_element_type=f32).astype(bf16)
        pos = lax.dot_general(pick[...], tail, nt, preferred_element_type=f32)
        pos_out[:, rows] = pos
        angle = inv_freq[...] * pos[0:1]
        cosine, sine = jnp.cos(angle), jnp.sin(angle)
        qt = lax.dot_general(wqa[...], qa, nt, preferred_element_type=f32)
        qt += lax.dot_general(wqb[...], qb[:, :qb.shape[1] - NOPE_DIM], nt, preferred_element_type=f32)
        lo, hi = qt[NOPE_DIM:NOPE_DIM + half], qt[NOPE_DIM + half:]
        qt_out[:NOPE_DIM, rows] = qt[:NOPE_DIM].astype(bf16)
        qt_out[NOPE_DIM:NOPE_DIM + half, rows] = (lo * cosine - hi * sine).astype(bf16)
        qt_out[NOPE_DIM + half:QK_DIM, rows] = (hi * cosine + lo * sine).astype(bf16)
        qt_out[QK_DIM:, rows] = jnp.zeros((2 * NOPE_DIM - QK_DIM, blk), bf16)


def gather_qkv(kv_own, qa_own, qb_own, w_uq, w_ukv, tok_total, blk):
    rows = kv_own.shape[0]
    f32, bf16 = jnp.float32, jnp.bfloat16
    half = ROPE_DIM // 2
    inv_freq = 10000.0 ** (-jnp.arange(half, dtype=f32) / half)
    lane = jnp.arange(NOPE_DIM)[None, :]
    pick = jnp.where(jnp.arange(8)[:, None] == 0, jnp.where(lane == ROPE_DIM, 64.0, jnp.where(lane == ROPE_DIM + 1, 1.0, 0.0)), 0.0).astype(bf16)
    vm = pl.BlockSpec(memory_space=pltpu.VMEM)
    wa = qa_own.shape[1]
    buf = lambda own: pltpu.VMEM((RING, RING, RING, CORES, rows, own.shape[1]), bf16)
    return pl.pallas_call(
        functools.partial(qkv_kernel, blk=blk),
        name="gather_qkv",
        out_shape=(
            jax.ShapeDtypeStruct((2 * NOPE_DIM, tok_total), bf16),
            jax.ShapeDtypeStruct((tok_total, 2 * NOPE_DIM), bf16),
            jax.ShapeDtypeStruct((VALUE_DIM, tok_total), bf16),
            jax.ShapeDtypeStruct((8, tok_total), f32),
        ),
        in_specs=[vm] * 9,
        out_specs=(vm,) * 4,
        scratch_shapes=[
            buf(kv_own), buf(qa_own), buf(qb_own),
            pltpu.SemaphoreType.DMA((3, GATHER_COPIES)),
            pltpu.SemaphoreType.DMA((3, GATHER_COPIES)),
        ],
        cost_estimate=pl.CostEstimate(flops=4_000_000_000, bytes_accessed=6_000_000, transcendentals=0),
        compiler_params=pltpu.CompilerParams(collective_id=2, has_side_effects=True, vmem_limit_bytes=40 << 20),
    )(kv_own, qa_own, qb_own, w_uq[:wa].T, w_uq[wa:].T, w_ukv[:, :NOPE_DIM], w_ukv[:, NOPE_DIM:].T, inv_freq[:, None], pick)


SUB_KEYS = 32


def attend_kernel(q_ref, k_ref, v_ref, pos_ref, wo_ref, y_ref, s_even, s_odd, p_even, p_odd, acc_o, stats, o_buf, o_all, w_buf, acc, y_half, y_in,
                  w_sem, send_sem, recv_sem, fwd_send, fwd_recv, y_sem, *, blk, n_buf):
    coord = my_coord()
    core, x, y, z = (coord[a] for a in ("core", "x", "y", "z"))
    y_top, y_low = y // 2, lax.rem(y, 2)
    lines = RING * RING
    n_chips = lines * RING
    chip_rows = o_all.shape[3]
    w_rows, cols = w_buf.shape[1], w_buf.shape[2]
    mesh_id = pl.DeviceIdType.MESH
    n_blk = q_ref.shape[1] // blk
    n_pairs = n_blk * (n_blk + 1) // 2
    per_z = n_blk // RING
    f32, bf16, i32 = jnp.float32, jnp.bfloat16, jnp.int32
    scale = SCORE_SCALE * LOG2E

    def line_of(n):
        step = n // 2
        return lax.rem(z + step // 2, RING) * RING + lax.rem(y_top + lax.rem(step, 2), 2) * 2 + lax.rem(y_low + lax.rem(n, 2), 2)

    def block_of(n):
        return lax.rem(z + RING - n // per_z, RING) * per_z + lax.rem(y_top + lax.rem(n, per_z), per_z)

    def w_copy(n):
        rows = pl.ds(pl.multiple_of(line_of(n) * w_rows, w_rows), w_rows)
        side = pl.ds(pl.multiple_of(core * cols, 128), cols)
        slot = lax.rem(n, n_buf)
        return pltpu.make_async_copy(wo_ref.at[rows, side], w_buf.at[slot], w_sem.at[slot])

    @pl.loop(0, n_buf)
    def _(n):
        w_copy(n).start()

    me_chip = (z * RING + y) * RING + x
    my_line = z * RING + y
    partner = {"sp": me_chip * CORES + 1 - core}

    barrier = pltpu.get_barrier_semaphore()
    pl.semaphore_signal(barrier, inc=1, device_id=partner, device_id_type=mesh_id)

    @pl.loop(1, n_chips)
    def _(n):
        to = {"sp": lax.rem(me_chip + n, n_chips) * CORES + core}
        pl.semaphore_signal(barrier, inc=1, device_id=to, device_id_type=mesh_id)

    for ref in (s_even, s_odd, p_even, p_odd):
        ref[...] = jnp.zeros_like(ref)
    acc_o[...] = jnp.zeros_like(acc_o)
    stats[...] = jnp.zeros_like(stats)
    acc[...] = jnp.zeros_like(acc)
    pl.semaphore_wait(barrier, n_chips)

    chips_per_blk = blk // chip_rows

    def send_block(i):
        line0 = i * (chips_per_blk // RING)

        @pl.loop(0, chips_per_blk)
        def _(n):
            yy = line0 + lax.rem(y_low + n // RING, chips_per_blk // RING)
            to = yy * RING + lax.rem(x + lax.rem(n, RING), RING)
            rows = pl.ds(pl.multiple_of(to * chip_rows, chip_rows), chip_rows)

            @pl.when(to == me_chip)
            def _():
                o_all[my_line, x, core] = o_buf[rows, :]

            @pl.when(to != me_chip)
            def _():
                pltpu.make_async_remote_copy(
                    src_ref=o_buf.at[rows, :], dst_ref=o_all.at[my_line, x, core], send_sem=send_sem,
                    recv_sem=recv_sem.at[my_line], device_id={"sp": to * CORES + core}, device_id_type=mesh_id).start()

    sub = SUB_KEYS
    fold = lambda v: v.reshape(sub // 8, 8, blk)
    row_id = lax.broadcasted_iota(i32, (sub, blk), 0)

    def body(t, s_a, s_b, p_a, p_b, carry):
        (n_a, i_a, j_a), (i_b, j_b), (i_c, j_c), i_done = carry
        m_old, l_old, top, alpha_c = stats[0:1], stats[1:2], stats[2:3], stats[3:4]

        keys_c = pl.ds(pl.multiple_of(j_c * blk, blk), blk)
        pv = jnp.dot(v_ref[:, keys_c], p_a[...], preferred_element_type=f32)
        acc_o[...] = acc_o[...] * alpha_c + pv

        first = j_b == 0
        m_prev = jnp.where(first, MASKED, m_old)
        m_new = jnp.maximum(m_prev, top)
        alpha_b = jnp.where(first, 0.0, jnp.exp2((m_prev - m_new) * scale))
        part = jnp.zeros((8, blk), f32)
        for g in range(blk // sub):
            p = jnp.exp2((s_b[g * sub:(g + 1) * sub, :] - m_new) * scale)
            part = part + jnp.sum(fold(p), axis=0)
            p_b[g * sub:(g + 1) * sub, :] = p.astype(bf16)
        l_new = l_old * alpha_b + jnp.sum(part, axis=0, keepdims=True)

        cols_a = pl.ds(pl.multiple_of(i_a * blk, blk), blk)
        pos = pos_ref[0:1, cols_a].astype(i32)
        first_key = i_a * blk + lax.broadcasted_iota(i32, (1, blk), 1) - pos - j_a * blk
        reach = pos.astype(jnp.uint32)
        peak = jnp.full((8, blk), MASKED, f32)
        wide = blk // 2
        for h in range(2):
            keys_a = pl.ds(pl.multiple_of(j_a * blk + h * wide, wide), wide)
            s = jnp.dot(k_ref[keys_a, :], q_ref[:, cols_a], preferred_element_type=f32)
            for g in range(wide // sub):
                back = row_id - (first_key - (h * wide + g * sub))
                kept = jnp.where(back.astype(jnp.uint32) <= reach, s[g * sub:(g + 1) * sub], MASKED)
                peak = jnp.maximum(peak, jnp.max(fold(kept), axis=0))
                s_a[h * wide + g * sub:h * wide + (g + 1) * sub, :] = kept
        top_new = jnp.max(peak, axis=0, keepdims=True)

        @pl.when(i_done >= 0)
        def _():
            send_block(i_done)

        done = (t >= 2) & (t < n_pairs + 2) & (j_c == i_c)

        @pl.when(done)
        def _():
            o_buf[pl.ds(pl.multiple_of(i_c * blk, blk), blk), :] = (acc_o[...] / stats[1:2]).T.astype(bf16)

        stats[0:1] = m_new
        stats[1:2] = l_new
        stats[2:3] = top_new
        stats[3:4] = alpha_b

        last = j_a == i_a
        n_next = jnp.where(last, jnp.minimum(n_a + 1, n_blk - 1), n_a)
        i_next = block_of(n_next)
        j_next = jnp.where(last, 0, j_a + 1)
        return (n_next, i_next, j_next), (i_a, j_a), (i_b, j_b), jnp.where(done, i_c, -1)

    zero = jnp.int32(0)
    def two(u, carry):
        carry = body(2 * u, s_even, s_odd, p_even, p_odd, carry)
        return body(2 * u + 1, s_odd, s_even, p_odd, p_even, carry)

    lax.fori_loop(0, (n_pairs + 4) // 2, two, ((zero, block_of(zero), zero), (zero, zero), (zero, zero), jnp.int32(-1)))

    def forward(n):
        at = o_all.at[line_of(n), :, core]
        return pltpu.make_async_remote_copy(
            src_ref=at, dst_ref=at, send_sem=fwd_send.at[n], recv_sem=fwd_recv.at[n], device_id=partner, device_id_type=mesh_id)

    def arrive(n, n_heads):
        at = o_all.at[line_of(n), pl.ds(0, n_heads), core]
        pltpu.make_async_copy(at, at, recv_sem.at[line_of(n)]).wait()
        forward(n).start()

    arrive(0, RING - 1)

    @pl.loop(0, lines)
    def _(n):
        @pl.when(n + 1 < lines)
        def _():
            arrive(n + 1, RING)

        forward(n).wait_recv()
        w_copy(n).wait()
        line = line_of(n)
        lhs = jnp.concatenate([o_all[line, i, j] for i in range(RING) for j in range(CORES)], axis=1)
        acc[...] += jnp.dot(lhs, w_buf[lax.rem(n, n_buf)], preferred_element_type=f32)

        @pl.when(n + n_buf < lines)
        def _():
            w_copy(n + n_buf).start()

    own_rows = chip_rows // CORES
    y_half[...] = acc[...].astype(bf16)
    swap = pltpu.make_async_remote_copy(
        src_ref=y_half.at[pl.ds(pl.multiple_of((1 - core) * own_rows, own_rows), own_rows), :], dst_ref=y_in,
        send_sem=y_sem.at[0], recv_sem=y_sem.at[1], device_id=partner, device_id_type=mesh_id)
    swap.start()
    mine = y_half[pl.ds(pl.multiple_of(core * own_rows, own_rows), own_rows), :]
    swap.wait_recv()
    other = y_in[...]
    y_ref[:, :cols] = jnp.where(core == 0, mine, other)
    y_ref[:, cols:] = jnp.where(core == 0, other, mine)
    swap.wait_send()

    @pl.loop(0, lines)
    def _(n):
        forward(n).wait_send()

    everything = o_buf.at[pl.ds(0, (n_chips - 1) * chip_rows), :]
    pltpu.make_async_copy(everything, everything, send_sem).wait()


def attend_project(qt, k, vt, pos_rows, w_o, blk, group_size, n_buf):
    tok = k.shape[0]
    own_rows = tok // group_size
    dim = w_o.shape[1]
    lines = RING * RING
    w_rows = w_o.shape[0] // lines
    half = dim // CORES
    f32, bf16 = jnp.float32, jnp.bfloat16
    vm = pl.BlockSpec(memory_space=pltpu.VMEM)
    return pl.pallas_call(
        functools.partial(attend_kernel, blk=blk, n_buf=n_buf),
        name="attend_project",
        out_shape=jax.ShapeDtypeStruct((own_rows, dim), bf16),
        in_specs=[vm, vm, vm, vm, pl.BlockSpec(memory_space=pl.ANY)],
        out_specs=vm,
        scratch_shapes=[
            pltpu.VMEM((blk, blk), f32),
            pltpu.VMEM((blk, blk), f32),
            pltpu.VMEM((blk, blk), bf16),
            pltpu.VMEM((blk, blk), bf16),
            pltpu.VMEM((VALUE_DIM, blk), f32),
            pltpu.VMEM((8, blk), f32),
            pltpu.VMEM((tok, VALUE_DIM), bf16),
            pltpu.VMEM((lines, RING, CORES, CORES * own_rows, VALUE_DIM), bf16),
            pltpu.VMEM((n_buf, w_rows, half), bf16),
            pltpu.VMEM((CORES * own_rows, half), f32),
            pltpu.VMEM((CORES * own_rows, half), bf16),
            pltpu.VMEM((own_rows, half), bf16),
            pltpu.SemaphoreType.DMA((n_buf,)),
            pltpu.SemaphoreType.DMA,
            pltpu.SemaphoreType.DMA((lines,)),
            pltpu.SemaphoreType.DMA((lines,)),
            pltpu.SemaphoreType.DMA((lines,)),
            pltpu.SemaphoreType.DMA((2,)),
        ],
        cost_estimate=pl.CostEstimate(flops=14_000_000_000, bytes_accessed=70_000_000, transcendentals=9_000_000),
        compiler_params=pltpu.CompilerParams(collective_id=3, has_side_effects=True, vmem_limit_bytes=58 << 20),
    )(qt, k, vt, pos_rows, w_o)


def ffn_kernel(y_ref, g_ref, *rest, dim, pad, sub, tile_n):
    n_wt = 5
    weights = rest[:n_wt]
    (out_ref, ybuf, wgu, wdn, hbuf, gubuf, part, far_l, far_r, in_l, in_r, far2_l, far2_r, in2_l, in2_r,
     w_sem, wx_send, wx_recv, ag_send, ag_recv, rs_send, rs_recv) = rest[n_wt:]
    coord = my_coord()

    def device(axis, by):
        c = {**coord, axis: lax.rem(coord[axis] + (by % RING), RING) if axis != "core" else 1 - coord[axis]}
        return {"sp": ((c["z"] * RING + c["y"]) * RING + c["x"]) * CORES + c["core"]}

    x_up, x_dn, y_up, y_dn = device("x", 1), device("x", -1), device("y", 1), device("y", -1)
    z_up, z_dn, partner = device("z", 1), device("z", -1), device("core", 1)
    up1, dn1, up2, dn2 = (x_up, y_up), (x_dn, y_dn), (y_up, x_up), (y_dn, x_dn)

    barrier = pltpu.get_barrier_semaphore()
    for nb in (x_up, x_dn, y_up, y_dn, z_up, z_dn, partner):
        pl.semaphore_signal(barrier, inc=1, device_id=nb, device_id_type=pl.DeviceIdType.MESH)

    w_copies = []

    def fetch(src, dst):
        cp = pltpu.make_async_copy(src, dst, w_sem.at[len(w_copies)])
        cp.start()
        w_copies.append(cp)

    up0 = 8 * pad
    own, left_a, left_b, right_a, right_b = weights
    cut = left_a.shape[0]
    fetch(own.at[0:pad], wgu.at[0:pad])
    fetch(own.at[pad:2 * pad], wgu.at[up0:up0 + pad])
    fetch(own.at[2 * pad:], wdn.at[0:pad])
    for n, (part_a, part_b) in ((1, (left_a, left_b)), (2, (right_a, right_b))):
        r = n * pad
        fetch(part_a.at[0:pad], wgu.at[r:r + pad])
        fetch(part_a.at[pad:cut], wgu.at[up0 + r:up0 + r + cut - pad])
        fetch(part_b.at[0:2 * pad - cut], wgu.at[up0 + r + cut - pad:up0 + r + pad])
        fetch(part_b.at[2 * pad - cut:], wdn.at[r:r + pad])

    wx_copies = []

    def exchange(buf, src, dst, rows, dev):
        n = len(wx_copies)
        cp = pltpu.make_async_remote_copy(
            src_ref=buf.at[src:src + rows], dst_ref=buf.at[dst:dst + rows], send_sem=wx_send.at[n], recv_sem=wx_recv.at[n],
            device_id=dev, device_id_type=pl.DeviceIdType.MESH)
        cp.start()
        wx_copies.append(cp)

    for h in range(2):
        ybuf[h, 0] = y_ref[h * sub:(h + 1) * sub, :]
    pl.semaphore_wait(barrier, 7)

    cols = (slice(0, dim // 2), slice(dim // 2, dim))
    ag_copies = {}
    ag_n = [0]

    def ag_send_to(h, src_slot, dst_slot, dev, col=None):
        c = slice(None) if col is None else cols[col]
        key = (h, dst_slot, col)
        rsem = dst_slot if col != 1 else RING * RING
        cp = pltpu.make_async_remote_copy(
            src_ref=ybuf.at[h, src_slot, :, c], dst_ref=ybuf.at[h, dst_slot, :, c],
            send_sem=ag_send.at[ag_n[0]], recv_sem=ag_recv.at[h, rsem],
            device_id=dev, device_id_type=pl.DeviceIdType.MESH)
        ag_n[0] += 1
        cp.start()
        ag_copies[key] = cp

    far = 2
    for h in range(2):
        ag_send_to(h, 0, 3 * RING, up1[h])
        ag_send_to(h, 0, 1 * RING, dn1[h])
    for h in range(2):
        ag_send_to(h, 0, 3, up2[h])
        ag_send_to(h, 0, 1, dn2[h])
    for cp in w_copies:
        cp.wait()
    split = cut - pad
    exchange(wgu, pad, 3 * pad, pad, z_up)
    exchange(wgu, up0 + pad, up0 + 3 * pad, split, z_up)
    exchange(wgu, up0 + 2 * pad + split, up0 + 3 * pad + split, pad - split, z_dn)
    exchange(wdn, 2 * pad, 3 * pad, pad, z_dn)
    exchange(wgu, 0, 4 * pad, 3 * pad, partner)
    exchange(wgu, up0, up0 + 4 * pad, 3 * pad, partner)
    exchange(wdn, 0, 4 * pad, 3 * pad, partner)
    for h in range(2):
        ag_copies[(h, 3 * RING, None)].wait_recv()
        ag_send_to(h, 3 * RING, far * RING, up1[h], 0)
        ag_copies[(h, 1 * RING, None)].wait_recv()
        ag_send_to(h, 1 * RING, far * RING, dn1[h], 1)
        for d1 in (3, 1):
            ag_send_to(h, d1 * RING, d1 * RING + 3, up2[h])
            ag_send_to(h, d1 * RING, d1 * RING + 1, dn2[h])
    for h in range(2):
        ag_copies[(h, far * RING, 0)].wait_recv()
        ag_copies[(h, far * RING, 1)].wait_recv()
        ag_send_to(h, far * RING, far * RING + 3, up2[h])
        ag_send_to(h, far * RING, far * RING + 1, dn2[h])
    for d1, d2, dev in ((0, 3, up2), (3, 3, up2), (1, 1, dn2), (2, 1, dn2)):
        for h in range(2):
            ag_copies[(h, d1 * RING + d2, None)].wait_recv()
            ag_send_to(h, d1 * RING + d2, d1 * RING + far, dev[h])
    for d1, d2 in ((0, 1), (3, 1), (1, 3), (2, 3), (0, 2), (3, 2), (1, 2), (2, 2)):
        for h in range(2):
            ag_copies[(h, d1 * RING + d2, None)].wait_recv()

    for n in range(4):
        wx_copies[n].wait_recv()
    exchange(wgu, 3 * pad, 7 * pad, pad, partner)
    exchange(wgu, up0 + 3 * pad, up0 + 7 * pad, pad, partner)
    exchange(wdn, 3 * pad, 7 * pad, pad, partner)
    for n in range(4, 10):
        wx_copies[n].wait_recv()

    rows = 2 * RING * sub
    nt = (((1,), (1,)), ((), ()))
    ff_pad = 8 * pad

    def compute(d1):
        for h in range(2):
            for d2 in range(RING):
                v = ybuf[h, d1 * RING + d2].astype(jnp.float32)
                mean_sq = jnp.mean(v * v, axis=-1, keepdims=True)
                r = (h * RING + d2) * sub
                hbuf[r:r + sub, :] = (v * lax.rsqrt(mean_sq + 1e-6) * g_ref[...].astype(jnp.float32)).astype(jnp.bfloat16)
        n_gu = gubuf.shape[1] // tile_n

        @pl.loop(0, n_gu)
        def _(j):
            c = pl.ds(pl.multiple_of(j * tile_n, tile_n), tile_n)
            gubuf[:, c] = lax.dot_general(hbuf[...], wgu[c, :], nt, preferred_element_type=jnp.float32)

        gate = gubuf[:, :ff_pad]
        act = (gate * jax.nn.sigmoid(gate) * gubuf[:, ff_pad:]).astype(jnp.bfloat16)
        wide = dim // 7 if dim % (7 * 128) == 0 else dim
        for j in range(dim // wide):
            c = slice(j * wide, (j + 1) * wide)
            res = jnp.dot(act, wdn[:, c], preferred_element_type=jnp.float32)
            for h in range(2):
                for d2 in range(RING):
                    r = (h * RING + d2) * sub
                    part[h, d1 * RING + d2, :, c] = res[r:r + sub]

    rs_copies = {}
    rs_n = [0]

    def rs_send_to(key, src, dst, dev):
        cp = pltpu.make_async_remote_copy(
            src_ref=src, dst_ref=dst, send_sem=rs_send.at[rs_n[0]], recv_sem=rs_recv.at[rs_n[0]],
            device_id=dev, device_id_type=pl.DeviceIdType.MESH)
        rs_n[0] += 1
        cp.start()
        rs_copies[key] = cp

    order = (2, 1, 3, 0)
    compute(far)
    for d2 in order:
        for h in range(2):
            rs_send_to(("fl", h, d2), part.at[h, far * RING + d2, :, cols[0]], far_l.at[h, d2], up1[h])
            rs_send_to(("fr", h, d2), part.at[h, far * RING + d2, :, cols[1]], far_r.at[h, d2], dn1[h])
    compute(1)
    compute(3)
    for d2 in order:
        for h in range(2):
            rs_copies[("fl", h, d2)].wait_recv()
            part[h, RING + d2, :, cols[0]] += far_l[h, d2]
            rs_send_to(("il", h, d2), part.at[h, RING + d2], in_l.at[h, d2], up1[h])
            rs_copies[("fr", h, d2)].wait_recv()
            part[h, 3 * RING + d2, :, cols[1]] += far_r[h, d2]
            rs_send_to(("ir", h, d2), part.at[h, 3 * RING + d2], in_r.at[h, d2], dn1[h])
    compute(0)

    def first_sum(h, d2):
        rs_copies[("il", h, d2)].wait_recv()
        rs_copies[("ir", h, d2)].wait_recv()
        part[h, d2] = part[h, d2] + in_l[h, d2] + in_r[h, d2]

    for h in range(2):
        first_sum(h, 2)
        rs_send_to(("gl", h), part.at[h, 2, :, cols[0]], far2_l.at[h], up2[h])
        rs_send_to(("gr", h), part.at[h, 2, :, cols[1]], far2_r.at[h], dn2[h])
    for h in range(2):
        first_sum(h, 1)
        rs_copies[("gl", h)].wait_recv()
        part[h, 1, :, cols[0]] += far2_l[h]
        rs_send_to(("jl", h), part.at[h, 1], in2_l.at[h], up2[h])
        first_sum(h, 3)
        rs_copies[("gr", h)].wait_recv()
        part[h, 3, :, cols[1]] += far2_r[h]
        rs_send_to(("jr", h), part.at[h, 3], in2_r.at[h], dn2[h])
    for h in range(2):
        first_sum(h, 0)
        rs_copies[("jl", h)].wait_recv()
        rs_copies[("jr", h)].wait_recv()
        total = part[h, 0] + in2_l[h] + in2_r[h]
        out_ref[h * sub:(h + 1) * sub, :] = (ybuf[h, 0].astype(jnp.float32) + total).astype(jnp.bfloat16)
    for cp in wx_copies + list(ag_copies.values()) + list(rs_copies.values()):
        cp.wait_send()


def ffn(y_own, g_ffn, weights, pad):
    rows, dim = y_own.shape
    sub = rows // 2
    chunk = 2 * RING * sub
    f32, bf16 = jnp.float32, jnp.bfloat16
    vm = pl.BlockSpec(memory_space=pltpu.VMEM)
    hbm = pl.BlockSpec(memory_space=pl.ANY)
    half = dim // 2
    return pl.pallas_call(
        functools.partial(ffn_kernel, dim=dim, pad=pad, sub=sub, tile_n=256 if (16 * pad) % 256 == 0 else 16 * pad),
        name="ffn",
        out_shape=jax.ShapeDtypeStruct((rows, dim), bf16),
        in_specs=[vm, vm] + [hbm] * 5,
        out_specs=vm,
        scratch_shapes=[
            pltpu.VMEM((2, RING * RING, sub, dim), bf16),
            pltpu.VMEM((16 * pad, dim), bf16),
            pltpu.VMEM((8 * pad, dim), bf16),
            pltpu.VMEM((chunk, dim), bf16),
            pltpu.VMEM((chunk, 16 * pad), f32),
            pltpu.VMEM((2, RING * RING, sub, dim), f32),
            pltpu.VMEM((2, RING, sub, half), f32),
            pltpu.VMEM((2, RING, sub, half), f32),
            pltpu.VMEM((2, RING, sub, dim), f32),
            pltpu.VMEM((2, RING, sub, dim), f32),
            pltpu.VMEM((2, sub, half), f32),
            pltpu.VMEM((2, sub, half), f32),
            pltpu.VMEM((2, sub, dim), f32),
            pltpu.VMEM((2, sub, dim), f32),
            pltpu.SemaphoreType.DMA((11,)),
            pltpu.SemaphoreType.DMA((10,)),
            pltpu.SemaphoreType.DMA((10,)),
            pltpu.SemaphoreType.DMA((32,)),
            pltpu.SemaphoreType.DMA((2, RING * RING + 1)),
            pltpu.SemaphoreType.DMA((40,)),
            pltpu.SemaphoreType.DMA((40,)),
        ],
        cost_estimate=pl.CostEstimate(flops=7_000_000_000, bytes_accessed=14_000_000, transcendentals=0),
        compiler_params=pltpu.CompilerParams(collective_id=1, has_side_effects=True, vmem_limit_bytes=56 << 20),
    )(y_own, g_ffn[None, :], *weights)


def weight_block(w_gate, w_up, w_down):
    cols = w_down.shape[0]
    pad = -(-cols // 16) * 16
    wide = lambda w: jnp.pad(w, ((0, pad - cols), (0, 0)))
    return jnp.concatenate([wide(w_gate.T), wide(w_up.T), wide(w_down)], axis=0), pad


def from_z_neighbours(block, group_size):
    plane = RING * RING * CORES
    up = [(d, (d + plane) % group_size) for d in range(group_size)]
    down = [(d, (d - plane) % group_size) for d in range(group_size)]
    return lax.ppermute(block, 'sp', up), lax.ppermute(block, 'sp', down)


def solution(mesh):
    group_size = mesh.shape['sp']
    tok_spec = P(('dp', 'sp'), None)
    row_spec = P(('dp', 'sp'))
    full_spec = P()
    col_spec = P(None, 'sp')

    def device_fn(x_blk, seg_blk, pos_blk, w_dq, g_q, w_uq, w_dkv, g_kv, w_ukv, w_o, g_ffn, w_gate, w_up, w_down):
        blk_len = x_blk.shape[0]
        tok_total = blk_len * group_size
        w_own, pad = weight_block(w_gate, w_up, w_down)
        cut = pad + (pad // 2) // 16 * 16
        left_a, right_a = from_z_neighbours(w_own[:cut], group_size)

        q_lin = jnp.dot(x_blk, w_dq, preferred_element_type=jnp.float32)
        c_q = rms_norm(q_lin, g_q).astype(jnp.bfloat16)
        kv_lin = jnp.dot(x_blk, w_dkv, preferred_element_type=jnp.float32)
        c_kv = rms_norm(kv_lin[:, :KV_LATENT], g_kv).astype(jnp.bfloat16)
        k_rope = apply_rope(kv_lin[:, KV_LATENT:], pos_blk).astype(jnp.bfloat16)
        pos_hi = (pos_blk // 64).astype(jnp.bfloat16)[:, None]
        pos_lo = (pos_blk % 64).astype(jnp.bfloat16)[:, None]
        spare = jnp.zeros((blk_len, NOPE_DIM - ROPE_DIM - 2), jnp.bfloat16)
        split = KV_LATENT
        q_rest = jnp.concatenate([c_q[:, split:], k_rope, pos_hi, pos_lo, spare], axis=1)
        blk = min(512, tok_total)
        qt, k, vt, pos_rows = gather_qkv(c_kv, c_q[:, :split], q_rest, w_uq, w_ukv, tok_total, blk)
        w_late, pos_rows = lax.optimization_barrier((w_own[cut:], pos_rows))
        left_b, right_b = from_z_neighbours(w_late, group_size)
        y_att = attend_project(qt, k, vt, pos_rows, w_o, blk, group_size, 11)
        return ffn(y_att, g_ffn, (w_own, left_a, left_b, right_a, right_b), pad)

    return jax.shard_map(device_fn, mesh=mesh, in_specs=(tok_spec, row_spec, row_spec, full_spec, full_spec, col_spec, full_spec, full_spec, col_spec, full_spec, full_spec, col_spec, col_spec, P('sp', None)), out_specs=tok_spec, check_vma=False)
```

```python
import functools

import jax
import jax.numpy as jnp
from jax import lax
from jax.experimental import pallas as pl
from jax.experimental.pallas import tpu as pltpu
from jax.sharding import PartitionSpec as P

NOPE_DIM = 128
ROPE_DIM = 64
VALUE_DIM = 128
KV_LATENT = 512
QK_DIM = NOPE_DIM + ROPE_DIM
KV_DIM = NOPE_DIM + VALUE_DIM
SCORE_SCALE = QK_DIM ** -0.5
LOG2E = 1.4426950408889634
MASKED = -0.7 * 3.4028234663852886e38

RING = 4
CORES = 2


def rms_norm(vec_in, gain_vec):
    mean_sq = jnp.mean(vec_in * vec_in, axis=-1, keepdims=True)
    return vec_in * lax.rsqrt(mean_sq + 1e-6) * gain_vec.astype(jnp.float32)


def rope_angles(positions):
    half_dim = ROPE_DIM // 2
    inv_freq = 10000.0 ** (-jnp.arange(half_dim, dtype=jnp.float32) / half_dim)
    return positions.astype(jnp.float32)[..., None] * inv_freq


def apply_rope(vec_in, positions):
    half_dim = ROPE_DIM // 2
    angles = rope_angles(positions)
    cosine = jnp.cos(angles)
    sine_v = jnp.sin(angles)
    lo_half = vec_in[..., :half_dim]
    hi_half = vec_in[..., half_dim:]
    return jnp.concatenate([lo_half * cosine - hi_half * sine_v, hi_half * cosine + lo_half * sine_v], axis=-1)


GATHER_ORDERS = (("z", "x", "y"), ("z", "y", "x"))


def gather_kernel_copies(bufs, coord, send_sem, recv_sem, fill_own, on_z_free, on_plane):
    core = coord["core"]

    def device(**moved):
        c = {**coord, **moved}
        return {"sp": ((c["z"] * RING + c["y"]) * RING + c["x"]) * CORES + c["core"]}

    def step(axis, by):
        return lax.rem(coord[axis] + (by % RING), RING)

    up = {a: device(**{a: step(a, 1)}) for a in "xyz"}
    down = {a: device(**{a: step(a, -1)}) for a in "xyz"}
    partner = device(core=1 - core)

    barrier = pltpu.get_barrier_semaphore()
    for nb in list(up.values()) + list(down.values()) + [partner]:
        pl.semaphore_signal(barrier, inc=1, device_id=nb, device_id_type=pl.DeviceIdType.MESH)
    fill_own()
    pl.semaphore_wait(barrier, 7)

    copies = [{} for _ in bufs]

    def send(p, key, dev, rows=None, **at):
        idx = tuple(slice(None) if at.get(a, 0) is None else at.get(a, coord[a]) for a in "zyx") + (core,)
        if rows is not None:
            idx = idx + (rows,)
        n = len(copies[p])
        cp = pltpu.make_async_remote_copy(
            src_ref=bufs[p].at[idx], dst_ref=bufs[p].at[idx], send_sem=send_sem.at[p, n], recv_sem=recv_sem.at[p, n],
            device_id=dev, device_id_type=pl.DeviceIdType.MESH)
        cp.start()
        copies[p][key] = cp

    n_p = len(bufs)
    pieces = range(n_p)
    half = bufs[0].shape[4] // 2
    order = (0, -1, 1, 2)

    def along_b(p, da):
        a, b, _ = GATHER_ORDERS[p]
        send(p, ("b+", da), up[b], **{a: step(a, da)})
        send(p, ("b-", da), down[b], **{a: step(a, da)})

    def along_d(p, db):
        a, b, d = GATHER_ORDERS[p]
        send(p, ("d+", db), up[d], **{a: None, b: step(b, db)})
        send(p, ("d-", db), down[d], **{a: None, b: step(b, db)})
        to_partner(p, db, 0)

    def to_partner(p, db, dd):
        a, b, d = GATHER_ORDERS[p]
        send(p, ("p", db, dd), partner, **{a: None, b: step(b, db), d: step(d, dd)})

    for p in pieces:
        a, b, d = GATHER_ORDERS[p]
        send(p, "a+", up[a])
        send(p, "a-", down[a])
        along_b(p, 0)
    for p in pieces:
        a, b, d = GATHER_ORDERS[p]
        copies[p]["a+"].wait_recv()
        send(p, "af+", up[a], rows=slice(0, half), **{a: step(a, -1)})
        copies[p]["a-"].wait_recv()
        send(p, "af-", down[a], rows=slice(half, 2 * half), **{a: step(a, 1)})
        along_b(p, -1)
        along_b(p, 1)
    on_z_free(up["z"], down["z"])
    for p in pieces:
        copies[p]["af+"].wait_recv()
        copies[p]["af-"].wait_recv()
        along_b(p, 2)
        along_d(p, 0)
    for p in pieces:
        a, b, d = GATHER_ORDERS[p]
        for da in (0, -1):
            copies[p][("b+", da)].wait_recv()
            send(p, ("bf+", da), up[b], **{a: step(a, da), b: step(b, -1)})
        for da in (1, 2):
            copies[p][("b-", da)].wait_recv()
            send(p, ("bf-", da), down[b], **{a: step(a, da), b: step(b, 1)})
        for da in (1, 2):
            copies[p][("b+", da)].wait_recv()
        along_d(p, -1)
        for da in (0, -1):
            copies[p][("b-", da)].wait_recv()
        along_d(p, 1)
    for p in pieces:
        for da in (0, -1):
            copies[p][("bf+", da)].wait_recv()
        for da in (1, 2):
            copies[p][("bf-", da)].wait_recv()
        along_d(p, 2)
    def whole_plane(dd):
        for db in order:
            copies[0][("p", db, dd)].wait_recv()
        on_plane(step(GATHER_ORDERS[0][2], dd))

    whole_plane(0)
    for db in order:
        for p in pieces:
            a, b, d = GATHER_ORDERS[p]
            copies[p][("d+", db)].wait_recv()
            if db in (0, -1):
                send(p, ("df+", db), up[d], **{a: None, b: step(b, db), d: step(d, -1)})
            to_partner(p, db, -1)
            copies[p][("d-", db)].wait_recv()
            if db in (1, 2):
                send(p, ("df-", db), down[d], **{a: None, b: step(b, db), d: step(d, 1)})
            to_partner(p, db, 1)
    whole_plane(-1)
    whole_plane(1)
    for db in order:
        for p in pieces:
            copies[p][("df+" if db in (0, -1) else "df-", db)].wait_recv()
            to_partner(p, db, 2)
    whole_plane(2)
    for p in pieces[1:]:
        for db in order:
            for dd in order:
                copies[p][("p", db, dd)].wait_recv()
    for p in pieces:
        for cp in copies[p].values():
            cp.wait_send()


GATHER_COPIES = 44


def my_coord():
    me = lax.axis_index("sp")
    return {
        "core": lax.rem(me, CORES),
        "x": lax.rem(me // CORES, RING),
        "y": lax.rem(me // (CORES * RING), RING),
        "z": me // (CORES * RING * RING),
    }


def qkv_kernel(kv_own, q_own, wq, wk, wv, inv_freq, pick, w_own, qt_out, k_out, vt_out, pos_out, w_left, w_right,
               kv_buf, q_buf, trig, send_sem, recv_sem, w_sem, *, blk):
    coord = my_coord()

    def fill_own():
        at = (coord["z"], coord["y"], coord["x"], coord["core"])
        kv_buf[at] = kv_own[...]
        q_buf[at] = q_own[...]

    nt = (((1,), (1,)), ((), ()))
    half = ROPE_DIM // 2
    f32, bf16 = jnp.float32, jnp.bfloat16
    row_tok = RING * CORES * kv_own.shape[0]
    w_copies = []

    def send_weights(up, down):
        for n, (dst, dev) in enumerate(((w_left, up), (w_right, down))):
            cp = pltpu.make_async_remote_copy(
                src_ref=w_own, dst_ref=dst, send_sem=w_sem.at[0, n], recv_sem=w_sem.at[1, n],
                device_id=dev, device_id_type=pl.DeviceIdType.MESH)
            cp.start()
            w_copies.append(cp)

    def keys_values(y):
        @pl.loop(0, RING)
        def _(z):
            lat = kv_buf[z, y].reshape(row_tok, kv_own.shape[1])
            tail = lat[:, KV_LATENT:]
            lat = lat[:, :KV_LATENT]
            rows = pl.ds(pl.multiple_of((z * RING + y) * row_tok, row_tok), row_tok)
            k_out[rows, :NOPE_DIM] = jnp.dot(lat, wk[...], preferred_element_type=f32).astype(bf16)
            k_out[rows, NOPE_DIM:] = tail
            vt_out[:, rows] = lax.dot_general(wv[...], lat, nt, preferred_element_type=f32).astype(bf16)
            pos = lax.dot_general(pick[...], tail, nt, preferred_element_type=f32)
            pos_out[:, rows] = pos
            angle = inv_freq[...] * pos[0:1]
            trig[:half, rows] = jnp.cos(angle)
            trig[half:, rows] = jnp.sin(angle)

    gather_kernel_copies((kv_buf, q_buf), coord, send_sem, recv_sem, fill_own, send_weights, keys_values)

    lines = blk // row_tok
    per_z = RING // lines

    @pl.loop(0, qt_out.shape[1] // blk)
    def _(n):
        at = (n // per_z, pl.ds(lax.rem(n, per_z) * lines, lines))
        lat = q_buf[at].reshape(blk, q_own.shape[1])
        rows = pl.ds(pl.multiple_of(n * blk, blk), blk)
        cosine, sine = trig[:half, rows], trig[half:, rows]
        qt = lax.dot_general(wq[...], lat, nt, preferred_element_type=f32)
        lo, hi = qt[NOPE_DIM:NOPE_DIM + half], qt[NOPE_DIM + half:]
        qt_out[:NOPE_DIM, rows] = qt[:NOPE_DIM].astype(bf16)
        qt_out[NOPE_DIM:NOPE_DIM + half, rows] = (lo * cosine - hi * sine).astype(bf16)
        qt_out[NOPE_DIM + half:QK_DIM, rows] = (hi * cosine + lo * sine).astype(bf16)
        qt_out[QK_DIM:, rows] = jnp.zeros((2 * NOPE_DIM - QK_DIM, blk), bf16)

    for cp in w_copies:
        cp.wait()


def gather_qkv(kv_own, q_own, w_uq, w_ukv, w_own, tok_total, blk):
    rows = kv_own.shape[0]
    f32, bf16 = jnp.float32, jnp.bfloat16
    half = ROPE_DIM // 2
    inv_freq = 10000.0 ** (-jnp.arange(half, dtype=f32) / half)
    lane = jnp.arange(NOPE_DIM)[None, :]
    pick = jnp.where(jnp.arange(8)[:, None] == 0, jnp.where(lane == ROPE_DIM, 64.0, jnp.where(lane == ROPE_DIM + 1, 1.0, 0.0)), 0.0).astype(bf16)
    vm = pl.BlockSpec(memory_space=pltpu.VMEM)
    hbm = pl.BlockSpec(memory_space=pl.ANY)
    n_p = len(GATHER_ORDERS)
    buf = lambda own: pltpu.VMEM((RING, RING, RING, CORES, rows, own.shape[1]), bf16)
    return pl.pallas_call(
        functools.partial(qkv_kernel, blk=blk),
        name="gather_qkv",
        out_shape=(
            jax.ShapeDtypeStruct((2 * NOPE_DIM, tok_total), bf16),
            jax.ShapeDtypeStruct((tok_total, 2 * NOPE_DIM), bf16),
            jax.ShapeDtypeStruct((VALUE_DIM, tok_total), bf16),
            jax.ShapeDtypeStruct((8, tok_total), f32),
            jax.ShapeDtypeStruct(w_own.shape, bf16),
            jax.ShapeDtypeStruct(w_own.shape, bf16),
        ),
        in_specs=[vm] * 7 + [hbm],
        out_specs=(vm,) * 4 + (hbm,) * 2,
        scratch_shapes=[
            buf(kv_own), buf(q_own),
            pltpu.VMEM((ROPE_DIM, tok_total), f32),
            pltpu.SemaphoreType.DMA((n_p, GATHER_COPIES)),
            pltpu.SemaphoreType.DMA((n_p, GATHER_COPIES)),
            pltpu.SemaphoreType.DMA((2, 2)),
        ],
        cost_estimate=pl.CostEstimate(flops=4_000_000_000, bytes_accessed=6_000_000, transcendentals=0),
        compiler_params=pltpu.CompilerParams(collective_id=2, has_side_effects=True, vmem_limit_bytes=40 << 20),
    )(kv_own, q_own, w_uq.T, w_ukv[:, :NOPE_DIM], w_ukv[:, NOPE_DIM:].T, inv_freq[:, None], pick, w_own)


SUB_KEYS = 32
FAR_EVERY = 4


def attend_kernel(q_ref, k_ref, v_ref, pos_ref, wo_ref, w_left, w_right, y_ref, w_far, s_even, s_odd, p_even, p_odd, acc_o, stats, o_buf, o_all, w_buf, acc, y_half, y_in,
                  w_sem, send_sem, recv_sem, fwd_send, fwd_recv, y_sem, far_sem, *, blk, n_buf):
    coord = my_coord()
    core, x, y, z = (coord[a] for a in ("core", "x", "y", "z"))
    y_top, y_low = y // 2, lax.rem(y, 2)
    lines = RING * RING
    n_chips = lines * RING
    chip_rows = o_all.shape[3]
    w_rows, cols = w_buf.shape[1], w_buf.shape[2]
    mesh_id = pl.DeviceIdType.MESH
    n_blk = q_ref.shape[1] // blk
    n_pairs = n_blk * (n_blk + 1) // 2
    per_z = n_blk // RING
    f32, bf16, i32 = jnp.float32, jnp.bfloat16, jnp.int32
    scale = SCORE_SCALE * LOG2E

    def line_of(n):
        step = n // 2
        return lax.rem(z + step // 2, RING) * RING + lax.rem(y_top + lax.rem(step, 2), 2) * 2 + lax.rem(y_low + lax.rem(n, 2), 2)

    def block_of(n):
        return lax.rem(z + RING - n // per_z, RING) * per_z + lax.rem(y_top + lax.rem(n, per_z), per_z)

    def w_copy(n):
        rows = pl.ds(pl.multiple_of(line_of(n) * w_rows, w_rows), w_rows)
        side = pl.ds(pl.multiple_of(core * cols, 128), cols)
        slot = lax.rem(n, n_buf)
        return pltpu.make_async_copy(wo_ref.at[rows, side], w_buf.at[slot], w_sem.at[slot])

    @pl.loop(0, n_buf)
    def _(n):
        w_copy(n).start()

    me_chip = (z * RING + y) * RING + x
    my_line = z * RING + y
    partner = {"sp": me_chip * CORES + 1 - core}

    far_rows = 16
    far_n = w_far.shape[0] // far_rows
    far_cut = far_n // 2
    z_up = {"sp": lax.rem(me_chip + lines, n_chips) * CORES + core}
    z_dn = {"sp": lax.rem(me_chip + n_chips - lines, n_chips) * CORES + core}

    def far_copy(src, n, dev):
        rows = pl.ds(pl.multiple_of(n * far_rows, far_rows), far_rows)
        return pltpu.make_async_remote_copy(
            src_ref=src.at[rows, :], dst_ref=w_far.at[rows, :], send_sem=far_sem.at[0], recv_sem=far_sem.at[1],
            device_id=dev, device_id_type=mesh_id)

    def far_step(n):
        @pl.when(n < far_cut)
        def _():
            far_copy(w_left, n, z_up).start()

        @pl.when(n < far_n - far_cut)
        def _():
            far_copy(w_right, far_cut + n, z_dn).start()

    barrier = pltpu.get_barrier_semaphore()
    pl.semaphore_signal(barrier, inc=1, device_id=partner, device_id_type=mesh_id)

    @pl.loop(1, n_chips)
    def _(n):
        to = {"sp": lax.rem(me_chip + n, n_chips) * CORES + core}
        pl.semaphore_signal(barrier, inc=1, device_id=to, device_id_type=mesh_id)

    for ref in (s_even, s_odd, p_even, p_odd):
        ref[...] = jnp.zeros_like(ref)
    acc_o[...] = jnp.zeros_like(acc_o)
    stats[...] = jnp.zeros_like(stats)
    acc[...] = jnp.zeros_like(acc)
    pl.semaphore_wait(barrier, n_chips)

    chips_per_blk = blk // chip_rows

    def send_block(i):
        line0 = i * (chips_per_blk // RING)

        @pl.loop(0, chips_per_blk)
        def _(n):
            yy = line0 + lax.rem(y_low + n // RING, chips_per_blk // RING)
            to = yy * RING + lax.rem(x + lax.rem(n, RING), RING)
            rows = pl.ds(pl.multiple_of(to * chip_rows, chip_rows), chip_rows)

            @pl.when(to == me_chip)
            def _():
                o_all[my_line, x, core] = o_buf[rows, :]

            @pl.when(to != me_chip)
            def _():
                pltpu.make_async_remote_copy(
                    src_ref=o_buf.at[rows, :], dst_ref=o_all.at[my_line, x, core], send_sem=send_sem,
                    recv_sem=recv_sem.at[my_line], device_id={"sp": to * CORES + core}, device_id_type=mesh_id).start()

    sub = SUB_KEYS
    fold = lambda v: v.reshape(sub // 8, 8, blk)
    row_id = lax.broadcasted_iota(i32, (sub, blk), 0)

    def body(t, s_a, s_b, p_a, p_b, carry):
        (n_a, i_a, j_a), (i_b, j_b), (i_c, j_c), i_done = carry
        m_old, l_old, top, alpha_c = stats[0:1], stats[1:2], stats[2:3], stats[3:4]

        keys_c = pl.ds(pl.multiple_of(j_c * blk, blk), blk)
        pv = jnp.dot(v_ref[:, keys_c], p_a[...], preferred_element_type=f32)
        acc_o[...] = acc_o[...] * alpha_c + pv

        first = j_b == 0
        m_prev = jnp.where(first, MASKED, m_old)
        m_new = jnp.maximum(m_prev, top)
        alpha_b = jnp.where(first, 0.0, jnp.exp2((m_prev - m_new) * scale))
        part = jnp.zeros((8, blk), f32)
        for g in range(blk // sub):
            p = jnp.exp2((s_b[g * sub:(g + 1) * sub, :] - m_new) * scale)
            part = part + jnp.sum(fold(p), axis=0)
            p_b[g * sub:(g + 1) * sub, :] = p.astype(bf16)
        l_new = l_old * alpha_b + jnp.sum(part, axis=0, keepdims=True)

        cols_a = pl.ds(pl.multiple_of(i_a * blk, blk), blk)
        pos = pos_ref[0:1, cols_a].astype(i32)
        first_key = i_a * blk + lax.broadcasted_iota(i32, (1, blk), 1) - pos - j_a * blk
        reach = pos.astype(jnp.uint32)
        peak = jnp.full((8, blk), MASKED, f32)
        wide = blk // 2
        for h in range(2):
            keys_a = pl.ds(pl.multiple_of(j_a * blk + h * wide, wide), wide)
            s = jnp.dot(k_ref[keys_a, :], q_ref[:, cols_a], preferred_element_type=f32)
            for g in range(wide // sub):
                back = row_id - (first_key - (h * wide + g * sub))
                kept = jnp.where(back.astype(jnp.uint32) <= reach, s[g * sub:(g + 1) * sub], MASKED)
                peak = jnp.maximum(peak, jnp.max(fold(kept), axis=0))
                s_a[h * wide + g * sub:h * wide + (g + 1) * sub, :] = kept
        top_new = jnp.max(peak, axis=0, keepdims=True)

        @pl.when(i_done >= 0)
        def _():
            send_block(i_done)

        @pl.when(lax.rem(t, FAR_EVERY) == 0)
        def _():
            far_step(t // FAR_EVERY)

        done = (t >= 2) & (t < n_pairs + 2) & (j_c == i_c)

        @pl.when(done)
        def _():
            o_buf[pl.ds(pl.multiple_of(i_c * blk, blk), blk), :] = (acc_o[...] / stats[1:2]).T.astype(bf16)

        stats[0:1] = m_new
        stats[1:2] = l_new
        stats[2:3] = top_new
        stats[3:4] = alpha_b

        last = j_a == i_a
        n_next = jnp.where(last, jnp.minimum(n_a + 1, n_blk - 1), n_a)
        i_next = block_of(n_next)
        j_next = jnp.where(last, 0, j_a + 1)
        return (n_next, i_next, j_next), (i_a, j_a), (i_b, j_b), jnp.where(done, i_c, -1)

    zero = jnp.int32(0)
    def two(u, carry):
        carry = body(2 * u, s_even, s_odd, p_even, p_odd, carry)
        return body(2 * u + 1, s_odd, s_even, p_odd, p_even, carry)

    lax.fori_loop(0, (n_pairs + 4) // 2, two, ((zero, block_of(zero), zero), (zero, zero), (zero, zero), jnp.int32(-1)))

    def forward(n):
        at = o_all.at[line_of(n), :, core]
        return pltpu.make_async_remote_copy(
            src_ref=at, dst_ref=at, send_sem=fwd_send.at[n], recv_sem=fwd_recv.at[n], device_id=partner, device_id_type=mesh_id)

    def arrive(n, n_heads):
        at = o_all.at[line_of(n), pl.ds(0, n_heads), core]
        pltpu.make_async_copy(at, at, recv_sem.at[line_of(n)]).wait()
        forward(n).start()

    arrive(0, RING - 1)

    @pl.loop(0, lines)
    def _(n):
        @pl.when(n + 1 < lines)
        def _():
            arrive(n + 1, RING)

        forward(n).wait_recv()
        w_copy(n).wait()
        line = line_of(n)
        lhs = jnp.concatenate([o_all[line, i, j] for i in range(RING) for j in range(CORES)], axis=1)
        acc[...] += jnp.dot(lhs, w_buf[lax.rem(n, n_buf)], preferred_element_type=f32)

        @pl.when(n + n_buf < lines)
        def _():
            w_copy(n + n_buf).start()

    own_rows = chip_rows // CORES
    y_half[...] = acc[...].astype(bf16)
    swap = pltpu.make_async_remote_copy(
        src_ref=y_half.at[pl.ds(pl.multiple_of((1 - core) * own_rows, own_rows), own_rows), :], dst_ref=y_in,
        send_sem=y_sem.at[0], recv_sem=y_sem.at[1], device_id=partner, device_id_type=mesh_id)
    swap.start()
    mine = y_half[pl.ds(pl.multiple_of(core * own_rows, own_rows), own_rows), :]
    swap.wait_recv()
    other = y_in[...]
    y_ref[:, :cols] = jnp.where(core == 0, mine, other)
    y_ref[:, cols:] = jnp.where(core == 0, other, mine)
    swap.wait_send()

    @pl.loop(0, lines)
    def _(n):
        forward(n).wait_send()

    everything = o_buf.at[pl.ds(0, (n_chips - 1) * chip_rows), :]
    pltpu.make_async_copy(everything, everything, send_sem).wait()
    pltpu.make_async_copy(w_far, w_far, far_sem.at[0]).wait()
    pltpu.make_async_copy(w_far, w_far, far_sem.at[1]).wait()


def attend_project(qt, k, vt, pos_rows, w_o, w_left, w_right, blk, group_size, n_buf):
    tok = k.shape[0]
    own_rows = tok // group_size
    dim = w_o.shape[1]
    lines = RING * RING
    w_rows = w_o.shape[0] // lines
    half = dim // CORES
    f32, bf16 = jnp.float32, jnp.bfloat16
    vm = pl.BlockSpec(memory_space=pltpu.VMEM)
    hbm = pl.BlockSpec(memory_space=pl.ANY)
    return pl.pallas_call(
        functools.partial(attend_kernel, blk=blk, n_buf=n_buf),
        name="attend_project",
        out_shape=(jax.ShapeDtypeStruct((own_rows, dim), bf16), jax.ShapeDtypeStruct(w_left.shape, bf16)),
        in_specs=[vm, vm, vm, vm, hbm, hbm, hbm],
        out_specs=(vm, hbm),
        scratch_shapes=[
            pltpu.VMEM((blk, blk), f32),
            pltpu.VMEM((blk, blk), f32),
            pltpu.VMEM((blk, blk), bf16),
            pltpu.VMEM((blk, blk), bf16),
            pltpu.VMEM((VALUE_DIM, blk), f32),
            pltpu.VMEM((8, blk), f32),
            pltpu.VMEM((tok, VALUE_DIM), bf16),
            pltpu.VMEM((lines, RING, CORES, CORES * own_rows, VALUE_DIM), bf16),
            pltpu.VMEM((n_buf, w_rows, half), bf16),
            pltpu.VMEM((CORES * own_rows, half), f32),
            pltpu.VMEM((CORES * own_rows, half), bf16),
            pltpu.VMEM((own_rows, half), bf16),
            pltpu.SemaphoreType.DMA((n_buf,)),
            pltpu.SemaphoreType.DMA,
            pltpu.SemaphoreType.DMA((lines,)),
            pltpu.SemaphoreType.DMA((lines,)),
            pltpu.SemaphoreType.DMA((lines,)),
            pltpu.SemaphoreType.DMA((2,)),
            pltpu.SemaphoreType.DMA((2,)),
        ],
        cost_estimate=pl.CostEstimate(flops=14_000_000_000, bytes_accessed=70_000_000, transcendentals=9_000_000),
        compiler_params=pltpu.CompilerParams(collective_id=3, has_side_effects=True, vmem_limit_bytes=58 << 20),
    )(qt, k, vt, pos_rows, w_o, w_left, w_right)


def ffn_kernel(y_ref, g_ref, *rest, dim, pad, sub, tile_n):
    n_wt = 4
    weights = rest[:n_wt]
    (out_ref, ybuf, wgu, wdn, hbuf, gubuf, part, far_l, far_r, in_l, in_r, far2_l, far2_r, in2_l, in2_r,
     w_sem, wx_send, wx_recv, ag_send, ag_recv, rs_send, rs_recv) = rest[n_wt:]
    coord = my_coord()

    def device(axis, by):
        c = {**coord, axis: lax.rem(coord[axis] + (by % RING), RING) if axis != "core" else 1 - coord[axis]}
        return {"sp": ((c["z"] * RING + c["y"]) * RING + c["x"]) * CORES + c["core"]}

    x_up, x_dn, y_up, y_dn = device("x", 1), device("x", -1), device("y", 1), device("y", -1)
    partner = device("core", 1)
    up1, dn1, up2, dn2 = (x_up, y_up), (x_dn, y_dn), (y_up, x_up), (y_dn, x_dn)

    barrier = pltpu.get_barrier_semaphore()
    for nb in (x_up, x_dn, y_up, y_dn, partner):
        pl.semaphore_signal(barrier, inc=1, device_id=nb, device_id_type=pl.DeviceIdType.MESH)

    w_copies = []

    def fetch(src, dst):
        cp = pltpu.make_async_copy(src, dst, w_sem.at[len(w_copies)])
        cp.start()
        w_copies.append(cp)

    up0 = 8 * pad
    for n, blk in enumerate(weights):
        r = n * pad
        fetch(blk.at[0:pad], wgu.at[r:r + pad])
        fetch(blk.at[pad:2 * pad], wgu.at[up0 + r:up0 + r + pad])
        fetch(blk.at[2 * pad:], wdn.at[r:r + pad])

    wx_copies = []

    def exchange(buf, src, dst, rows, dev):
        n = len(wx_copies)
        cp = pltpu.make_async_remote_copy(
            src_ref=buf.at[src:src + rows], dst_ref=buf.at[dst:dst + rows], send_sem=wx_send.at[n], recv_sem=wx_recv.at[n],
            device_id=dev, device_id_type=pl.DeviceIdType.MESH)
        cp.start()
        wx_copies.append(cp)

    for h in range(2):
        ybuf[h, 0] = y_ref[h * sub:(h + 1) * sub, :]
    pl.semaphore_wait(barrier, 5)

    cols = (slice(0, dim // 2), slice(dim // 2, dim))
    ag_copies = {}
    ag_n = [0]

    def ag_send_to(h, src_slot, dst_slot, dev, col=None):
        c = slice(None) if col is None else cols[col]
        key = (h, dst_slot, col)
        rsem = dst_slot if col != 1 else RING * RING
        cp = pltpu.make_async_remote_copy(
            src_ref=ybuf.at[h, src_slot, :, c], dst_ref=ybuf.at[h, dst_slot, :, c],
            send_sem=ag_send.at[ag_n[0]], recv_sem=ag_recv.at[h, rsem],
            device_id=dev, device_id_type=pl.DeviceIdType.MESH)
        ag_n[0] += 1
        cp.start()
        ag_copies[key] = cp

    far = 2
    for h in range(2):
        ag_send_to(h, 0, 3 * RING, up1[h])
        ag_send_to(h, 0, 1 * RING, dn1[h])
    for h in range(2):
        ag_send_to(h, 0, 3, up2[h])
        ag_send_to(h, 0, 1, dn2[h])
    for cp in w_copies:
        cp.wait()
    exchange(wgu, 0, 4 * pad, 4 * pad, partner)
    exchange(wgu, up0, up0 + 4 * pad, 4 * pad, partner)
    exchange(wdn, 0, 4 * pad, 4 * pad, partner)
    for h in range(2):
        ag_copies[(h, 3 * RING, None)].wait_recv()
        ag_send_to(h, 3 * RING, far * RING, up1[h], 0)
        ag_copies[(h, 1 * RING, None)].wait_recv()
        ag_send_to(h, 1 * RING, far * RING, dn1[h], 1)
        for d1 in (3, 1):
            ag_send_to(h, d1 * RING, d1 * RING + 3, up2[h])
            ag_send_to(h, d1 * RING, d1 * RING + 1, dn2[h])
    for h in range(2):
        ag_copies[(h, far * RING, 0)].wait_recv()
        ag_copies[(h, far * RING, 1)].wait_recv()
        ag_send_to(h, far * RING, far * RING + 3, up2[h])
        ag_send_to(h, far * RING, far * RING + 1, dn2[h])
    for d1, d2, dev in ((0, 3, up2), (3, 3, up2), (1, 1, dn2), (2, 1, dn2)):
        for h in range(2):
            ag_copies[(h, d1 * RING + d2, None)].wait_recv()
            ag_send_to(h, d1 * RING + d2, d1 * RING + far, dev[h])
    for d1, d2 in ((0, 1), (3, 1), (1, 3), (2, 3), (0, 2), (3, 2), (1, 2), (2, 2)):
        for h in range(2):
            ag_copies[(h, d1 * RING + d2, None)].wait_recv()

    for cp in wx_copies:
        cp.wait_recv()

    rows = 2 * RING * sub
    nt = (((1,), (1,)), ((), ()))
    ff_pad = 8 * pad

    def compute(d1):
        for h in range(2):
            for d2 in range(RING):
                v = ybuf[h, d1 * RING + d2].astype(jnp.float32)
                mean_sq = jnp.mean(v * v, axis=-1, keepdims=True)
                r = (h * RING + d2) * sub
                hbuf[r:r + sub, :] = (v * lax.rsqrt(mean_sq + 1e-6) * g_ref[...].astype(jnp.float32)).astype(jnp.bfloat16)
        n_gu = gubuf.shape[1] // tile_n

        @pl.loop(0, n_gu)
        def _(j):
            c = pl.ds(pl.multiple_of(j * tile_n, tile_n), tile_n)
            gubuf[:, c] = lax.dot_general(hbuf[...], wgu[c, :], nt, preferred_element_type=jnp.float32)

        gate = gubuf[:, :ff_pad]
        act = (gate * jax.nn.sigmoid(gate) * gubuf[:, ff_pad:]).astype(jnp.bfloat16)
        wide = dim // 7 if dim % (7 * 128) == 0 else dim
        for j in range(dim // wide):
            c = slice(j * wide, (j + 1) * wide)
            res = jnp.dot(act, wdn[:, c], preferred_element_type=jnp.float32)
            for h in range(2):
                for d2 in range(RING):
                    r = (h * RING + d2) * sub
                    part[h, d1 * RING + d2, :, c] = res[r:r + sub]

    rs_copies = {}
    rs_n = [0]

    def rs_send_to(key, src, dst, dev):
        cp = pltpu.make_async_remote_copy(
            src_ref=src, dst_ref=dst, send_sem=rs_send.at[rs_n[0]], recv_sem=rs_recv.at[rs_n[0]],
            device_id=dev, device_id_type=pl.DeviceIdType.MESH)
        rs_n[0] += 1
        cp.start()
        rs_copies[key] = cp

    order = (2, 1, 3, 0)
    compute(far)
    for d2 in order:
        for h in range(2):
            rs_send_to(("fl", h, d2), part.at[h, far * RING + d2, :, cols[0]], far_l.at[h, d2], up1[h])
            rs_send_to(("fr", h, d2), part.at[h, far * RING + d2, :, cols[1]], far_r.at[h, d2], dn1[h])
    compute(1)
    compute(3)
    for d2 in order:
        for h in range(2):
            rs_copies[("fl", h, d2)].wait_recv()
            part[h, RING + d2, :, cols[0]] += far_l[h, d2]
            rs_send_to(("il", h, d2), part.at[h, RING + d2], in_l.at[h, d2], up1[h])
            rs_copies[("fr", h, d2)].wait_recv()
            part[h, 3 * RING + d2, :, cols[1]] += far_r[h, d2]
            rs_send_to(("ir", h, d2), part.at[h, 3 * RING + d2], in_r.at[h, d2], dn1[h])
    compute(0)

    def first_sum(h, d2):
        rs_copies[("il", h, d2)].wait_recv()
        rs_copies[("ir", h, d2)].wait_recv()
        part[h, d2] = part[h, d2] + in_l[h, d2] + in_r[h, d2]

    for h in range(2):
        first_sum(h, 2)
        rs_send_to(("gl", h), part.at[h, 2, :, cols[0]], far2_l.at[h], up2[h])
        rs_send_to(("gr", h), part.at[h, 2, :, cols[1]], far2_r.at[h], dn2[h])
    for h in range(2):
        first_sum(h, 1)
        rs_copies[("gl", h)].wait_recv()
        part[h, 1, :, cols[0]] += far2_l[h]
        rs_send_to(("jl", h), part.at[h, 1], in2_l.at[h], up2[h])
        first_sum(h, 3)
        rs_copies[("gr", h)].wait_recv()
        part[h, 3, :, cols[1]] += far2_r[h]
        rs_send_to(("jr", h), part.at[h, 3], in2_r.at[h], dn2[h])
    for h in range(2):
        first_sum(h, 0)
        rs_copies[("jl", h)].wait_recv()
        rs_copies[("jr", h)].wait_recv()
        total = part[h, 0] + in2_l[h] + in2_r[h]
        out_ref[h * sub:(h + 1) * sub, :] = (ybuf[h, 0].astype(jnp.float32) + total).astype(jnp.bfloat16)
    for cp in wx_copies + list(ag_copies.values()) + list(rs_copies.values()):
        cp.wait_send()


def ffn(y_own, g_ffn, weights, pad):
    rows, dim = y_own.shape
    sub = rows // 2
    chunk = 2 * RING * sub
    f32, bf16 = jnp.float32, jnp.bfloat16
    vm = pl.BlockSpec(memory_space=pltpu.VMEM)
    hbm = pl.BlockSpec(memory_space=pl.ANY)
    half = dim // 2
    return pl.pallas_call(
        functools.partial(ffn_kernel, dim=dim, pad=pad, sub=sub, tile_n=256 if (16 * pad) % 256 == 0 else 16 * pad),
        name="ffn",
        out_shape=jax.ShapeDtypeStruct((rows, dim), bf16),
        in_specs=[vm, vm] + [hbm] * 4,
        out_specs=vm,
        scratch_shapes=[
            pltpu.VMEM((2, RING * RING, sub, dim), bf16),
            pltpu.VMEM((16 * pad, dim), bf16),
            pltpu.VMEM((8 * pad, dim), bf16),
            pltpu.VMEM((chunk, dim), bf16),
            pltpu.VMEM((chunk, 16 * pad), f32),
            pltpu.VMEM((2, RING * RING, sub, dim), f32),
            pltpu.VMEM((2, RING, sub, half), f32),
            pltpu.VMEM((2, RING, sub, half), f32),
            pltpu.VMEM((2, RING, sub, dim), f32),
            pltpu.VMEM((2, RING, sub, dim), f32),
            pltpu.VMEM((2, sub, half), f32),
            pltpu.VMEM((2, sub, half), f32),
            pltpu.VMEM((2, sub, dim), f32),
            pltpu.VMEM((2, sub, dim), f32),
            pltpu.SemaphoreType.DMA((12,)),
            pltpu.SemaphoreType.DMA((3,)),
            pltpu.SemaphoreType.DMA((3,)),
            pltpu.SemaphoreType.DMA((32,)),
            pltpu.SemaphoreType.DMA((2, RING * RING + 1)),
            pltpu.SemaphoreType.DMA((40,)),
            pltpu.SemaphoreType.DMA((40,)),
        ],
        cost_estimate=pl.CostEstimate(flops=7_000_000_000, bytes_accessed=14_000_000, transcendentals=0),
        compiler_params=pltpu.CompilerParams(collective_id=1, has_side_effects=True, vmem_limit_bytes=56 << 20),
    )(y_own, g_ffn[None, :], *weights)


def weight_block(w_gate, w_up, w_down):
    cols = w_down.shape[0]
    pad = -(-cols // 16) * 16
    wide = lambda w: jnp.pad(w, ((0, pad - cols), (0, 0)))
    return jnp.concatenate([wide(w_gate.T), wide(w_up.T), wide(w_down)], axis=0), pad


def solution(mesh):
    group_size = mesh.shape['sp']
    tok_spec = P(('dp', 'sp'), None)
    row_spec = P(('dp', 'sp'))
    full_spec = P()
    col_spec = P(None, 'sp')

    def device_fn(x_blk, seg_blk, pos_blk, w_dq, g_q, w_uq, w_dkv, g_kv, w_ukv, w_o, g_ffn, w_gate, w_up, w_down):
        blk_len = x_blk.shape[0]
        tok_total = blk_len * group_size
        w_own, pad = weight_block(w_gate, w_up, w_down)

        q_lin = jnp.dot(x_blk, w_dq, preferred_element_type=jnp.float32)
        c_q = rms_norm(q_lin, g_q).astype(jnp.bfloat16)
        kv_lin = jnp.dot(x_blk, w_dkv, preferred_element_type=jnp.float32)
        c_kv = rms_norm(kv_lin[:, :KV_LATENT], g_kv).astype(jnp.bfloat16)
        k_rope = apply_rope(kv_lin[:, KV_LATENT:], pos_blk).astype(jnp.bfloat16)
        pos_hi = (pos_blk // 64).astype(jnp.bfloat16)[:, None]
        pos_lo = (pos_blk % 64).astype(jnp.bfloat16)[:, None]
        spare = jnp.zeros((blk_len, NOPE_DIM - ROPE_DIM - 2), jnp.bfloat16)
        kv_blk = jnp.concatenate([c_kv, k_rope, pos_hi, pos_lo, spare], axis=1)
        blk = min(512, tok_total)
        qt, k, vt, pos_rows, w_left, w_right = gather_qkv(kv_blk, c_q, w_uq, w_ukv, w_own, tok_total, blk)
        y_att, w_far = attend_project(qt, k, vt, pos_rows, w_o, w_left, w_right, blk, group_size, 11)
        return ffn(y_att, g_ffn, (w_own, w_left, w_right, w_far), pad)

    return jax.shard_map(device_fn, mesh=mesh, in_specs=(tok_spec, row_spec, row_spec, full_spec, full_spec, col_spec, full_spec, full_spec, col_spec, full_spec, full_spec, col_spec, col_spec, P('sp', None)), out_specs=tok_spec, check_vma=False)
```

```python
import functools

import jax
import jax.numpy as jnp
from jax import lax
from jax.experimental import pallas as pl
from jax.experimental.pallas import tpu as pltpu
from jax.sharding import PartitionSpec as P

NOPE_DIM = 128
ROPE_DIM = 64
VALUE_DIM = 128
KV_LATENT = 512
QK_DIM = NOPE_DIM + ROPE_DIM
KV_DIM = NOPE_DIM + VALUE_DIM
SCORE_SCALE = QK_DIM ** -0.5
LOG2E = 1.4426950408889634
MASKED = -0.7 * 3.4028234663852886e38

RING = 4
CORES = 2


def rms_norm(vec_in, gain_vec):
    mean_sq = jnp.mean(vec_in * vec_in, axis=-1, keepdims=True)
    return vec_in * lax.rsqrt(mean_sq + 1e-6) * gain_vec.astype(jnp.float32)


GATHER_ORDERS = (("z", "x", "y"), ("z", "y", "x"))


def gather_latents(bufs, coord, send_sem, recv_sem, on_z_free, on_plane):
    core = coord["core"]

    def device(**moved):
        c = {**coord, **moved}
        return {"sp": ((c["z"] * RING + c["y"]) * RING + c["x"]) * CORES + c["core"]}

    def step(axis, by):
        return lax.rem(coord[axis] + (by % RING), RING)

    up = {a: device(**{a: step(a, 1)}) for a in "xyz"}
    down = {a: device(**{a: step(a, -1)}) for a in "xyz"}
    partner = device(core=1 - core)
    copies = [{} for _ in bufs]

    def send(p, key, dev, rows=None, **at):
        idx = tuple(slice(None) if at.get(a, 0) is None else at.get(a, coord[a]) for a in "zyx") + (core,)
        if rows is not None:
            idx = idx + (rows,)
        n = len(copies[p])
        cp = pltpu.make_async_remote_copy(
            src_ref=bufs[p].at[idx], dst_ref=bufs[p].at[idx], send_sem=send_sem.at[p, n], recv_sem=recv_sem.at[p, n],
            device_id=dev, device_id_type=pl.DeviceIdType.MESH)
        cp.start()
        copies[p][key] = cp

    n_p = len(bufs)
    pieces = range(n_p)
    half = bufs[0].shape[4] // 2
    order = (0, -1, 1, 2)

    def along_b(p, da):
        a, b, _ = GATHER_ORDERS[p]
        send(p, ("b+", da), up[b], **{a: step(a, da)})
        send(p, ("b-", da), down[b], **{a: step(a, da)})

    def along_d(p, db):
        a, b, d = GATHER_ORDERS[p]
        send(p, ("d+", db), up[d], **{a: None, b: step(b, db)})
        send(p, ("d-", db), down[d], **{a: None, b: step(b, db)})
        to_partner(p, db, 0)

    def to_partner(p, db, dd):
        a, b, d = GATHER_ORDERS[p]
        send(p, ("p", db, dd), partner, **{a: None, b: step(b, db), d: step(d, dd)})

    for p in pieces:
        a, b, d = GATHER_ORDERS[p]
        send(p, "a+", up[a])
        send(p, "a-", down[a])
        along_b(p, 0)
    for p in pieces:
        a, b, d = GATHER_ORDERS[p]
        copies[p]["a+"].wait_recv()
        send(p, "af+", up[a], rows=slice(0, half), **{a: step(a, -1)})
        copies[p]["a-"].wait_recv()
        send(p, "af-", down[a], rows=slice(half, 2 * half), **{a: step(a, 1)})
        along_b(p, -1)
        along_b(p, 1)
    on_z_free()
    for p in pieces:
        copies[p]["af+"].wait_recv()
        copies[p]["af-"].wait_recv()
        along_b(p, 2)
        along_d(p, 0)
    for p in pieces:
        a, b, d = GATHER_ORDERS[p]
        for da in (0, -1):
            copies[p][("b+", da)].wait_recv()
            send(p, ("bf+", da), up[b], **{a: step(a, da), b: step(b, -1)})
        for da in (1, 2):
            copies[p][("b-", da)].wait_recv()
            send(p, ("bf-", da), down[b], **{a: step(a, da), b: step(b, 1)})
        for da in (1, 2):
            copies[p][("b+", da)].wait_recv()
        along_d(p, -1)
        for da in (0, -1):
            copies[p][("b-", da)].wait_recv()
        along_d(p, 1)
    for p in pieces:
        for da in (0, -1):
            copies[p][("bf+", da)].wait_recv()
        for da in (1, 2):
            copies[p][("bf-", da)].wait_recv()
        along_d(p, 2)
    def whole_plane(dd):
        for db in order:
            copies[0][("p", db, dd)].wait_recv()
        on_plane(step(GATHER_ORDERS[0][2], dd))

    whole_plane(0)
    for db in order:
        for p in pieces:
            a, b, d = GATHER_ORDERS[p]
            copies[p][("d+", db)].wait_recv()
            if db in (0, -1):
                send(p, ("df+", db), up[d], **{a: None, b: step(b, db), d: step(d, -1)})
            to_partner(p, db, -1)
            copies[p][("d-", db)].wait_recv()
            if db in (1, 2):
                send(p, ("df-", db), down[d], **{a: None, b: step(b, db), d: step(d, 1)})
            to_partner(p, db, 1)
    whole_plane(-1)
    whole_plane(1)
    for db in order:
        for p in pieces:
            copies[p][("df+" if db in (0, -1) else "df-", db)].wait_recv()
            to_partner(p, db, 2)
    whole_plane(2)
    for p in pieces[1:]:
        for db in order:
            for dd in order:
                copies[p][("p", db, dd)].wait_recv()
    for p in pieces:
        for cp in copies[p].values():
            cp.wait_send()


GATHER_COPIES = 44


def my_coord():
    me = lax.axis_index("sp")
    return {
        "core": lax.rem(me, CORES),
        "x": lax.rem(me // CORES, RING),
        "y": lax.rem(me // (CORES * RING), RING),
        "z": me // (CORES * RING * RING),
    }


SUB_KEYS = 32
LATENT_PARTS = 4
WEIGHT_HEAD = 32


def attend_kernel(x_ref, pos_own, w_dq, g_q, w_dkv, g_kv, w_uq, w_ukv, lane_freq, inv_freq, pick, wo_ref, w_own,
                  y_ref, w_left, w_right, w_far,
                  kv_buf, q_buf, trig, q_ref, k_ref, v_ref, pos_ref, dq_buf, dkv_buf, kv_lin, wq_win, wkv_win, wq, wv,
                  s_even, s_odd, p_even, p_odd, acc_o, stats, o_buf, o_all, w_buf, acc, y_half, y_in,
                  lat_sem, head_sem, g_send, g_recv, block_sem, w_sem, send_sem, recv_sem, fwd_send, fwd_recv, y_sem,
                  *, blk, n_buf):
    coord = my_coord()
    core, x, y, z = (coord[a] for a in ("core", "x", "y", "z"))
    me = lax.axis_index("sp")
    y_top, y_low = y // 2, lax.rem(y, 2)
    lines = RING * RING
    n_chips = lines * RING
    chip_rows = o_all.shape[3]
    w_rows, cols = w_buf.shape[1], w_buf.shape[2]
    mesh_id = pl.DeviceIdType.MESH
    n_blk = q_ref.shape[1] // blk
    n_pairs = n_blk * (n_blk + 1) // 2
    per_z = n_blk // RING
    f32, bf16, i32 = jnp.float32, jnp.bfloat16, jnp.int32
    scale = SCORE_SCALE * LOG2E
    nt = (((1,), (1,)), ((), ()))
    half = ROPE_DIM // 2
    own_tok, dim = x_ref.shape
    part_rows = dim // LATENT_PARTS

    def lat_copies(n):
        rows = pl.ds(n * part_rows, part_rows)
        return (pltpu.make_async_copy(w_dq.at[rows, :], dq_buf.at[n % 2], lat_sem.at[0, n % 2]),
                pltpu.make_async_copy(w_dkv.at[:, rows], dkv_buf.at[n % 2], lat_sem.at[1, n % 2]))

    for n in range(2):
        for cp in lat_copies(n):
            cp.start()
    wide_q = wq_win.shape[1]
    head_copies = (
        pltpu.make_async_copy(w_uq.at[:, pl.ds(pl.multiple_of(me * QK_DIM - core * (wide_q - QK_DIM), 128), wide_q)], wq_win, head_sem.at[0]),
        pltpu.make_async_copy(w_ukv.at[:, pl.ds(pl.multiple_of(me * KV_DIM, 128), KV_DIM)], wkv_win, head_sem.at[1]))
    for cp in head_copies:
        cp.start()

    me_chip = (z * RING + y) * RING + x
    my_line = z * RING + y
    partner = {"sp": me_chip * CORES + 1 - core}
    z_up = {"sp": lax.rem(me_chip + lines, n_chips) * CORES + core}
    z_dn = {"sp": lax.rem(me_chip + n_chips - lines, n_chips) * CORES + core}

    barrier = pltpu.get_barrier_semaphore()
    pl.semaphore_signal(barrier, inc=1, device_id=partner, device_id_type=mesh_id)

    @pl.loop(1, n_chips)
    def _(n):
        to = {"sp": lax.rem(me_chip + n, n_chips) * CORES + core}
        pl.semaphore_signal(barrier, inc=1, device_id=to, device_id_type=mesh_id)

    for ref in (s_even, s_odd, p_even, p_odd):
        ref[...] = jnp.zeros_like(ref)
    acc_o[...] = jnp.zeros_like(acc_o)
    stats[...] = jnp.zeros_like(stats)
    acc[...] = jnp.zeros_like(acc)
    kv_lin[...] = jnp.zeros_like(kv_lin)
    pl.semaphore_wait(barrier, n_chips)

    total_rows = w_own.shape[0]
    cut = total_rows * 7 // 15
    block_copies = {}

    def send_rows(key, src, dst, lo, hi, dev):
        n = len(block_copies)
        cp = pltpu.make_async_remote_copy(
            src_ref=src.at[lo:hi], dst_ref=dst.at[lo:hi], send_sem=block_sem.at[0, n], recv_sem=block_sem.at[1, n],
            device_id=dev, device_id_type=mesh_id)
        cp.start()
        block_copies[key] = cp

    send_rows("l0", w_own, w_left, 0, WEIGHT_HEAD, z_up)
    send_rows("r0", w_own, w_right, cut, cut + WEIGHT_HEAD, z_dn)

    def send_blocks():
        send_rows("l1", w_own, w_left, WEIGHT_HEAD, cut, z_up)
        send_rows("r1", w_own, w_right, cut + WEIGHT_HEAD, total_rows, z_dn)
        send_rows("l2", w_own, w_left, cut, total_rows, z_up)
        send_rows("r2", w_own, w_right, 0, cut, z_dn)

    def pass_on():
        for key in ("l0", "l1", "r0", "r1"):
            block_copies[key].wait_recv()
        send_rows("f0", w_left, w_far, 0, cut, z_up)
        send_rows("f1", w_right, w_far, cut, total_rows, z_dn)

    q_lin = jnp.zeros((own_tok, dq_buf.shape[2]), f32)
    kv_sum = jnp.zeros((own_tok, dkv_buf.shape[1]), f32)
    for n in range(LATENT_PARTS):
        for cp in lat_copies(n):
            cp.wait()
        x_part = x_ref[:, n * part_rows:(n + 1) * part_rows]
        q_lin = q_lin + jnp.dot(x_part, dq_buf[n % 2], preferred_element_type=f32)
        kv_sum = kv_sum + lax.dot_general(x_part, dkv_buf[n % 2], nt, preferred_element_type=f32)
        if n + 2 < LATENT_PARTS:
            for cp in lat_copies(n + 2):
                cp.start()
    here = (z, y, x, core)
    q_buf[here] = rms_norm(q_lin, g_q[...]).astype(bf16)
    kv_buf[here + (slice(None), slice(0, KV_LATENT))] = rms_norm(kv_sum[:, :KV_LATENT], g_kv[...]).astype(bf16)
    kv_lin[:, :KV_LATENT + ROPE_DIM] = kv_sum
    turn = kv_lin[:, KV_LATENT:]
    lane = lax.broadcasted_iota(i32, turn.shape, 1)
    pos_f = pos_own[...].astype(f32)
    angle = pos_f * lane_freq[...]
    other = jnp.where(lane < half, -pltpu.roll(turn, turn.shape[1] - half, 1), pltpu.roll(turn, half, 1))
    turned = turn * jnp.cos(angle) + other * jnp.sin(angle)
    pos_hi = jnp.floor(pos_f * (1.0 / 64.0))
    tail = jnp.where(lane < ROPE_DIM, turned, jnp.where(lane == ROPE_DIM, pos_hi, jnp.where(lane == ROPE_DIM + 1, pos_f - 64.0 * pos_hi, 0.0)))
    kv_buf[here + (slice(None), slice(KV_LATENT, None))] = tail.astype(bf16)

    def line_of(n):
        step = n // 2
        return lax.rem(z + step // 2, RING) * RING + lax.rem(y_top + lax.rem(step, 2), 2) * 2 + lax.rem(y_low + lax.rem(n, 2), 2)

    def block_of(n):
        return lax.rem(z + RING - n // per_z, RING) * per_z + lax.rem(y_top + lax.rem(n, per_z), per_z)

    def w_copy(n):
        rows = pl.ds(pl.multiple_of(line_of(n) * w_rows, w_rows), w_rows)
        side = pl.ds(pl.multiple_of(core * cols, 128), cols)
        slot = lax.rem(n, n_buf)
        return pltpu.make_async_copy(wo_ref.at[rows, side], w_buf.at[slot], w_sem.at[slot])

    def head_weights():
        for cp in head_copies:
            cp.wait()
        turned_w = wq_win[...].astype(f32).T
        low, high = turned_w[:QK_DIM], turned_w[wide_q - QK_DIM:]
        wq[...] = jnp.where(core == 0, low, high).astype(bf16)
        wv[...] = wkv_win[:, NOPE_DIM:].astype(f32).T.astype(bf16)

        @pl.loop(0, n_buf)
        def _(n):
            w_copy(n).start()

    row_tok = RING * CORES * own_tok

    def keys_values(yy):
        @pl.loop(0, RING)
        def _(zz):
            lat = kv_buf[zz, yy].reshape(row_tok, kv_buf.shape[5])
            tail = lat[:, KV_LATENT:]
            lat = lat[:, :KV_LATENT]
            rows = pl.ds(pl.multiple_of((zz * RING + yy) * row_tok, row_tok), row_tok)
            k_ref[rows, :NOPE_DIM] = jnp.dot(lat, wkv_win[:, :NOPE_DIM], preferred_element_type=f32).astype(bf16)
            k_ref[rows, NOPE_DIM:] = tail
            v_ref[:, rows] = lax.dot_general(wv[...], lat, nt, preferred_element_type=f32).astype(bf16)
            pos = lax.dot_general(pick[...], tail, nt, preferred_element_type=f32)
            pos_ref[:, rows] = pos
            angle = inv_freq[...] * pos[0:1]
            trig[:half, rows] = jnp.cos(angle)
            trig[half:, rows] = jnp.sin(angle)

    def on_z_free():
        send_blocks()
        head_weights()

    gather_latents((kv_buf, q_buf), coord, g_send, g_recv, on_z_free, keys_values)
    pass_on()

    lines_per_blk = blk // row_tok
    steps_z = RING // lines_per_blk

    @pl.loop(0, n_blk)
    def _(n):
        at = (n // steps_z, pl.ds(lax.rem(n, steps_z) * lines_per_blk, lines_per_blk))
        lat = q_buf[at].reshape(blk, q_buf.shape[5])
        rows = pl.ds(pl.multiple_of(n * blk, blk), blk)
        cosine, sine = trig[:half, rows], trig[half:, rows]
        qt = lax.dot_general(wq[...], lat, nt, preferred_element_type=f32)
        lo, hi = qt[NOPE_DIM:NOPE_DIM + half], qt[NOPE_DIM + half:]
        q_ref[:NOPE_DIM, rows] = qt[:NOPE_DIM].astype(bf16)
        q_ref[NOPE_DIM:NOPE_DIM + half, rows] = (lo * cosine - hi * sine).astype(bf16)
        q_ref[NOPE_DIM + half:QK_DIM, rows] = (hi * cosine + lo * sine).astype(bf16)
        q_ref[QK_DIM:, rows] = jnp.zeros((2 * NOPE_DIM - QK_DIM, blk), bf16)

    chips_per_blk = blk // chip_rows

    def send_block(i):
        line0 = i * (chips_per_blk // RING)

        @pl.loop(0, chips_per_blk)
        def _(n):
            yy = line0 + lax.rem(y_low + n // RING, chips_per_blk // RING)
            to = yy * RING + lax.rem(x + lax.rem(n, RING), RING)
            rows = pl.ds(pl.multiple_of(to * chip_rows, chip_rows), chip_rows)

            @pl.when(to == me_chip)
            def _():
                o_all[my_line, x, core] = o_buf[rows, :]

            @pl.when(to != me_chip)
            def _():
                pltpu.make_async_remote_copy(
                    src_ref=o_buf.at[rows, :], dst_ref=o_all.at[my_line, x, core], send_sem=send_sem,
                    recv_sem=recv_sem.at[my_line], device_id={"sp": to * CORES + core}, device_id_type=mesh_id).start()

    sub = SUB_KEYS
    fold = lambda v: v.reshape(sub // 8, 8, blk)
    row_id = lax.broadcasted_iota(i32, (sub, blk), 0)

    def body(t, s_a, s_b, p_a, p_b, carry):
        (n_a, i_a, j_a), (i_b, j_b), (i_c, j_c), i_done = carry
        m_old, l_old, top, alpha_c = stats[0:1], stats[1:2], stats[2:3], stats[3:4]

        keys_c = pl.ds(pl.multiple_of(j_c * blk, blk), blk)
        pv = jnp.dot(v_ref[:, keys_c], p_a[...], preferred_element_type=f32)
        acc_o[...] = acc_o[...] * alpha_c + pv

        first = j_b == 0
        m_prev = jnp.where(first, MASKED, m_old)
        m_new = jnp.maximum(m_prev, top)
        alpha_b = jnp.where(first, 0.0, jnp.exp2((m_prev - m_new) * scale))
        part = jnp.zeros((8, blk), f32)
        for g in range(blk // sub):
            p = jnp.exp2((s_b[g * sub:(g + 1) * sub, :] - m_new) * scale)
            part = part + jnp.sum(fold(p), axis=0)
            p_b[g * sub:(g + 1) * sub, :] = p.astype(bf16)
        l_new = l_old * alpha_b + jnp.sum(part, axis=0, keepdims=True)

        cols_a = pl.ds(pl.multiple_of(i_a * blk, blk), blk)
        pos = pos_ref[0:1, cols_a].astype(i32)
        first_key = i_a * blk + lax.broadcasted_iota(i32, (1, blk), 1) - pos - j_a * blk
        reach = pos.astype(jnp.uint32)
        peak = jnp.full((8, blk), MASKED, f32)
        wide = blk // 2
        for h in range(2):
            keys_a = pl.ds(pl.multiple_of(j_a * blk + h * wide, wide), wide)
            s = jnp.dot(k_ref[keys_a, :], q_ref[:, cols_a], preferred_element_type=f32)
            for g in range(wide // sub):
                back = row_id - (first_key - (h * wide + g * sub))
                kept = jnp.where(back.astype(jnp.uint32) <= reach, s[g * sub:(g + 1) * sub], MASKED)
                peak = jnp.maximum(peak, jnp.max(fold(kept), axis=0))
                s_a[h * wide + g * sub:h * wide + (g + 1) * sub, :] = kept
        top_new = jnp.max(peak, axis=0, keepdims=True)

        @pl.when(i_done >= 0)
        def _():
            send_block(i_done)

        done = (t >= 2) & (t < n_pairs + 2) & (j_c == i_c)

        @pl.when(done)
        def _():
            o_buf[pl.ds(pl.multiple_of(i_c * blk, blk), blk), :] = (acc_o[...] / stats[1:2]).T.astype(bf16)

        stats[0:1] = m_new
        stats[1:2] = l_new
        stats[2:3] = top_new
        stats[3:4] = alpha_b

        last = j_a == i_a
        n_next = jnp.where(last, jnp.minimum(n_a + 1, n_blk - 1), n_a)
        i_next = block_of(n_next)
        j_next = jnp.where(last, 0, j_a + 1)
        return (n_next, i_next, j_next), (i_a, j_a), (i_b, j_b), jnp.where(done, i_c, -1)

    zero = jnp.int32(0)

    def two(u, carry):
        carry = body(2 * u, s_even, s_odd, p_even, p_odd, carry)
        return body(2 * u + 1, s_odd, s_even, p_odd, p_even, carry)

    lax.fori_loop(0, (n_pairs + 4) // 2, two, ((zero, block_of(zero), zero), (zero, zero), (zero, zero), jnp.int32(-1)))

    def forward(n):
        at = o_all.at[line_of(n), :, core]
        return pltpu.make_async_remote_copy(
            src_ref=at, dst_ref=at, send_sem=fwd_send.at[n], recv_sem=fwd_recv.at[n], device_id=partner, device_id_type=mesh_id)

    def arrive(n, n_heads):
        at = o_all.at[line_of(n), pl.ds(0, n_heads), core]
        pltpu.make_async_copy(at, at, recv_sem.at[line_of(n)]).wait()
        forward(n).start()

    arrive(0, RING - 1)

    @pl.loop(0, lines)
    def _(n):
        @pl.when(n + 1 < lines)
        def _():
            arrive(n + 1, RING)

        forward(n).wait_recv()
        w_copy(n).wait()
        line = line_of(n)
        lhs = jnp.concatenate([o_all[line, i, j] for i in range(RING) for j in range(CORES)], axis=1)
        acc[...] += jnp.dot(lhs, w_buf[lax.rem(n, n_buf)], preferred_element_type=f32)

        @pl.when(n + n_buf < lines)
        def _():
            w_copy(n + n_buf).start()

    own_rows = chip_rows // CORES
    y_half[...] = acc[...].astype(bf16)
    swap = pltpu.make_async_remote_copy(
        src_ref=y_half.at[pl.ds(pl.multiple_of((1 - core) * own_rows, own_rows), own_rows), :], dst_ref=y_in,
        send_sem=y_sem.at[0], recv_sem=y_sem.at[1], device_id=partner, device_id_type=mesh_id)
    swap.start()
    mine = y_half[pl.ds(pl.multiple_of(core * own_rows, own_rows), own_rows), :]
    swap.wait_recv()
    other = y_in[...]
    y_ref[:, :cols] = jnp.where(core == 0, mine, other)
    y_ref[:, cols:] = jnp.where(core == 0, other, mine)
    swap.wait_send()

    @pl.loop(0, lines)
    def _(n):
        forward(n).wait_send()

    everything = o_buf.at[pl.ds(0, (n_chips - 1) * chip_rows), :]
    pltpu.make_async_copy(everything, everything, send_sem).wait()
    for key in ("l2", "r2", "f0", "f1"):
        block_copies[key].wait_recv()
    for cp in block_copies.values():
        cp.wait_send()


def attend_project(x_blk, pos_blk, w_dq, g_q, w_dkv, g_kv, w_uq, w_ukv, w_o, w_own, blk, group_size, n_buf):
    own_rows, dim = x_blk.shape
    tok = own_rows * group_size
    lines = RING * RING
    w_rows = w_o.shape[0] // lines
    side = dim // CORES
    f32, bf16 = jnp.float32, jnp.bfloat16
    half = ROPE_DIM // 2
    inv_freq = 10000.0 ** (-jnp.arange(half, dtype=f32) / half)
    lane = jnp.arange(NOPE_DIM)[None, :]
    pick = jnp.where(jnp.arange(8)[:, None] == 0, jnp.where(lane == ROPE_DIM, 64.0, jnp.where(lane == ROPE_DIM + 1, 1.0, 0.0)), 0.0).astype(bf16)
    q_lat = w_dq.shape[1]
    kv_wide = KV_LATENT + NOPE_DIM
    part = dim // LATENT_PARTS
    wide_q = 2 * NOPE_DIM
    vm = pl.BlockSpec(memory_space=pltpu.VMEM)
    hbm = pl.BlockSpec(memory_space=pl.ANY)
    n_p = len(GATHER_ORDERS)
    dma = pltpu.SemaphoreType.DMA
    w_out = jax.ShapeDtypeStruct(w_own.shape, bf16)
    return pl.pallas_call(
        functools.partial(attend_kernel, blk=blk, n_buf=n_buf),
        name="attend_project",
        out_shape=(jax.ShapeDtypeStruct((own_rows, dim), bf16), w_out, w_out, w_out),
        in_specs=[vm, vm, hbm, vm, hbm, vm, hbm, hbm, vm, vm, vm, hbm, hbm],
        out_specs=(vm, hbm, hbm, hbm),
        scratch_shapes=[
            pltpu.VMEM((RING, RING, RING, CORES, own_rows, kv_wide), bf16),
            pltpu.VMEM((RING, RING, RING, CORES, own_rows, q_lat), bf16),
            pltpu.VMEM((ROPE_DIM, tok), f32),
            pltpu.VMEM((2 * NOPE_DIM, tok), bf16),
            pltpu.VMEM((tok, 2 * NOPE_DIM), bf16),
            pltpu.VMEM((VALUE_DIM, tok), bf16),
            pltpu.VMEM((8, tok), f32),
            pltpu.VMEM((2, part, q_lat), bf16),
            pltpu.VMEM((2, KV_LATENT + ROPE_DIM, part), bf16),
            pltpu.VMEM((own_rows, kv_wide), f32),
            pltpu.VMEM((q_lat, wide_q), bf16),
            pltpu.VMEM((KV_LATENT, KV_DIM), bf16),
            pltpu.VMEM((QK_DIM, q_lat), bf16),
            pltpu.VMEM((VALUE_DIM, KV_LATENT), bf16),
            pltpu.VMEM((blk, blk), f32),
            pltpu.VMEM((blk, blk), f32),
            pltpu.VMEM((blk, blk), bf16),
            pltpu.VMEM((blk, blk), bf16),
            pltpu.VMEM((VALUE_DIM, blk), f32),
            pltpu.VMEM((8, blk), f32),
            pltpu.VMEM((tok, VALUE_DIM), bf16),
            pltpu.VMEM((lines, RING, CORES, CORES * own_rows, VALUE_DIM), bf16),
            pltpu.VMEM((n_buf, w_rows, side), bf16),
            pltpu.VMEM((CORES * own_rows, side), f32),
            pltpu.VMEM((CORES * own_rows, side), bf16),
            pltpu.VMEM((own_rows, side), bf16),
            dma((2, 2)), dma((2,)),
            dma((n_p, GATHER_COPIES)), dma((n_p, GATHER_COPIES)),
            dma((2, 8)),
            dma((n_buf,)), dma, dma((lines,)), dma((lines,)), dma((lines,)), dma((2,)),
        ],
        cost_estimate=pl.CostEstimate(flops=18_000_000_000, bytes_accessed=80_000_000, transcendentals=9_000_000),
        compiler_params=pltpu.CompilerParams(collective_id=3, has_side_effects=True, vmem_limit_bytes=62 << 20),
    )(x_blk, pos_blk[:, None], w_dq, g_q[None, :], w_dkv.T, g_kv[None, :], w_uq, w_ukv, jnp.tile(inv_freq, NOPE_DIM // half)[None, :],
      inv_freq[:, None], pick, w_o, w_own)


def ffn_kernel(y_ref, g_ref, *rest, dim, pad, sub, tile_n):
    n_wt = 4
    weights = rest[:n_wt]
    (out_ref, ybuf, wgu, wdn, hbuf, gubuf, part, far_l, far_r, in_l, in_r, far2_l, far2_r, in2_l, in2_r,
     w_sem, wx_send, wx_recv, ag_send, ag_recv, rs_send, rs_recv) = rest[n_wt:]
    coord = my_coord()

    def device(axis, by):
        c = {**coord, axis: lax.rem(coord[axis] + (by % RING), RING) if axis != "core" else 1 - coord[axis]}
        return {"sp": ((c["z"] * RING + c["y"]) * RING + c["x"]) * CORES + c["core"]}

    x_up, x_dn, y_up, y_dn = device("x", 1), device("x", -1), device("y", 1), device("y", -1)
    partner = device("core", 1)
    up1, dn1, up2, dn2 = (x_up, y_up), (x_dn, y_dn), (y_up, x_up), (y_dn, x_dn)

    barrier = pltpu.get_barrier_semaphore()
    for nb in (x_up, x_dn, y_up, y_dn, partner):
        pl.semaphore_signal(barrier, inc=1, device_id=nb, device_id_type=pl.DeviceIdType.MESH)

    w_copies = []

    def fetch(src, dst):
        cp = pltpu.make_async_copy(src, dst, w_sem.at[len(w_copies)])
        cp.start()
        w_copies.append(cp)

    up0 = 8 * pad
    for n, blk in enumerate(weights):
        r = n * pad
        fetch(blk.at[0:pad], wgu.at[r:r + pad])
        fetch(blk.at[pad:2 * pad], wgu.at[up0 + r:up0 + r + pad])
        fetch(blk.at[2 * pad:], wdn.at[r:r + pad])

    wx_copies = []

    def exchange(buf, src, dst, rows, dev):
        n = len(wx_copies)
        cp = pltpu.make_async_remote_copy(
            src_ref=buf.at[src:src + rows], dst_ref=buf.at[dst:dst + rows], send_sem=wx_send.at[n], recv_sem=wx_recv.at[n],
            device_id=dev, device_id_type=pl.DeviceIdType.MESH)
        cp.start()
        wx_copies.append(cp)

    for h in range(2):
        ybuf[h, 0] = y_ref[h * sub:(h + 1) * sub, :]
    pl.semaphore_wait(barrier, 5)

    cols = (slice(0, dim // 2), slice(dim // 2, dim))
    ag_copies = {}
    ag_n = [0]

    def ag_send_to(h, src_slot, dst_slot, dev, col=None):
        c = slice(None) if col is None else cols[col]
        key = (h, dst_slot, col)
        rsem = dst_slot if col != 1 else RING * RING
        cp = pltpu.make_async_remote_copy(
            src_ref=ybuf.at[h, src_slot, :, c], dst_ref=ybuf.at[h, dst_slot, :, c],
            send_sem=ag_send.at[ag_n[0]], recv_sem=ag_recv.at[h, rsem],
            device_id=dev, device_id_type=pl.DeviceIdType.MESH)
        ag_n[0] += 1
        cp.start()
        ag_copies[key] = cp

    far = 2
    for h in range(2):
        ag_send_to(h, 0, 3 * RING, up1[h])
        ag_send_to(h, 0, 1 * RING, dn1[h])
    for h in range(2):
        ag_send_to(h, 0, 3, up2[h])
        ag_send_to(h, 0, 1, dn2[h])
    for cp in w_copies:
        cp.wait()
    exchange(wgu, 0, 4 * pad, 4 * pad, partner)
    exchange(wgu, up0, up0 + 4 * pad, 4 * pad, partner)
    exchange(wdn, 0, 4 * pad, 4 * pad, partner)
    for h in range(2):
        ag_copies[(h, 3 * RING, None)].wait_recv()
        ag_send_to(h, 3 * RING, far * RING, up1[h], 0)
        ag_copies[(h, 1 * RING, None)].wait_recv()
        ag_send_to(h, 1 * RING, far * RING, dn1[h], 1)
        for d1 in (3, 1):
            ag_send_to(h, d1 * RING, d1 * RING + 3, up2[h])
            ag_send_to(h, d1 * RING, d1 * RING + 1, dn2[h])
    for h in range(2):
        ag_copies[(h, far * RING, 0)].wait_recv()
        ag_copies[(h, far * RING, 1)].wait_recv()
        ag_send_to(h, far * RING, far * RING + 3, up2[h])
        ag_send_to(h, far * RING, far * RING + 1, dn2[h])
    for d1, d2, dev in ((0, 3, up2), (3, 3, up2), (1, 1, dn2), (2, 1, dn2)):
        for h in range(2):
            ag_copies[(h, d1 * RING + d2, None)].wait_recv()
            ag_send_to(h, d1 * RING + d2, d1 * RING + far, dev[h])
    for d1, d2 in ((0, 1), (3, 1), (1, 3), (2, 3), (0, 2), (3, 2), (1, 2), (2, 2)):
        for h in range(2):
            ag_copies[(h, d1 * RING + d2, None)].wait_recv()

    for cp in wx_copies:
        cp.wait_recv()

    rows = 2 * RING * sub
    nt = (((1,), (1,)), ((), ()))
    ff_pad = 8 * pad

    def compute(d1):
        for h in range(2):
            for d2 in range(RING):
                v = ybuf[h, d1 * RING + d2].astype(jnp.float32)
                mean_sq = jnp.mean(v * v, axis=-1, keepdims=True)
                r = (h * RING + d2) * sub
                hbuf[r:r + sub, :] = (v * lax.rsqrt(mean_sq + 1e-6) * g_ref[...].astype(jnp.float32)).astype(jnp.bfloat16)
        n_gu = gubuf.shape[1] // tile_n

        @pl.loop(0, n_gu)
        def _(j):
            c = pl.ds(pl.multiple_of(j * tile_n, tile_n), tile_n)
            gubuf[:, c] = lax.dot_general(hbuf[...], wgu[c, :], nt, preferred_element_type=jnp.float32)

        gate = gubuf[:, :ff_pad]
        act = (gate * jax.nn.sigmoid(gate) * gubuf[:, ff_pad:]).astype(jnp.bfloat16)
        wide = dim // 7 if dim % (7 * 128) == 0 else dim
        for j in range(dim // wide):
            c = slice(j * wide, (j + 1) * wide)
            res = jnp.dot(act, wdn[:, c], preferred_element_type=jnp.float32)
            for h in range(2):
                for d2 in range(RING):
                    r = (h * RING + d2) * sub
                    part[h, d1 * RING + d2, :, c] = res[r:r + sub]

    rs_copies = {}
    rs_n = [0]

    def rs_send_to(key, src, dst, dev):
        cp = pltpu.make_async_remote_copy(
            src_ref=src, dst_ref=dst, send_sem=rs_send.at[rs_n[0]], recv_sem=rs_recv.at[rs_n[0]],
            device_id=dev, device_id_type=pl.DeviceIdType.MESH)
        rs_n[0] += 1
        cp.start()
        rs_copies[key] = cp

    order = (2, 1, 3, 0)
    compute(far)
    for d2 in order:
        for h in range(2):
            rs_send_to(("fl", h, d2), part.at[h, far * RING + d2, :, cols[0]], far_l.at[h, d2], up1[h])
            rs_send_to(("fr", h, d2), part.at[h, far * RING + d2, :, cols[1]], far_r.at[h, d2], dn1[h])
    compute(1)
    compute(3)
    for d2 in order:
        for h in range(2):
            rs_copies[("fl", h, d2)].wait_recv()
            part[h, RING + d2, :, cols[0]] += far_l[h, d2]
            rs_send_to(("il", h, d2), part.at[h, RING + d2], in_l.at[h, d2], up1[h])
            rs_copies[("fr", h, d2)].wait_recv()
            part[h, 3 * RING + d2, :, cols[1]] += far_r[h, d2]
            rs_send_to(("ir", h, d2), part.at[h, 3 * RING + d2], in_r.at[h, d2], dn1[h])
    compute(0)

    def first_sum(h, d2):
        rs_copies[("il", h, d2)].wait_recv()
        rs_copies[("ir", h, d2)].wait_recv()
        part[h, d2] = part[h, d2] + in_l[h, d2] + in_r[h, d2]

    for h in range(2):
        first_sum(h, 2)
        rs_send_to(("gl", h), part.at[h, 2, :, cols[0]], far2_l.at[h], up2[h])
        rs_send_to(("gr", h), part.at[h, 2, :, cols[1]], far2_r.at[h], dn2[h])
    for h in range(2):
        first_sum(h, 1)
        rs_copies[("gl", h)].wait_recv()
        part[h, 1, :, cols[0]] += far2_l[h]
        rs_send_to(("jl", h), part.at[h, 1], in2_l.at[h], up2[h])
        first_sum(h, 3)
        rs_copies[("gr", h)].wait_recv()
        part[h, 3, :, cols[1]] += far2_r[h]
        rs_send_to(("jr", h), part.at[h, 3], in2_r.at[h], dn2[h])
    for h in range(2):
        first_sum(h, 0)
        rs_copies[("jl", h)].wait_recv()
        rs_copies[("jr", h)].wait_recv()
        total = part[h, 0] + in2_l[h] + in2_r[h]
        out_ref[h * sub:(h + 1) * sub, :] = (ybuf[h, 0].astype(jnp.float32) + total).astype(jnp.bfloat16)
    for cp in wx_copies + list(ag_copies.values()) + list(rs_copies.values()):
        cp.wait_send()


def ffn(y_own, g_ffn, weights, pad):
    rows, dim = y_own.shape
    sub = rows // 2
    chunk = 2 * RING * sub
    f32, bf16 = jnp.float32, jnp.bfloat16
    vm = pl.BlockSpec(memory_space=pltpu.VMEM)
    hbm = pl.BlockSpec(memory_space=pl.ANY)
    half = dim // 2
    return pl.pallas_call(
        functools.partial(ffn_kernel, dim=dim, pad=pad, sub=sub, tile_n=256 if (16 * pad) % 256 == 0 else 16 * pad),
        name="ffn",
        out_shape=jax.ShapeDtypeStruct((rows, dim), bf16),
        in_specs=[vm, vm] + [hbm] * 4,
        out_specs=vm,
        scratch_shapes=[
            pltpu.VMEM((2, RING * RING, sub, dim), bf16),
            pltpu.VMEM((16 * pad, dim), bf16),
            pltpu.VMEM((8 * pad, dim), bf16),
            pltpu.VMEM((chunk, dim), bf16),
            pltpu.VMEM((chunk, 16 * pad), f32),
            pltpu.VMEM((2, RING * RING, sub, dim), f32),
            pltpu.VMEM((2, RING, sub, half), f32),
            pltpu.VMEM((2, RING, sub, half), f32),
            pltpu.VMEM((2, RING, sub, dim), f32),
            pltpu.VMEM((2, RING, sub, dim), f32),
            pltpu.VMEM((2, sub, half), f32),
            pltpu.VMEM((2, sub, half), f32),
            pltpu.VMEM((2, sub, dim), f32),
            pltpu.VMEM((2, sub, dim), f32),
            pltpu.SemaphoreType.DMA((12,)),
            pltpu.SemaphoreType.DMA((3,)),
            pltpu.SemaphoreType.DMA((3,)),
            pltpu.SemaphoreType.DMA((32,)),
            pltpu.SemaphoreType.DMA((2, RING * RING + 1)),
            pltpu.SemaphoreType.DMA((40,)),
            pltpu.SemaphoreType.DMA((40,)),
        ],
        cost_estimate=pl.CostEstimate(flops=7_000_000_000, bytes_accessed=14_000_000, transcendentals=0),
        compiler_params=pltpu.CompilerParams(collective_id=1, has_side_effects=True, vmem_limit_bytes=56 << 20),
    )(y_own, g_ffn[None, :], *weights)


def weight_block(w_gate, w_up, w_down):
    cols = w_down.shape[0]
    pad = -(-cols // 16) * 16
    wide = lambda w: jnp.pad(w, ((0, pad - cols), (0, 0)))
    return jnp.concatenate([wide(w_gate.T), wide(w_up.T), wide(w_down)], axis=0), pad


def solution(mesh):
    group_size = mesh.shape['sp']
    tok_spec = P(('dp', 'sp'), None)
    row_spec = P(('dp', 'sp'))
    full_spec = P()
    col_spec = P(None, 'sp')

    def device_fn(x_blk, seg_blk, pos_blk, w_dq, g_q, w_uq, w_dkv, g_kv, w_ukv, w_o, g_ffn, w_gate, w_up, w_down):
        blk_len = x_blk.shape[0]
        tok_total = blk_len * group_size
        w_own, pad = weight_block(w_gate, w_up, w_down)

        y_att, w_left, w_right, w_far = attend_project(
            x_blk, pos_blk, w_dq, g_q, w_dkv, g_kv, w_uq, w_ukv, w_o, w_own, min(512, tok_total), group_size, 8)
        return ffn(y_att, g_ffn, (w_own, w_left, w_right, w_far), pad)

    return jax.shard_map(device_fn, mesh=mesh, in_specs=(tok_spec, row_spec, row_spec, full_spec, full_spec, full_spec, full_spec, full_spec, full_spec, full_spec, full_spec, col_spec, col_spec, P('sp', None)), out_specs=tok_spec, check_vma=False)
```
